512 devices in a mesh: grp: 2 (over y), ctx: 64 (over z, core), sub: 4 (over x).
Axes of the slice: x: 4, y: 2, z: 32, core: 2. Of those that a mesh axis runs over, the one named last changes fastest.
The devices are a block of a 4x8x32 slice.
Arguments:
- queries: bfloat16 [1024, 3072], P(('grp', 'ctx'), 'sub'), parts along dimension 0, may hold values from -1024 to 1024
- latent_cache: bfloat16 [49152, 576], P(('grp', 'ctx')), parts along dimension 0, may hold values from -8 to 8
- cache_len: int32 [128], P(('grp', 'ctx')), parts along dimension 0, may hold values from 16 to 384, as said below
- kv_up: bfloat16 [32, 256, 512], P(('grp', 'sub'), None, 'ctx'), parts along dimension 0, may hold values from -1 to 1
- o_weight: bfloat16 [2048, 2048], P('sub', 'ctx'), may hold values from -0.5 to 0.5
- residual: bfloat16 [1024, 2048], P(('grp', 'ctx')), parts along dimension 0, may hold values from -3 to 3
- norm_gain: bfloat16 [2048], replicated, may hold values from 0.25 to 1.75
- route_ids: int32 [1024, 6], P(('grp', 'ctx')), parts along dimension 0, may hold values from 0 to 63, all different within a row; in each aligned block of 8 rows (0 to 7, 8 to 15, ...) at most 2 rows name the same one
- route_weights: float32 [1024, 6], P(('grp', 'ctx')), parts along dimension 0, may hold values from 0.1 to 0.6
- w_gate: bfloat16 [64, 2048, 1408], P('ctx', None, 'sub'), may hold values from -0.125 to 0.125
- w_up: bfloat16 [64, 2048, 1408], P('ctx', None, 'sub'), may hold values from -0.125 to 0.125
- w_down: bfloat16 [64, 1408, 2048], P('ctx', 'sub'), may hold values from -0.15625 to 0.15625
Outputs:
- layer_out: bfloat16 [1024, 2048], P(('grp', 'ctx'), 'sub'), parts along dimension 0
The draws below stay inside these ranges and needn't reach their ends.
There are 2 independent parts, one for each index of `grp`. The reference program is written for one: setup_inputs(seed, part) draws one part's arguments, and reference() takes and returns one part's arrays. A program takes and returns all parts, laid end to end along the dimension named above; an argument that names none is the same for every part. Nothing has to cross between parts.
Inputs may be any that keep to these rules, and one draw needn't show every extreme that they name: `route_ids`: each row names 6 different experts. Among the 8 rows of one ctx index no expert is named more than 2 times, and in every draw some expert is named exactly 2 times by the rows of some ctx index. cache_len[c] positions at the start of shard c are live; at least one shard is full.
All inputs are finite; a program needn't handle non-finite values.
Results may differ from the reference program's by a relative error of at most 0.015.
Values may be sent and summed in bfloat16 or wider, within the bound.
No kernel may reach another device: no remote copies, remote signals or barrier semaphores. Data moves between devices by JAX's collectives and lax.ppermute only.
A program may use at most 64 MiB of HBM per device.

```python
import math
import jax
import jax.numpy as jnp
import numpy as np
from jax import lax

D = 2048
HEADS = 16
NOPE = 128
ROPE = 64
VDIM = 128
LATENT = 512
FF = 1408
EXPERTS = 64
TOP = 6
TOK_DEV = 8
CACHE_DEV = 384
CAP = 2
SPAN = 512
CACHE = 24576
N_CTX = 64


def draw_tables(key):
    base_key = jax.random.fold_in(key, 7)
    cache_key, up_key, query_key = jax.random.split(base_key, 3)
    row_width = LATENT + ROPE
    cache_rows = jnp.clip(jax.random.normal(cache_key, (CACHE, row_width), jnp.float32), -6.0, 6.0)
    up_table = jnp.clip(jax.random.normal(up_key, (HEADS, NOPE + VDIM, LATENT), jnp.float32), -6.0, 6.0) * LATENT ** (-0.5)
    query_table = jnp.clip(jax.random.normal(query_key, (SPAN, HEADS, NOPE + ROPE), jnp.float32), -6.0, 6.0) * 2.5
    return (cache_rows, up_table, query_table)


def draw_queries(key, part):
    tables = draw_tables(key)
    return tables[2].reshape(SPAN, HEADS * (NOPE + ROPE)).astype(jnp.bfloat16)


def draw_latent_cache(key, part):
    tables = draw_tables(key)
    return tables[0].astype(jnp.bfloat16)


def draw_kv_up(key, part):
    tables = draw_tables(key)
    return tables[1].astype(jnp.bfloat16)


def draw_cache_len(key, part):
    length_key, full_key = jax.random.split(jax.random.fold_in(key, 11))
    halvings = jax.random.randint(length_key, (N_CTX,), 0, 5)
    lengths = jnp.maximum(jnp.right_shift(jnp.full((N_CTX,), CACHE_DEV, jnp.int32), halvings.astype(jnp.int32)), 16)
    full_index = jax.random.randint(full_key, (), 0, N_CTX)
    return jnp.where(jnp.arange(N_CTX, dtype=jnp.int32) == full_index, CACHE_DEV, lengths).astype(jnp.int32)


def shard_levels(key, dims, cuts, least, top_value):
    def one(position, blocks):
        draws = jax.random.uniform(jax.random.fold_in(jax.random.fold_in(key, 6), position), (blocks,), jnp.float32, least / len(cuts), top_value / len(cuts))
        return jnp.repeat(jnp.exp(draws), dims[position] // blocks).reshape((-1,) + (1,) * (len(dims) - position - 1))

    gain = one(*cuts[0])
    for cut in cuts[1:]:
        gain = gain * one(*cut)
    return gain


def assign_block(rng, own, number, rows, count, top, bound, lean):
    ranking = jax.random.permutation(rng, count)
    packed, usual = portions_of(count, rows * top, bound, lean, True), portions_of(count, rows * top, bound, lean, False)
    places = jnp.arange(count)

    def named(sizes, rotation):
        used = int((sizes > 0).sum())
        fixed = max(1, used // 4)
        moved = fixed + (places - fixed + rotation * (used - fixed)) % max(1, count - fixed)
        return jnp.zeros((count,), jnp.int32).at[ranking[jnp.where(places < fixed, places, moved)]].set(jnp.asarray(sizes, jnp.int32))

    sizes = jnp.where(number % 4 == 0, named(packed, number // 4), named(usual, number - number // 4 - 1))
    mixed = jax.random.permutation(jax.random.fold_in(own, 3), count)
    giver, sink = mixed[0:count // 2 * 2:2], mixed[1:count // 2 * 2:2]
    margin = jnp.minimum(sizes[giver] - 1, bound - sizes[sink]) // 2
    margin = jnp.where((giver == ranking[0]) | (sink == ranking[0]) | (sizes[sink] == 0), 0, jnp.maximum(margin, 0))
    moved = jax.random.randint(jax.random.fold_in(own, 4), (count // 2,), 0, 1 << 20) % (margin + 1)
    sizes = sizes.at[giver].add(-moved).at[sink].add(moved)
    items = jnp.searchsorted(jnp.cumsum(sizes), jnp.arange(rows * top), side="right").astype(jnp.int32)
    table = items.reshape(top, rows).T
    table = table[jax.random.permutation(jax.random.fold_in(own, 1), rows)]
    rotation = jax.random.randint(jax.random.fold_in(own, 2), (rows, 1), 0, top)
    return jnp.take_along_axis(table, (jnp.arange(top)[None, :] + rotation) % top, axis=1)


def portions_of(number_of, total, bound, lean, full):
    loads = [(1 << 20) // math.isqrt(standing ** lean) + 1 for standing in range(1, number_of + 1)]
    largest = bound if full else min(bound, max(-(-total // number_of), total * loads[0] // sum(loads)))
    least = 1 if total - largest >= number_of - 1 else 0
    counts, spare = [largest] + [least] * (number_of - 1), total - largest - least * (number_of - 1)
    while spare > 0:
        movable = [i for i in range(1, number_of) if counts[i] < largest] or [i for i in range(1, number_of) if counts[i] < bound]
        pool, budget = sum([loads[i] for i in movable]), spare
        for i in movable:
            extra = min(bound - counts[i], max(1, budget * loads[i] // pool), spare)
            counts[i] = counts[i] + extra
            spare = spare - extra
    return np.array(counts)


def bell_draw(key, extent, spread, reach, cuts=(), kind=jnp.bfloat16):
    loudness = shard_levels(key, extent, cuts, -0.22, 0.18) if cuts else 1.0
    array = jax.random.normal(key, extent, jnp.float32) * spread * loudness
    return jnp.minimum(jnp.maximum(array, -reach), reach).astype(kind)


def setup_inputs(seed: int = 0, part: int = 0) -> dict:
    keys = jax.random.split(jax.random.key(seed), 13)
    part_keys = jax.random.split(jax.random.fold_in(keys[12], part), 13)
    queries = draw_queries(jax.random.fold_in(jax.random.fold_in(keys[12], part), 71), part)
    latent_cache = draw_latent_cache(jax.random.fold_in(jax.random.fold_in(keys[12], part), 71), part)
    cache_len = draw_cache_len(jax.random.fold_in(jax.random.fold_in(keys[12], part), 71), part)
    kv_up = draw_kv_up(jax.random.fold_in(jax.random.fold_in(keys[12], part), 71), part)
    o_weight = bell_draw(keys[4], (HEADS * VDIM, D), (HEADS * VDIM // 16) ** -0.5, 0.5, ((0, 4), (1, 64)))
    residual = bell_draw(part_keys[5], (SPAN, D), 0.5, 3.0, ((0, 64),))
    norm_gain = jnp.clip(1.0 + 0.15 * jax.random.normal(keys[6], (D,), jnp.float32), 0.25, 1.75).astype(jnp.bfloat16)
    route_ids_keys = jax.random.split(jax.random.fold_in(part_keys[7], 1), SPAN // TOK_DEV)
    route_ids_turns = jax.random.permutation(jax.random.fold_in(part_keys[7], 3), SPAN // TOK_DEV)
    route_ids = jax.vmap(lambda own, number: assign_block(jax.random.fold_in(part_keys[7], 2), own, number, TOK_DEV, EXPERTS, TOP, CAP, 2))(route_ids_keys, route_ids_turns).reshape((SPAN, TOP))
    route_weights = jnp.clip(0.1 + 0.5 * jax.random.uniform(part_keys[8], (SPAN, TOP), jnp.float32) ** shard_levels(part_keys[8], (SPAN, TOP), ((0, 64),), -0.2, 0.2), 0.1, 0.6)
    w_gate = bell_draw(keys[9], (EXPERTS, D, FF), D ** -0.5, 0.125, ((0, 64), (2, 4)))
    w_up = bell_draw(keys[10], (EXPERTS, D, FF), D ** -0.5, 0.125, ((0, 64), (2, 4)))
    w_down = bell_draw(keys[11], (EXPERTS, FF, D), FF ** -0.5, 0.15625, ((0, 64), (1, 4)))
    return dict(queries=queries, latent_cache=latent_cache, cache_len=cache_len, kv_up=kv_up, o_weight=o_weight, residual=residual, norm_gain=norm_gain, route_ids=route_ids, route_weights=route_weights, w_gate=w_gate, w_up=w_up, w_down=w_down)


epsilon = 1e-06

def shard_attention(absorbed, cache_rows, live_mask, up_value):
    scores = jnp.einsum('qhc,kc->qhk', absorbed.astype(jnp.float32), cache_rows.astype(jnp.float32)) * (NOPE + ROPE) ** (-0.5)
    scores = jnp.where(live_mask[None, None, :], scores, -jnp.inf)
    highest = lax.optimization_barrier(jnp.max(scores, axis=2))
    weights = jnp.exp(scores - highest[:, :, None]).astype(jnp.bfloat16)
    totals = lax.optimization_barrier(jnp.sum(weights.astype(jnp.float32), axis=2))
    latent_out = jnp.einsum('qhk,kl->qhl', weights.astype(jnp.float32), cache_rows[:, :LATENT].astype(jnp.float32)).astype(jnp.bfloat16)
    head_out = jnp.einsum('qhl,hvl->qhv', latent_out.astype(jnp.float32), up_value.astype(jnp.float32))
    return (highest, totals, head_out)

def reference(queries, latent_cache, cache_len, kv_up, o_weight, residual, norm_gain, route_ids, route_weights, w_gate, w_up, w_down):
    query_heads = queries.reshape(SPAN, HEADS, NOPE + ROPE)
    query_latent = jnp.einsum('qhn,hnl->qhl', query_heads[:, :, :NOPE].astype(jnp.float32), kv_up[:, :NOPE, :].astype(jnp.float32)).astype(jnp.bfloat16)
    absorbed = jnp.concatenate([query_latent, query_heads[:, :, NOPE:]], axis=2)
    up_value = kv_up[:, NOPE:, :]
    blocks = latent_cache.reshape(N_CTX, CACHE_DEV, LATENT + ROPE)
    positions = jnp.arange(CACHE_DEV, dtype=jnp.int32)

    def fold_shard(running, shard_item):
        highest, totals, summed = running
        cache_rows, length = shard_item
        shard_high, shard_total, shard_head = shard_attention(absorbed, cache_rows, positions < length, up_value)
        new_high = jnp.maximum(highest, shard_high)
        old_factor = jnp.exp(highest - new_high)
        new_factor = jnp.exp(shard_high - new_high)
        return ((new_high, totals * old_factor + shard_total * new_factor, summed * old_factor[:, :, None] + shard_head * new_factor[:, :, None]), None)
    initial = (jnp.full((SPAN, HEADS), -jnp.inf, jnp.float32), jnp.zeros((SPAN, HEADS), jnp.float32), jnp.zeros((SPAN, HEADS, VDIM), jnp.float32))
    (highest, totals, summed), unused = lax.scan(fold_shard, initial, (blocks, cache_len))
    attention = (summed / totals[:, :, None]).astype(jnp.bfloat16).reshape(SPAN, HEADS * VDIM)
    hidden = residual.astype(jnp.float32) + jnp.dot(attention, o_weight, preferred_element_type=jnp.float32)
    inverse_rms = lax.rsqrt(lax.optimization_barrier(jnp.mean(hidden * hidden, axis=1)) + epsilon)
    normed = (hidden * inverse_rms[:, None] * norm_gain.astype(jnp.float32)).astype(jnp.bfloat16)
    pair_count = TOK_DEV * TOP
    expert_ids = route_ids.reshape(N_CTX, pair_count)
    onehot = (expert_ids[:, :, None] == jnp.arange(EXPERTS, dtype=jnp.int32)[None, None, :]).astype(jnp.int32)
    earlier = jnp.cumsum(onehot, axis=1) - onehot
    slot_ids = lax.optimization_barrier(jnp.sum(earlier * onehot, axis=2))
    targets = (expert_ids * CAP + slot_ids).reshape(N_CTX, TOK_DEV, TOP)
    columns = jnp.arange(EXPERTS * CAP, dtype=jnp.int32)
    matches = targets[:, :, :, None] == columns[None, None, None, :]
    select = lax.optimization_barrier(jnp.sum(matches.astype(jnp.float32), axis=2))
    normed_blocks = normed.reshape(N_CTX, TOK_DEV, D)
    dispatched = jnp.einsum('ctj,ctd->cjd', select, normed_blocks.astype(jnp.float32)).astype(jnp.bfloat16)
    by_expert = dispatched.reshape(N_CTX, EXPERTS, CAP, D).transpose(1, 0, 2, 3).reshape(EXPERTS, N_CTX * CAP, D)

    def run_expert(operands):
        rows_in, gate_matrix, up_matrix, down_matrix = operands
        gate_act = jnp.dot(rows_in, gate_matrix, preferred_element_type=jnp.float32)
        up_act = jnp.dot(rows_in, up_matrix, preferred_element_type=jnp.float32)
        gated_rows = (jax.nn.silu(gate_act) * up_act).astype(jnp.bfloat16)
        return jnp.dot(gated_rows, down_matrix, preferred_element_type=jnp.float32).astype(jnp.bfloat16)
    expert_out = lax.map(run_expert, (by_expert, w_gate, w_up, w_down))
    back_rows = expert_out.reshape(EXPERTS, N_CTX, CAP, D).transpose(1, 0, 2, 3).reshape(N_CTX, EXPERTS * CAP, D)
    mixing = lax.optimization_barrier(jnp.sum(jnp.where(matches, route_weights.reshape(N_CTX, TOK_DEV, TOP)[:, :, :, None], 0.0), axis=2))
    routed = jnp.einsum('ctj,cjd->ctd', mixing, back_rows.astype(jnp.float32), precision=lax.Precision.HIGHEST)
    return (hidden + routed.reshape(SPAN, D)).astype(jnp.bfloat16)
```

```python
import jax
import jax.numpy as jnp
from jax import lax
from jax.experimental import pallas as pl
from jax.experimental.pallas import tpu as pltpu
from jax.sharding import Mesh
from jax.sharding import PartitionSpec as P

D = 2048
NOPE = 128
ROPE = 64
VDIM = 128
LATENT = 512
TOP = 6
CAP = 2
NEAR = 4
CTX = ("far", "near", "core")
GRP_CTX = ("grp", "far", "near", "core")
SEGMENT = ("near", "core")
Z = ("far", "near")
EXTRA = 128

epsilon = 1e-06


def thirds(x):
    high = x.astype(jnp.bfloat16)
    rest = x - high.astype(jnp.float32)
    middle = rest.astype(jnp.bfloat16)
    low = (rest - middle.astype(jnp.float32)).astype(jnp.bfloat16)
    return high.astype(jnp.float32), middle.astype(jnp.float32), low.astype(jnp.float32)


def log_block(logs, rows):
    lane = lax.broadcasted_iota(jnp.int32, (rows, EXTRA), 1)
    heads = len(logs)
    block = jnp.zeros((rows, EXTRA), jnp.float32)
    for h, x in enumerate(logs):
        for piece, part in enumerate(thirds(x)):
            block = jnp.where(lane == heads * piece + h, part, block)
    return block.astype(jnp.bfloat16)


def attention_kernel(core, length, mine, other, cache, out, heads):
    planes, _, _ = mine.shape
    rows = planes * 8
    keys = cache.shape[1]
    first = core[0] == 0
    live = lax.broadcasted_iota(jnp.int32, (1, keys), 1) < length[0]
    scale = (NOPE + ROPE) ** (-0.5)
    latents = cache[:LATENT, :]
    rotary = cache[LATENT:, :]
    per_row = 256 // NOPE
    q_rows = heads // per_row * 8
    kv_at = q_rows + 8
    logs, tops = [], []
    for h in range(heads):
        a = mine[:, kv_at + 8 * h : kv_at + 8 * h + 8, :]
        b = other[:, kv_at + 8 * h : kv_at + 8 * h + 8, :]
        up = jnp.stack([jnp.where(first, a, b), jnp.where(first, b, a)], axis=1)
        up = up.reshape(planes * 16, 256)
        at, lane = 8 * (h // per_row), NOPE * (h % per_row)
        nope = jnp.concatenate(
            [x[:, at : at + 8, lane : lane + NOPE].reshape(rows, NOPE) for x in (mine, other)], axis=0
        )
        rope = jnp.concatenate(
            [x[:, q_rows : q_rows + 8, ROPE * h : ROPE * h + ROPE].reshape(rows, ROPE) for x in (mine, other)],
            axis=0,
        )
        absorbed = lax.dot_general(
            nope, up[:, :NOPE], (((1,), (1,)), ((), ())), preferred_element_type=jnp.float32
        ).astype(jnp.bfloat16)
        scores = jnp.dot(absorbed, latents, preferred_element_type=jnp.float32)
        scores = (scores + jnp.dot(rope, rotary, preferred_element_type=jnp.float32)) * scale
        scores = jnp.where(live, scores, -jnp.inf)
        highest = jnp.max(scores, axis=1, keepdims=True)
        weights = jnp.exp(scores - highest).astype(jnp.bfloat16)
        total = jnp.sum(weights.astype(jnp.float32), axis=1, keepdims=True)
        mixed = lax.dot_general(
            weights, latents, (((1,), (1,)), ((), ())), preferred_element_type=jnp.float32
        ).astype(jnp.bfloat16)
        head = jnp.dot(mixed, up[:, NOPE:], preferred_element_type=jnp.float32)
        tops.append((head / total).astype(jnp.bfloat16))
        logs.append(highest + jnp.log(total))
    result = jnp.concatenate([*tops, log_block(logs, 2 * rows)], axis=1)
    result = result.reshape(2, planes, 8, result.shape[1])
    for z in range(planes):
        out[z % NEAR, pl.ds(core[0], 1), z // NEAR] = result[0, z][None]
        out[z % NEAR, pl.ds(1 - core[0], 1), z // NEAR] = result[1, z][None]


def merged(parts, heads):
    sources, rows, _ = parts.shape
    width = heads * VDIM
    lane = lax.broadcasted_iota(jnp.int32, (EXTRA, width), 0)
    col = lax.broadcasted_iota(jnp.int32, (EXTRA, width), 1)
    spread = ((lane < 3 * heads) & (lane % heads == col // VDIM)).astype(jnp.bfloat16)
    packed = parts[:, :, width:].reshape(sources * rows, EXTRA)
    logs = jnp.dot(packed, spread, preferred_element_type=jnp.float32).reshape(sources, rows, width)
    top = jnp.max(logs, axis=0)
    shares = jnp.exp(logs - top[None])
    total = jnp.sum(shares, axis=0)
    mixed = jnp.sum(shares * parts[:, :, :width].astype(jnp.float32), axis=0)
    return mixed / total, top + jnp.log(total)


def merge_kernel(parts, out, heads):
    mixed, logs = merged(parts[...], heads)
    rows = mixed.shape[0]
    block = log_block([logs[:, VDIM * h : VDIM * h + EXTRA] for h in range(heads)], rows)
    out[...] = jnp.concatenate([mixed.astype(jnp.bfloat16), block], axis=1)


def project_kernel(parts, weight, out, heads):
    mixed, _ = merged(parts[...], heads)
    out[...] = lax.dot_general(
        mixed.astype(jnp.bfloat16), weight[...], (((1,), (1,)), ((), ())), preferred_element_type=jnp.float32
    ).astype(jnp.bfloat16)


def gathered(packed):
    near = lax.all_gather(packed, Z, axis=0, tiled=False)
    far = lax.ppermute(near, "core", [(0, 1), (1, 0)])
    return near, far


def body(
    queries,
    latent_cache,
    cache_len,
    kv_up,
    o_weight,
    residual,
    norm_gain,
    route_ids,
    route_weights,
    w_gate,
    w_up,
    w_down,
):
    ctx_count = lax.axis_size(CTX)
    sub_count = lax.axis_size("sub")
    heads = kv_up.shape[0]
    tokens = queries.shape[0]
    width = heads * VDIM + EXTRA
    planes = ctx_count // 2

    split = queries.reshape(tokens, heads, NOPE + ROPE)
    nope = split[:, :, :NOPE].reshape(tokens, heads * NOPE // 256, 256).transpose(1, 0, 2)
    rope = split[:, :, NOPE:].reshape(tokens, heads * ROPE // 256, 256).transpose(1, 0, 2)
    ups = kv_up.transpose(0, 2, 1)
    packed = jnp.concatenate(
        [nope.reshape(-1, 256), rope.reshape(-1, 256), ups.reshape(-1, 256)], axis=0
    )
    mine, other = gathered(packed)
    o_full = lax.all_gather(o_weight, CTX, axis=1, tiled=True)

    smem = pl.BlockSpec(memory_space=pltpu.SMEM)
    vmem = pl.BlockSpec(memory_space=pltpu.VMEM)
    partial = pl.pallas_call(
        lambda *refs: attention_kernel(*refs, heads),
        out_shape=jax.ShapeDtypeStruct((NEAR, 2, planes // NEAR, tokens, width), jnp.bfloat16),
        in_specs=[smem, smem, vmem, vmem, vmem],
        out_specs=vmem,
        name="attention",
    )(lax.axis_index("core").reshape(1), cache_len, mine, other, latent_cache.T)
    segment = NEAR * 2
    rows = ctx_count // segment * tokens
    partial = lax.all_to_all(partial.reshape(segment, rows, width), SEGMENT, 0, 0, tiled=True)
    partial = pl.pallas_call(
        lambda *refs: merge_kernel(*refs, heads),
        out_shape=jax.ShapeDtypeStruct((rows, width), jnp.bfloat16),
        in_specs=[vmem],
        out_specs=vmem,
        name="merge",
    )(partial)
    partial = lax.all_to_all(partial.reshape(ctx_count // segment, tokens, width), "far", 0, 0, tiled=True)
    projected = pl.pallas_call(
        lambda *refs: project_kernel(*refs, heads),
        out_shape=jax.ShapeDtypeStruct((tokens, D), jnp.bfloat16),
        in_specs=[vmem, vmem],
        out_specs=vmem,
        name="project",
    )(partial, o_full.T)

    shares = lax.all_to_all(
        jnp.broadcast_to(projected[None], (sub_count, tokens, D)), "sub", 0, 0, tiled=True
    )
    hidden = residual.astype(jnp.float32) + shares.astype(jnp.float32).sum(axis=0)
    inverse_rms = lax.rsqrt(jnp.mean(hidden * hidden, axis=1) + epsilon)
    normed = (hidden * inverse_rms[:, None] * norm_gain.astype(jnp.float32)).astype(jnp.bfloat16)
    quarter = D // sub_count
    offset = lax.axis_index("sub") * quarter
    hidden_part = lax.dynamic_slice_in_dim(hidden, offset, quarter, 1)
    normed_part = lax.dynamic_slice_in_dim(normed, offset, quarter, 1)

    experts = w_gate.shape[0]
    expert_total = experts * ctx_count
    pairs = tokens * TOP
    expert_ids = route_ids.reshape(pairs)
    onehot = (expert_ids[:, None] == lax.broadcasted_iota(jnp.int32, (1, expert_total), 1)).astype(jnp.int32)
    earlier = jnp.cumsum(onehot, axis=0) - onehot
    slot_ids = jnp.sum(earlier * onehot, axis=1)
    targets = (expert_ids * CAP + slot_ids).reshape(tokens, TOP)
    matches = targets[:, :, None] == lax.broadcasted_iota(jnp.int32, (1, 1, expert_total * CAP), 2)
    select = jnp.sum(matches.astype(jnp.int32), axis=1).astype(jnp.bfloat16)
    outgoing = jnp.einsum("tj,td->jd", select, normed_part, preferred_element_type=jnp.float32).astype(
        jnp.bfloat16
    )
    outgoing = outgoing.reshape(ctx_count, experts * CAP, quarter)
    received = lax.all_to_all(outgoing, CTX, split_axis=0, concat_axis=0, tiled=True)
    received = received.reshape(ctx_count * experts * CAP, quarter)
    received = lax.all_gather(received, "sub", axis=1, tiled=True)
    received = received.reshape(ctx_count, experts, CAP, D)
    gate_act = jnp.einsum("sekd,edf->sekf", received, w_gate, preferred_element_type=jnp.float32)
    up_act = jnp.einsum("sekd,edf->sekf", received, w_up, preferred_element_type=jnp.float32)
    gated_rows = (jax.nn.silu(gate_act) * up_act).astype(jnp.bfloat16)
    partial_out = jnp.einsum("sekf,efd->sekd", gated_rows, w_down, preferred_element_type=jnp.float32)
    partial_out = partial_out.astype(jnp.bfloat16).reshape(ctx_count * experts * CAP, sub_count, quarter)
    parts = lax.all_to_all(partial_out.transpose(1, 0, 2), "sub", 0, 0, tiled=True)
    summed = jnp.sum(parts.astype(jnp.float32), axis=0).astype(jnp.bfloat16)
    summed = summed.reshape(ctx_count, experts * CAP, quarter)
    back_rows = lax.all_to_all(summed, CTX, split_axis=0, concat_axis=0, tiled=True)
    back_rows = back_rows.reshape(expert_total * CAP, quarter)
    mixing = jnp.sum(jnp.where(matches, route_weights[:, :, None], 0.0), axis=1)
    routed = jnp.dot(mixing, back_rows.astype(jnp.float32))
    return (hidden_part + routed).astype(jnp.bfloat16)


def solution(mesh):
    planes = mesh.shape["ctx"] // 2
    split = Mesh(
        mesh.devices.reshape(mesh.shape["grp"], planes // NEAR, NEAR, 2, mesh.shape["sub"]),
        ("grp", "far", "near", "core", "sub"),
    )
    return jax.shard_map(
        body,
        mesh=split,
        in_specs=(
            P(GRP_CTX, "sub"),
            P(GRP_CTX, None),
            P(GRP_CTX),
            P(("grp", "sub"), None, CTX),
            P("sub", CTX),
            P(GRP_CTX, None),
            P(),
            P(GRP_CTX, None),
            P(GRP_CTX, None),
            P(CTX, None, "sub"),
            P(CTX, None, "sub"),
            P(CTX, "sub", None),
        ),
        out_specs=P(GRP_CTX, "sub"),
        check_vma=False,
    )
```

```python
import jax
import jax.numpy as jnp
from jax import lax
from jax.experimental import pallas as pl
from jax.experimental.pallas import tpu as pltpu
from jax.sharding import Mesh
from jax.sharding import PartitionSpec as P

D = 2048
NOPE = 128
ROPE = 64
VDIM = 128
LATENT = 512
TOP = 6
CAP = 2
NEAR = 4
CTX = ("far", "near", "core")
GRP_CTX = ("grp", "far", "near", "core")
SEGMENT = ("near", "core")
Z = ("far", "near")
EXTRA = 128

epsilon = 1e-06


def thirds(x):
    high = x.astype(jnp.bfloat16)
    rest = x - high.astype(jnp.float32)
    middle = rest.astype(jnp.bfloat16)
    low = (rest - middle.astype(jnp.float32)).astype(jnp.bfloat16)
    return high.astype(jnp.float32), middle.astype(jnp.float32), low.astype(jnp.float32)


def log_block(logs, rows):
    lane = lax.broadcasted_iota(jnp.int32, (rows, EXTRA), 1)
    heads = len(logs)
    block = jnp.zeros((rows, EXTRA), jnp.float32)
    for h, x in enumerate(logs):
        for piece, part in enumerate(thirds(x)):
            block = jnp.where(lane == heads * piece + h, part, block)
    return block.astype(jnp.bfloat16)


def attention_kernel(core, length, mine, other, cache, out, heads):
    planes, _, _ = mine.shape
    rows = planes * 8
    keys = cache.shape[1]
    first = core[0] == 0
    live = lax.broadcasted_iota(jnp.int32, (1, keys), 1) < length[0]
    scale = (NOPE + ROPE) ** (-0.5)
    latents = cache[:LATENT, :]
    rotary = cache[LATENT:, :]
    per_row = 256 // NOPE
    q_rows = heads // per_row * 8
    kv_at = q_rows + 8
    logs, tops = [], []
    for h in range(heads):
        a = mine[:, kv_at + 8 * h : kv_at + 8 * h + 8, :]
        b = other[:, kv_at + 8 * h : kv_at + 8 * h + 8, :]
        up = jnp.stack([jnp.where(first, a, b), jnp.where(first, b, a)], axis=1)
        up = up.reshape(planes * 16, 256)
        at, lane = 8 * (h // per_row), NOPE * (h % per_row)
        nope = jnp.concatenate(
            [x[:, at : at + 8, lane : lane + NOPE].reshape(rows, NOPE) for x in (mine, other)], axis=0
        )
        rope = jnp.concatenate(
            [x[:, q_rows : q_rows + 8, ROPE * h : ROPE * h + ROPE].reshape(rows, ROPE) for x in (mine, other)],
            axis=0,
        )
        absorbed = lax.dot_general(
            nope, up[:, :NOPE], (((1,), (1,)), ((), ())), preferred_element_type=jnp.float32
        ).astype(jnp.bfloat16)
        scores = jnp.dot(absorbed, latents, preferred_element_type=jnp.float32)
        scores = (scores + jnp.dot(rope, rotary, preferred_element_type=jnp.float32)) * scale
        scores = jnp.where(live, scores, -jnp.inf)
        highest = jnp.max(scores, axis=1, keepdims=True)
        weights = jnp.exp(scores - highest).astype(jnp.bfloat16)
        total = jnp.sum(weights.astype(jnp.float32), axis=1, keepdims=True)
        mixed = lax.dot_general(
            weights, latents, (((1,), (1,)), ((), ())), preferred_element_type=jnp.float32
        ).astype(jnp.bfloat16)
        head = jnp.dot(mixed, up[:, NOPE:], preferred_element_type=jnp.float32)
        tops.append((head / total).astype(jnp.bfloat16))
        logs.append(highest + jnp.log(total))
    result = jnp.concatenate([*tops, log_block(logs, 2 * rows)], axis=1)
    result = result.reshape(2, planes, 8, result.shape[1])
    for z in range(planes):
        out[z % NEAR, pl.ds(core[0], 1), z // NEAR] = result[0, z][None]
        out[z % NEAR, pl.ds(1 - core[0], 1), z // NEAR] = result[1, z][None]


def merged(parts, heads):
    sources, rows, _ = parts.shape
    width = heads * VDIM
    lane = lax.broadcasted_iota(jnp.int32, (EXTRA, width), 0)
    col = lax.broadcasted_iota(jnp.int32, (EXTRA, width), 1)
    spread = ((lane < 3 * heads) & (lane % heads == col // VDIM)).astype(jnp.bfloat16)
    packed = parts[:, :, width:].reshape(sources * rows, EXTRA)
    logs = jnp.dot(packed, spread, preferred_element_type=jnp.float32).reshape(sources, rows, width)
    top = jnp.max(logs, axis=0)
    shares = jnp.exp(logs - top[None])
    total = jnp.sum(shares, axis=0)
    mixed = jnp.sum(shares * parts[:, :, :width].astype(jnp.float32), axis=0)
    return mixed / total, top + jnp.log(total)


def merge_kernel(parts, out, heads):
    mixed, logs = merged(parts[...], heads)
    rows = mixed.shape[0]
    block = log_block([logs[:, VDIM * h : VDIM * h + EXTRA] for h in range(heads)], rows)
    out[...] = jnp.concatenate([mixed.astype(jnp.bfloat16), block], axis=1)


def project_kernel(parts, weight, out, heads):
    mixed, _ = merged(parts[...], heads)
    out[...] = lax.dot_general(
        mixed.astype(jnp.bfloat16), weight[...], (((1,), (1,)), ((), ())), preferred_element_type=jnp.float32
    ).astype(jnp.bfloat16)


def gathered(packed):
    near = lax.all_gather(packed, Z, axis=0, tiled=False)
    far = lax.ppermute(near, "core", [(0, 1), (1, 0)])
    return near, far


def body(
    queries,
    latent_cache,
    cache_len,
    kv_up,
    o_weight,
    residual,
    norm_gain,
    route_ids,
    route_weights,
    w_gate,
    w_up,
    w_down,
):
    ctx_count = lax.axis_size(CTX)
    sub_count = lax.axis_size("sub")
    heads = kv_up.shape[0]
    tokens = queries.shape[0]
    width = heads * VDIM + EXTRA
    planes = ctx_count // 2

    split = queries.reshape(tokens, heads, NOPE + ROPE)
    nope = split[:, :, :NOPE].reshape(tokens, heads * NOPE // 256, 256).transpose(1, 0, 2)
    rope = split[:, :, NOPE:].reshape(tokens, heads * ROPE // 256, 256).transpose(1, 0, 2)
    ups = kv_up.transpose(0, 2, 1)
    packed = jnp.concatenate(
        [nope.reshape(-1, 256), rope.reshape(-1, 256), ups.reshape(-1, 256)], axis=0
    )
    mine, other = gathered(packed)
    o_full = lax.all_gather(o_weight, CTX, axis=1, tiled=True)

    smem = pl.BlockSpec(memory_space=pltpu.SMEM)
    vmem = pl.BlockSpec(memory_space=pltpu.VMEM)
    partial = pl.pallas_call(
        lambda *refs: attention_kernel(*refs, heads),
        out_shape=jax.ShapeDtypeStruct((NEAR, 2, planes // NEAR, tokens, width), jnp.bfloat16),
        in_specs=[smem, smem, vmem, vmem, vmem],
        out_specs=vmem,
        compiler_params=pltpu.CompilerParams(vmem_limit_bytes=24 * 2**20),
        name="attention",
    )(lax.axis_index("core").reshape(1), cache_len, mine, other, latent_cache.T)
    segment = NEAR * 2
    rows = ctx_count // segment * tokens
    partial = lax.all_to_all(partial.reshape(segment, rows, width), SEGMENT, 0, 0, tiled=True)
    partial = pl.pallas_call(
        lambda *refs: merge_kernel(*refs, heads),
        out_shape=jax.ShapeDtypeStruct((rows, width), jnp.bfloat16),
        in_specs=[vmem],
        out_specs=vmem,
        compiler_params=pltpu.CompilerParams(vmem_limit_bytes=12 * 2**20),
        name="merge",
    )(partial)
    partial = lax.all_to_all(partial.reshape(ctx_count // segment, tokens, width), "far", 0, 0, tiled=True)
    projected = pl.pallas_call(
        lambda *refs: project_kernel(*refs, heads),
        out_shape=jax.ShapeDtypeStruct((tokens, D), jnp.bfloat16),
        in_specs=[vmem, vmem],
        out_specs=vmem,
        compiler_params=pltpu.CompilerParams(vmem_limit_bytes=12 * 2**20),
        name="project",
    )(partial, o_full.T)

    shares = lax.all_to_all(
        jnp.broadcast_to(projected[None], (sub_count, tokens, D)), "sub", 0, 0, tiled=True
    )
    hidden = residual.astype(jnp.float32) + shares.astype(jnp.float32).sum(axis=0)
    inverse_rms = lax.rsqrt(jnp.mean(hidden * hidden, axis=1) + epsilon)
    normed = (hidden * inverse_rms[:, None] * norm_gain.astype(jnp.float32)).astype(jnp.bfloat16)
    quarter = D // sub_count
    offset = lax.axis_index("sub") * quarter
    hidden_part = lax.dynamic_slice_in_dim(hidden, offset, quarter, 1)
    normed_part = lax.dynamic_slice_in_dim(normed, offset, quarter, 1)

    experts = w_gate.shape[0]
    expert_total = experts * ctx_count
    pairs = tokens * TOP
    expert_ids = route_ids.reshape(pairs)
    onehot = (expert_ids[:, None] == lax.broadcasted_iota(jnp.int32, (1, expert_total), 1)).astype(jnp.int32)
    earlier = jnp.cumsum(onehot, axis=0) - onehot
    slot_ids = jnp.sum(earlier * onehot, axis=1)
    targets = (expert_ids * CAP + slot_ids).reshape(tokens, TOP)
    matches = targets[:, :, None] == lax.broadcasted_iota(jnp.int32, (1, 1, expert_total * CAP), 2)
    select = jnp.sum(matches.astype(jnp.int32), axis=1).astype(jnp.bfloat16)
    outgoing = jnp.einsum("tj,td->jd", select, normed_part, preferred_element_type=jnp.float32).astype(
        jnp.bfloat16
    )
    outgoing = outgoing.reshape(ctx_count, experts * CAP, quarter)
    received = lax.all_to_all(outgoing, CTX, split_axis=0, concat_axis=0, tiled=True)
    received = received.reshape(ctx_count * experts * CAP, quarter)
    received = lax.all_gather(received, "sub", axis=1, tiled=True)
    received = received.reshape(ctx_count, experts, CAP, D)
    gate_act = jnp.einsum("sekd,edf->sekf", received, w_gate, preferred_element_type=jnp.float32)
    up_act = jnp.einsum("sekd,edf->sekf", received, w_up, preferred_element_type=jnp.float32)
    gated_rows = (jax.nn.silu(gate_act) * up_act).astype(jnp.bfloat16)
    partial_out = jnp.einsum("sekf,efd->sekd", gated_rows, w_down, preferred_element_type=jnp.float32)
    partial_out = partial_out.astype(jnp.bfloat16).reshape(ctx_count * experts * CAP, sub_count, quarter)
    parts = lax.all_to_all(partial_out.transpose(1, 0, 2), "sub", 0, 0, tiled=True)
    summed = jnp.sum(parts.astype(jnp.float32), axis=0).astype(jnp.bfloat16)
    summed = summed.reshape(ctx_count, experts * CAP, quarter)
    back_rows = lax.all_to_all(summed, CTX, split_axis=0, concat_axis=0, tiled=True)
    back_rows = back_rows.reshape(expert_total * CAP, quarter)
    mixing = jnp.sum(jnp.where(matches, route_weights[:, :, None], 0.0), axis=1)
    routed = jnp.dot(mixing, back_rows.astype(jnp.float32))
    return (hidden_part + routed).astype(jnp.bfloat16)


def solution(mesh):
    planes = mesh.shape["ctx"] // 2
    split = Mesh(
        mesh.devices.reshape(mesh.shape["grp"], planes // NEAR, NEAR, 2, mesh.shape["sub"]),
        ("grp", "far", "near", "core", "sub"),
    )
    return jax.shard_map(
        body,
        mesh=split,
        in_specs=(
            P(GRP_CTX, "sub"),
            P(GRP_CTX, None),
            P(GRP_CTX),
            P(("grp", "sub"), None, CTX),
            P("sub", CTX),
            P(GRP_CTX, None),
            P(),
            P(GRP_CTX, None),
            P(GRP_CTX, None),
            P(CTX, None, "sub"),
            P(CTX, None, "sub"),
            P(CTX, "sub", None),
        ),
        out_specs=P(GRP_CTX, "sub"),
        check_vma=False,
    )
```

```python
import jax
import jax.numpy as jnp
from jax import lax
from jax.experimental import pallas as pl
from jax.experimental.pallas import tpu as pltpu
from jax.sharding import Mesh
from jax.sharding import PartitionSpec as P

D = 2048
NOPE = 128
ROPE = 64
VDIM = 128
LATENT = 512
TOP = 6
CAP = 2
NEAR = 4
CTX = ("far", "near", "core")
GRP_CTX = ("grp", "far", "near", "core")
SEGMENT = ("near", "core")
Z = ("far", "near")
EXTRA = 128

epsilon = 1e-06


def thirds(x):
    high = x.astype(jnp.bfloat16)
    rest = x - high.astype(jnp.float32)
    middle = rest.astype(jnp.bfloat16)
    low = (rest - middle.astype(jnp.float32)).astype(jnp.bfloat16)
    return high.astype(jnp.float32), middle.astype(jnp.float32), low.astype(jnp.float32)


def log_block(logs, rows):
    lane = lax.broadcasted_iota(jnp.int32, (rows, EXTRA), 1)
    heads = len(logs)
    block = jnp.zeros((rows, EXTRA), jnp.float32)
    for h, x in enumerate(logs):
        for piece, part in enumerate(thirds(x)):
            block = jnp.where(lane == heads * piece + h, part, block)
    return block.astype(jnp.bfloat16)


def attention_kernel(core, length, mine, other, cache, out, heads):
    planes, _, _ = mine.shape
    rows = planes * 8
    keys = cache.shape[1]
    first = core[0] == 0
    live = lax.broadcasted_iota(jnp.int32, (1, keys), 1) < length[0]
    scale = (NOPE + ROPE) ** (-0.5)
    latents = cache[:LATENT, :]
    rotary = cache[LATENT:, :]
    per_row = 256 // NOPE
    q_rows = heads // per_row * 8
    kv_at = q_rows + 8
    logs, tops = [], []
    for h in range(heads):
        a = mine[:, kv_at + 8 * h : kv_at + 8 * h + 8, :]
        b = other[:, kv_at + 8 * h : kv_at + 8 * h + 8, :]
        up = jnp.stack([jnp.where(first, a, b), jnp.where(first, b, a)], axis=1)
        up = up.reshape(planes * 16, 256)
        at, lane = 8 * (h // per_row), NOPE * (h % per_row)
        nope = jnp.concatenate(
            [x[:, at : at + 8, lane : lane + NOPE].reshape(rows, NOPE) for x in (mine, other)], axis=0
        )
        rope = jnp.concatenate(
            [x[:, q_rows : q_rows + 8, ROPE * h : ROPE * h + ROPE].reshape(rows, ROPE) for x in (mine, other)],
            axis=0,
        )
        absorbed = lax.dot_general(
            nope, up[:, :NOPE], (((1,), (1,)), ((), ())), preferred_element_type=jnp.float32
        ).astype(jnp.bfloat16)
        scores = jnp.dot(absorbed, latents, preferred_element_type=jnp.float32)
        scores = (scores + jnp.dot(rope, rotary, preferred_element_type=jnp.float32)) * scale
        scores = jnp.where(live, scores, -jnp.inf)
        highest = jnp.max(scores, axis=1, keepdims=True)
        weights = jnp.exp(scores - highest).astype(jnp.bfloat16)
        total = jnp.sum(weights.astype(jnp.float32), axis=1, keepdims=True)
        mixed = lax.dot_general(
            weights, latents, (((1,), (1,)), ((), ())), preferred_element_type=jnp.float32
        ).astype(jnp.bfloat16)
        head = jnp.dot(mixed, up[:, NOPE:], preferred_element_type=jnp.float32)
        tops.append((head / total).astype(jnp.bfloat16))
        logs.append(highest + jnp.log(total))
    result = jnp.concatenate([*tops, log_block(logs, 2 * rows)], axis=1)
    result = result.reshape(2, planes, 8, result.shape[1])
    for z in range(planes):
        out[z % NEAR, pl.ds(core[0], 1), z // NEAR] = result[0, z][None]
        out[z % NEAR, pl.ds(1 - core[0], 1), z // NEAR] = result[1, z][None]


def merged(parts, heads):
    sources, rows, _ = parts.shape
    width = heads * VDIM
    lane = lax.broadcasted_iota(jnp.int32, (EXTRA, width), 0)
    col = lax.broadcasted_iota(jnp.int32, (EXTRA, width), 1)
    spread = ((lane < 3 * heads) & (lane % heads == col // VDIM)).astype(jnp.bfloat16)
    packed = parts[:, :, width:].reshape(sources * rows, EXTRA)
    logs = jnp.dot(packed, spread, preferred_element_type=jnp.float32).reshape(sources, rows, width)
    top = jnp.max(logs, axis=0)
    shares = jnp.exp(logs - top[None])
    total = jnp.sum(shares, axis=0)
    mixed = jnp.sum(shares * parts[:, :, :width].astype(jnp.float32), axis=0)
    return mixed / total, top + jnp.log(total)


def merge_kernel(parts, out, heads):
    mixed, logs = merged(parts[...], heads)
    rows = mixed.shape[0]
    block = log_block([logs[:, VDIM * h : VDIM * h + EXTRA] for h in range(heads)], rows)
    out[...] = jnp.concatenate([mixed.astype(jnp.bfloat16), block], axis=1)


def project_kernel(parts, weight, out, heads):
    mixed, _ = merged(parts[...], heads)
    projected = lax.dot_general(
        mixed.astype(jnp.bfloat16), weight[...], (((1,), (1,)), ((), ())), preferred_element_type=jnp.float32
    ).astype(jnp.bfloat16)
    for s in range(out.shape[0]):
        out[s] = projected


def named_by(ids, expert):
    found = jnp.zeros((ids.shape[0], expert.shape[1]), jnp.float32)
    for k in range(TOP):
        found = jnp.where(ids[:, k : k + 1] == expert, 1.0, found)
    return found


def earlier_rows(named, tokens):
    rows = named.shape[0]
    r = lax.broadcasted_iota(jnp.int32, (rows, rows), 0)
    c = lax.broadcasted_iota(jnp.int32, (rows, rows), 1)
    before = ((r // tokens == c // tokens) & (c < r)).astype(jnp.bfloat16)
    return jnp.dot(before, named.astype(jnp.bfloat16), preferred_element_type=jnp.float32)


def norm_kernel(sub, shares, residual, gain, ids, out, hidden_part):
    tokens = residual.shape[0]
    quarter = hidden_part.shape[1]
    hidden = residual[...].astype(jnp.float32) + jnp.sum(shares[...].astype(jnp.float32), axis=0)
    inverse_rms = lax.rsqrt(jnp.mean(hidden * hidden, axis=1, keepdims=True) + epsilon)
    own = pl.ds(pl.multiple_of(sub[0] * quarter, quarter), quarter)
    part = residual[:, own].astype(jnp.float32) + jnp.sum(shares[:, :, own].astype(jnp.float32), axis=0)
    hidden_part[...] = part
    normed = (part * inverse_rms * gain[:, own].astype(jnp.float32)).astype(jnp.bfloat16)
    lane = lax.broadcasted_iota(jnp.int32, (tokens, EXTRA), 1)
    named = jnp.zeros((tokens, EXTRA), jnp.float32)
    for k in range(TOP):
        named = jnp.where(lane == k, ids[:, k : k + 1].astype(jnp.float32), named)
    block = jnp.concatenate([normed, named.astype(jnp.bfloat16)], axis=1)
    for f in range(out.shape[0]):
        out[f] = block


def route_kernel(far, blocks, out):
    sources, tokens, width = blocks.shape
    segment, slots, quarter = out.shape
    rows = sources * tokens
    ids = blocks[:, :, quarter:].astype(jnp.float32).reshape(rows, width - quarter)
    col = lax.broadcasted_iota(jnp.int32, (1, segment * slots), 1)
    expert = (far[0] * segment + col // slots).astype(jnp.float32)
    named = named_by(ids, expert)
    row = lax.broadcasted_iota(jnp.int32, (rows, segment * slots), 0)
    lane = lax.broadcasted_iota(jnp.int32, (rows, segment * slots), 1)
    right = (lane // CAP % sources == row // tokens) & (
        earlier_rows(named, tokens) == (lane % CAP).astype(jnp.float32)
    )
    chosen = jnp.where(right, named, 0.0)
    taken = lax.dot_general(
        chosen,
        blocks[:, :, :quarter].astype(jnp.float32).reshape(rows, quarter),
        (((0,), (0,)), ((), ())),
        preferred_element_type=jnp.float32,
    )
    out[...] = taken.reshape(segment, slots, quarter).astype(jnp.bfloat16)


def expert_kernel(received, gate, up, down, out):
    subs, _, quarter = received.shape
    side = (((1,), (1,)), ((), ()))
    gate_act, up_act = 0.0, 0.0
    for s in range(subs):
        rows = received[s]
        cols = slice(s * quarter, (s + 1) * quarter)
        gate_act += lax.dot_general(rows, gate[:, cols], side, preferred_element_type=jnp.float32)
        up_act += lax.dot_general(rows, up[:, cols], side, preferred_element_type=jnp.float32)
    gated = (gate_act / (1.0 + jnp.exp(-gate_act)) * up_act).astype(jnp.bfloat16)
    for s in range(subs):
        cols = slice(s * quarter, (s + 1) * quarter)
        out[s] = jnp.dot(gated, down[:, cols], preferred_element_type=jnp.float32).astype(jnp.bfloat16)


def final_kernel(hidden_part, back, ids, weights, out, segment):
    tokens = ids.shape[0]
    slots = back.shape[0]
    fars = slots // (segment * CAP)
    col = lax.broadcasted_iota(jnp.int32, (1, slots), 1)
    expert = col // CAP % fars * segment + col // (CAP * fars)
    named = named_by(ids[...], expert)
    share = jnp.zeros((tokens, slots), jnp.float32)
    for k in range(TOP):
        share = jnp.where(ids[:, k : k + 1] == expert, weights[:, k : k + 1], share)
    lane = lax.broadcasted_iota(jnp.int32, (tokens, slots), 1)
    share = jnp.where(earlier_rows(named, tokens) == (lane % CAP).astype(jnp.float32), share, 0.0)
    routed = jnp.dot(share.astype(jnp.bfloat16), back[...], preferred_element_type=jnp.float32)
    out[...] = (hidden_part[...] + routed).astype(jnp.bfloat16)


def gathered(packed):
    near = lax.all_gather(packed, Z, axis=0, tiled=False)
    far = lax.ppermute(near, "core", [(0, 1), (1, 0)])
    return near, far


def body(
    queries,
    latent_cache,
    cache_len,
    kv_up,
    o_weight,
    residual,
    norm_gain,
    route_ids,
    route_weights,
    w_gate,
    w_up,
    w_down,
):
    ctx_count = lax.axis_size(CTX)
    sub_count = lax.axis_size("sub")
    heads = kv_up.shape[0]
    tokens = queries.shape[0]
    width = heads * VDIM + EXTRA
    planes = ctx_count // 2

    split = queries.reshape(tokens, heads, NOPE + ROPE)
    nope = split[:, :, :NOPE].reshape(tokens, heads * NOPE // 256, 256).transpose(1, 0, 2)
    rope = split[:, :, NOPE:].reshape(tokens, heads * ROPE // 256, 256).transpose(1, 0, 2)
    ups = kv_up.transpose(0, 2, 1)
    packed = jnp.concatenate(
        [nope.reshape(-1, 256), rope.reshape(-1, 256), ups.reshape(-1, 256)], axis=0
    )
    mine, other = gathered(packed)
    o_full = lax.all_gather(o_weight, CTX, axis=1, tiled=True)

    smem = pl.BlockSpec(memory_space=pltpu.SMEM)
    vmem = pl.BlockSpec(memory_space=pltpu.VMEM)
    partial = pl.pallas_call(
        lambda *refs: attention_kernel(*refs, heads),
        out_shape=jax.ShapeDtypeStruct((NEAR, 2, planes // NEAR, tokens, width), jnp.bfloat16),
        in_specs=[smem, smem, vmem, vmem, vmem],
        out_specs=vmem,
        compiler_params=pltpu.CompilerParams(vmem_limit_bytes=24 * 2**20),
        name="attention",
    )(lax.axis_index("core").reshape(1), cache_len, mine, other, latent_cache.T)
    segment = NEAR * 2
    rows = ctx_count // segment * tokens
    partial = lax.all_to_all(partial.reshape(segment, rows, width), SEGMENT, 0, 0, tiled=True)
    partial = pl.pallas_call(
        lambda *refs: merge_kernel(*refs, heads),
        out_shape=jax.ShapeDtypeStruct((rows, width), jnp.bfloat16),
        in_specs=[vmem],
        out_specs=vmem,
        compiler_params=pltpu.CompilerParams(vmem_limit_bytes=12 * 2**20),
        name="merge",
    )(partial)
    partial = lax.all_to_all(partial.reshape(ctx_count // segment, tokens, width), "far", 0, 0, tiled=True)
    projected = pl.pallas_call(
        lambda *refs: project_kernel(*refs, heads),
        out_shape=jax.ShapeDtypeStruct((sub_count, tokens, D), jnp.bfloat16),
        in_specs=[vmem, vmem],
        out_specs=vmem,
        compiler_params=pltpu.CompilerParams(vmem_limit_bytes=12 * 2**20),
        name="project",
    )(partial, o_full.T)

    shares = lax.all_to_all(projected, "sub", 0, 0, tiled=True)
    quarter = D // sub_count
    fars = ctx_count // segment
    blocks, hidden_part = pl.pallas_call(
        norm_kernel,
        out_shape=(
            jax.ShapeDtypeStruct((fars, tokens, quarter + EXTRA), jnp.bfloat16),
            jax.ShapeDtypeStruct((tokens, quarter), jnp.float32),
        ),
        in_specs=[smem, vmem, vmem, vmem, vmem],
        out_specs=(vmem, vmem),
        compiler_params=pltpu.CompilerParams(vmem_limit_bytes=8 * 2**20),
        name="norm",
    )(lax.axis_index("sub").reshape(1), shares, residual, norm_gain.reshape(1, D), route_ids)
    blocks = lax.all_to_all(blocks, "far", 0, 0, tiled=True)
    rows = fars * CAP
    outgoing = pl.pallas_call(
        route_kernel,
        out_shape=jax.ShapeDtypeStruct((segment, rows, quarter), jnp.bfloat16),
        in_specs=[smem, vmem],
        out_specs=vmem,
        compiler_params=pltpu.CompilerParams(vmem_limit_bytes=8 * 2**20),
        name="route",
    )(lax.axis_index("far").reshape(1), blocks)
    received = lax.all_to_all(outgoing, SEGMENT, 0, 0, tiled=True).reshape(segment * rows, quarter)
    received = lax.all_gather(received, "sub", axis=0, tiled=False)
    partial_out = pl.pallas_call(
        expert_kernel,
        out_shape=jax.ShapeDtypeStruct((sub_count, segment * rows, quarter), jnp.bfloat16),
        in_specs=[vmem] * 4,
        out_specs=vmem,
        compiler_params=pltpu.CompilerParams(vmem_limit_bytes=16 * 2**20),
        name="experts",
    )(received, w_gate[0].T, w_up[0].T, w_down[0])
    parts = lax.all_to_all(partial_out, "sub", 0, 0, tiled=True)
    summed = jnp.sum(parts.astype(jnp.float32), axis=0).astype(jnp.bfloat16)
    summed = summed.reshape(ctx_count, CAP, quarter)
    back = lax.all_to_all(summed, (*SEGMENT, "far"), 0, 0, tiled=True)
    return pl.pallas_call(
        lambda *refs: final_kernel(*refs, segment),
        out_shape=jax.ShapeDtypeStruct((tokens, quarter), jnp.bfloat16),
        in_specs=[vmem] * 4,
        out_specs=vmem,
        compiler_params=pltpu.CompilerParams(vmem_limit_bytes=8 * 2**20),
        name="final",
    )(hidden_part, back.reshape(ctx_count * CAP, quarter), route_ids, route_weights)


def solution(mesh):
    planes = mesh.shape["ctx"] // 2
    split = Mesh(
        mesh.devices.reshape(mesh.shape["grp"], planes // NEAR, NEAR, 2, mesh.shape["sub"]),
        ("grp", "far", "near", "core", "sub"),
    )
    return jax.shard_map(
        body,
        mesh=split,
        in_specs=(
            P(GRP_CTX, "sub"),
            P(GRP_CTX, None),
            P(GRP_CTX),
            P(("grp", "sub"), None, CTX),
            P("sub", CTX),
            P(GRP_CTX, None),
            P(),
            P(GRP_CTX, None),
            P(GRP_CTX, None),
            P(CTX, None, "sub"),
            P(CTX, None, "sub"),
            P(CTX, "sub", None),
        ),
        out_specs=P(GRP_CTX, "sub"),
        check_vma=False,
    )
```

```python
import jax
import jax.numpy as jnp
from jax import lax
from jax.experimental import pallas as pl
from jax.experimental.pallas import tpu as pltpu
from jax.sharding import Mesh
from jax.sharding import PartitionSpec as P

D = 2048
NOPE = 128
ROPE = 64
VDIM = 128
LATENT = 512
TOP = 6
CAP = 2
NEAR = 4
CTX = ("far", "near", "core")
GRP_CTX = ("grp", "far", "near", "core")
SEGMENT = ("near", "core")
Z = ("far", "near")
EXTRA = 128

epsilon = 1e-06


def thirds(x):
    high = x.astype(jnp.bfloat16)
    rest = x - high.astype(jnp.float32)
    middle = rest.astype(jnp.bfloat16)
    low = (rest - middle.astype(jnp.float32)).astype(jnp.bfloat16)
    return high.astype(jnp.float32), middle.astype(jnp.float32), low.astype(jnp.float32)


def log_block(logs, rows):
    lane = lax.broadcasted_iota(jnp.int32, (rows, EXTRA), 1)
    heads = len(logs)
    block = jnp.zeros((rows, EXTRA), jnp.float32)
    for h, x in enumerate(logs):
        for piece, part in enumerate(thirds(x)):
            block = jnp.where(lane == heads * piece + h, part, block)
    return block.astype(jnp.bfloat16)


def attention_kernel(place, mine, other, own_cache, pair_cache, out, heads):
    planes = mine.shape[0]
    rows = planes * 8
    first = place[0] == 0
    scale = (NOPE + ROPE) ** (-0.5)
    per_row = 256 // NOPE
    q_rows = heads // per_row * 8
    kv_at = q_rows + 8
    caches = [(c[:LATENT, :], c[LATENT : LATENT + ROPE, :], c[LATENT + ROPE :, :]) for c in (own_cache, pair_cache)]
    logs, tops = [], []
    for h in range(heads):
        a = mine[:, kv_at + 8 * h : kv_at + 8 * h + 8, :]
        b = other[:, kv_at + 8 * h : kv_at + 8 * h + 8, :]
        up = jnp.stack([jnp.where(first, a, b), jnp.where(first, b, a)], axis=1)
        up = up.reshape(planes * 16, 256)
        at, lane = 8 * (h // per_row), NOPE * (h % per_row)
        nope = mine[:, at : at + 8, lane : lane + NOPE].reshape(rows, NOPE)
        rope = mine[:, q_rows : q_rows + 8, ROPE * h : ROPE * h + ROPE].reshape(rows, ROPE)
        absorbed = lax.dot_general(
            nope, up[:, :NOPE], (((1,), (1,)), ((), ())), preferred_element_type=jnp.float32
        ).astype(jnp.bfloat16)
        scores = []
        for latents, rotary, live in caches:
            score = jnp.dot(absorbed, latents, preferred_element_type=jnp.float32)
            score = (score + jnp.dot(rope, rotary, preferred_element_type=jnp.float32)) * scale
            scores.append(jnp.where(live[:1].astype(jnp.float32) > 0.5, score, -jnp.inf))
        highest = jnp.maximum(
            jnp.max(scores[0], axis=1, keepdims=True), jnp.max(scores[1], axis=1, keepdims=True)
        )
        total, mixed = 0.0, 0.0
        for score, (latents, _, _) in zip(scores, caches):
            weights = jnp.exp(score - highest).astype(jnp.bfloat16)
            total += jnp.sum(weights.astype(jnp.float32), axis=1, keepdims=True)
            mixed += lax.dot_general(
                weights, latents, (((1,), (1,)), ((), ())), preferred_element_type=jnp.float32
            )
        head = jnp.dot(mixed.astype(jnp.bfloat16), up[:, NOPE:], preferred_element_type=jnp.float32)
        tops.append((head / total).astype(jnp.bfloat16))
        logs.append(highest + jnp.log(total))
    result = jnp.concatenate([*tops, log_block(logs, rows)], axis=1)
    result = result.reshape(planes, 8, result.shape[1])
    for z in range(planes):
        out[z % NEAR, z // NEAR] = result[z]


def merged(parts, heads):
    sources, rows, _ = parts.shape
    width = heads * VDIM
    lane = lax.broadcasted_iota(jnp.int32, (EXTRA, width), 0)
    col = lax.broadcasted_iota(jnp.int32, (EXTRA, width), 1)
    spread = ((lane < 3 * heads) & (lane % heads == col // VDIM)).astype(jnp.bfloat16)
    packed = parts[:, :, width:].reshape(sources * rows, EXTRA)
    logs = jnp.dot(packed, spread, preferred_element_type=jnp.float32).reshape(sources, rows, width)
    top = jnp.max(logs, axis=0)
    shares = jnp.exp(logs - top[None])
    total = jnp.sum(shares, axis=0)
    mixed = jnp.sum(shares * parts[:, :, :width].astype(jnp.float32), axis=0)
    return mixed / total, top + jnp.log(total)


def merge_kernel(parts, out, heads):
    mixed, logs = merged(parts[...], heads)
    rows = mixed.shape[0]
    block = log_block([logs[:, VDIM * h : VDIM * h + EXTRA] for h in range(heads)], rows)
    out[...] = jnp.concatenate([mixed.astype(jnp.bfloat16), block], axis=1)


def project_kernel(parts, weight, out, heads, cols):
    mixed, _ = merged(parts[...], heads)
    projected = lax.dot_general(
        mixed.astype(jnp.bfloat16), weight[...], (((1,), (1,)), ((), ())), preferred_element_type=jnp.float32
    ).astype(jnp.bfloat16)
    size = 2 * NEAR * cols
    to = lax.broadcasted_iota(jnp.int32, (size, size), 1)
    source = to // cols % 2 * (NEAR * cols) + to // (2 * cols) * cols + to % cols
    turn = (lax.broadcasted_iota(jnp.int32, (size, size), 0) == source).astype(jnp.bfloat16)
    for at in range(0, projected.shape[1], size):
        part = jnp.dot(projected[:, at : at + size], turn, preferred_element_type=jnp.float32).astype(jnp.bfloat16)
        for s in range(out.shape[0]):
            out[s, :, at : at + size] = part


def named_by(ids, expert):
    found = jnp.zeros((ids.shape[0], expert.shape[1]), jnp.float32)
    for k in range(TOP):
        found = jnp.where(ids[:, k : k + 1] == expert, 1.0, found)
    return found


def earlier_rows(named, tokens):
    rows = named.shape[0]
    r = lax.broadcasted_iota(jnp.int32, (rows, rows), 0)
    c = lax.broadcasted_iota(jnp.int32, (rows, rows), 1)
    before = ((r // tokens == c // tokens) & (c < r)).astype(jnp.bfloat16)
    return jnp.dot(before, named.astype(jnp.bfloat16), preferred_element_type=jnp.float32)


def norm_kernel(place, shares, residual, gain, ids, out, hidden_part):
    tokens = residual.shape[0]
    quarter = hidden_part.shape[1]
    hidden = residual[...].astype(jnp.float32) + jnp.sum(shares[...].astype(jnp.float32), axis=0)
    inverse_rms = lax.rsqrt(jnp.mean(hidden * hidden, axis=1, keepdims=True) + epsilon)
    own = pl.ds(pl.multiple_of(place[1] * quarter, quarter), quarter)
    part = residual[:, own].astype(jnp.float32) + jnp.sum(shares[:, :, own].astype(jnp.float32), axis=0)
    hidden_part[...] = part
    normed = (part * inverse_rms * gain[:, own].astype(jnp.float32)).astype(jnp.bfloat16)
    lane = lax.broadcasted_iota(jnp.int32, (tokens, EXTRA), 1)
    named = jnp.zeros((tokens, EXTRA), jnp.float32)
    for k in range(TOP):
        named = jnp.where(lane == k, ids[:, k : k + 1].astype(jnp.float32), named)
    block = jnp.concatenate([normed, named.astype(jnp.bfloat16)], axis=1)
    for f in range(out.shape[0]):
        out[f] = block


def route_kernel(place, blocks, out):
    sources, tokens, width = blocks.shape
    segment, slots, quarter = out.shape
    rows = sources * tokens
    ids = blocks[:, :, quarter:].astype(jnp.float32).reshape(rows, width - quarter)
    col = lax.broadcasted_iota(jnp.int32, (1, segment * slots), 1)
    expert = (place[2] * segment + col // slots).astype(jnp.float32)
    named = named_by(ids, expert)
    row = lax.broadcasted_iota(jnp.int32, (rows, segment * slots), 0)
    lane = lax.broadcasted_iota(jnp.int32, (rows, segment * slots), 1)
    right = (lane // CAP % sources == row // tokens) & (
        earlier_rows(named, tokens) == (lane % CAP).astype(jnp.float32)
    )
    chosen = jnp.where(right, named, 0.0)
    taken = lax.dot_general(
        chosen,
        blocks[:, :, :quarter].astype(jnp.float32).reshape(rows, quarter),
        (((0,), (0,)), ((), ())),
        preferred_element_type=jnp.float32,
    )
    out[...] = taken.reshape(segment, slots, quarter).astype(jnp.bfloat16)


def expert_kernel(received, gate, up, down, out):
    subs, _, quarter = received.shape
    side = (((1,), (1,)), ((), ()))
    gate_act, up_act = 0.0, 0.0
    for s in range(subs):
        rows = received[s]
        cols = slice(s * quarter, (s + 1) * quarter)
        gate_act += lax.dot_general(rows, gate[:, cols], side, preferred_element_type=jnp.float32)
        up_act += lax.dot_general(rows, up[:, cols], side, preferred_element_type=jnp.float32)
    gated = (gate_act / (1.0 + jnp.exp(-gate_act)) * up_act).astype(jnp.bfloat16)
    for s in range(subs):
        cols = slice(s * quarter, (s + 1) * quarter)
        out[s] = jnp.dot(gated, down[:, cols], preferred_element_type=jnp.float32).astype(jnp.bfloat16)


def final_kernel(hidden_part, back, ids, weights, out, segment):
    tokens = ids.shape[0]
    slots = back.shape[0]
    fars = slots // (segment * CAP)
    col = lax.broadcasted_iota(jnp.int32, (1, slots), 1)
    expert = col // CAP % fars * segment + col // (CAP * fars)
    named = named_by(ids[...], expert)
    share = jnp.zeros((tokens, slots), jnp.float32)
    for k in range(TOP):
        share = jnp.where(ids[:, k : k + 1] == expert, weights[:, k : k + 1], share)
    lane = lax.broadcasted_iota(jnp.int32, (tokens, slots), 1)
    share = jnp.where(earlier_rows(named, tokens) == (lane % CAP).astype(jnp.float32), share, 0.0)
    routed = jnp.dot(share.astype(jnp.bfloat16), back[...], preferred_element_type=jnp.float32)
    out[...] = (hidden_part[...] + routed).astype(jnp.bfloat16)


def gathered(packed):
    near = lax.all_gather(packed, Z, axis=0, tiled=False)
    far = lax.ppermute(near, "core", [(0, 1), (1, 0)])
    return near, far


def body(
    queries,
    latent_cache,
    cache_len,
    kv_up,
    o_weight,
    residual,
    norm_gain,
    route_ids,
    route_weights,
    w_gate,
    w_up,
    w_down,
):
    ctx_count = lax.axis_size(CTX)
    sub_count = lax.axis_size("sub")
    heads = kv_up.shape[0]
    tokens = queries.shape[0]
    width = heads * VDIM + EXTRA
    planes = ctx_count // 2

    split = queries.reshape(tokens, heads, NOPE + ROPE)
    nope = split[:, :, :NOPE].reshape(tokens, heads * NOPE // 256, 256).transpose(1, 0, 2)
    rope = split[:, :, NOPE:].reshape(tokens, heads * ROPE // 256, 256).transpose(1, 0, 2)
    ups = kv_up.transpose(0, 2, 1)
    packed = jnp.concatenate(
        [nope.reshape(-1, 256), rope.reshape(-1, 256), ups.reshape(-1, 256)], axis=0
    )
    place = jnp.stack([lax.axis_index("core"), lax.axis_index("sub"), lax.axis_index("far")])
    cols = o_weight.shape[1]
    near_o = lax.all_to_all(
        jnp.broadcast_to(o_weight.T[None], (NEAR, cols, o_weight.shape[0])), "near", 0, 0, tiled=True
    )
    o_full = lax.all_gather(near_o, ("far", "core"), axis=0, tiled=False)
    live = lax.broadcasted_iota(jnp.int32, (8, latent_cache.shape[0]), 1) < cache_len[0]
    own_cache = jnp.concatenate([latent_cache.T, live.astype(jnp.bfloat16)], axis=0)
    pair_cache = lax.ppermute(own_cache, "core", [(0, 1), (1, 0)])
    mine, other = gathered(packed)

    smem = pl.BlockSpec(memory_space=pltpu.SMEM)
    vmem = pl.BlockSpec(memory_space=pltpu.VMEM)
    fars = planes // NEAR
    rows = fars * tokens
    partial = pl.pallas_call(
        lambda *refs: attention_kernel(*refs, heads),
        out_shape=jax.ShapeDtypeStruct((NEAR, fars, tokens, width), jnp.bfloat16),
        in_specs=[smem, vmem, vmem, vmem, vmem],
        out_specs=vmem,
        compiler_params=pltpu.CompilerParams(vmem_limit_bytes=24 * 2**20),
        name="attention",
    )(place, mine, other, own_cache, pair_cache)
    segment = NEAR * 2
    partial = lax.all_to_all(partial.reshape(NEAR, rows, width), "near", 0, 0, tiled=True)
    partial = pl.pallas_call(
        lambda *refs: merge_kernel(*refs, heads),
        out_shape=jax.ShapeDtypeStruct((rows, width), jnp.bfloat16),
        in_specs=[vmem],
        out_specs=vmem,
        compiler_params=pltpu.CompilerParams(vmem_limit_bytes=12 * 2**20),
        name="merge",
    )(partial)
    partial = lax.all_to_all(partial.reshape(fars, tokens, width), "far", 0, 0, tiled=True)
    projected = pl.pallas_call(
        lambda *refs: project_kernel(*refs, heads, o_weight.shape[1]),
        out_shape=jax.ShapeDtypeStruct((sub_count, tokens, D), jnp.bfloat16),
        in_specs=[vmem, vmem],
        out_specs=vmem,
        compiler_params=pltpu.CompilerParams(vmem_limit_bytes=12 * 2**20),
        name="project",
    )(partial, o_full.reshape(D, o_weight.shape[0]))

    shares = lax.all_to_all(projected, "sub", 0, 0, tiled=True)
    quarter = D // sub_count
    blocks, hidden_part = pl.pallas_call(
        norm_kernel,
        out_shape=(
            jax.ShapeDtypeStruct((fars, tokens, quarter + EXTRA), jnp.bfloat16),
            jax.ShapeDtypeStruct((tokens, quarter), jnp.float32),
        ),
        in_specs=[smem, vmem, vmem, vmem, vmem],
        out_specs=(vmem, vmem),
        compiler_params=pltpu.CompilerParams(vmem_limit_bytes=8 * 2**20),
        name="norm",
    )(place, shares, residual, norm_gain.reshape(1, D), route_ids)
    blocks = lax.all_to_all(blocks, "far", 0, 0, tiled=True)
    rows = fars * CAP
    outgoing = pl.pallas_call(
        route_kernel,
        out_shape=jax.ShapeDtypeStruct((segment, rows, quarter), jnp.bfloat16),
        in_specs=[smem, vmem],
        out_specs=vmem,
        compiler_params=pltpu.CompilerParams(vmem_limit_bytes=8 * 2**20),
        name="route",
    )(place, blocks)
    received = lax.all_to_all(outgoing, SEGMENT, 0, 0, tiled=True).reshape(segment * rows, quarter)
    received = lax.all_gather(received, "sub", axis=0, tiled=False)
    partial_out = pl.pallas_call(
        expert_kernel,
        out_shape=jax.ShapeDtypeStruct((sub_count, segment * rows, quarter), jnp.bfloat16),
        in_specs=[vmem] * 4,
        out_specs=vmem,
        compiler_params=pltpu.CompilerParams(vmem_limit_bytes=16 * 2**20),
        name="experts",
    )(received, w_gate[0].T, w_up[0].T, w_down[0])
    parts = lax.all_to_all(partial_out, "sub", 0, 0, tiled=True)
    summed = jnp.sum(parts.astype(jnp.float32), axis=0).astype(jnp.bfloat16)
    summed = summed.reshape(ctx_count, CAP, quarter)
    back = lax.all_to_all(summed, (*SEGMENT, "far"), 0, 0, tiled=True)
    return pl.pallas_call(
        lambda *refs: final_kernel(*refs, segment),
        out_shape=jax.ShapeDtypeStruct((tokens, quarter), jnp.bfloat16),
        in_specs=[vmem] * 4,
        out_specs=vmem,
        compiler_params=pltpu.CompilerParams(vmem_limit_bytes=8 * 2**20),
        name="final",
    )(hidden_part, back.reshape(ctx_count * CAP, quarter), route_ids, route_weights)


def solution(mesh):
    planes = mesh.shape["ctx"] // 2
    split = Mesh(
        mesh.devices.reshape(mesh.shape["grp"], planes // NEAR, NEAR, 2, mesh.shape["sub"]),
        ("grp", "far", "near", "core", "sub"),
    )
    return jax.shard_map(
        body,
        mesh=split,
        in_specs=(
            P(GRP_CTX, "sub"),
            P(GRP_CTX, None),
            P(GRP_CTX),
            P(("grp", "sub"), None, CTX),
            P("sub", CTX),
            P(GRP_CTX, None),
            P(),
            P(GRP_CTX, None),
            P(GRP_CTX, None),
            P(CTX, None, "sub"),
            P(CTX, None, "sub"),
            P(CTX, "sub", None),
        ),
        out_specs=P(GRP_CTX, "sub"),
        check_vma=False,
    )
```

```python
import jax
import jax.numpy as jnp
from jax import lax
from jax.experimental import pallas as pl
from jax.experimental.pallas import tpu as pltpu
from jax.sharding import Mesh
from jax.sharding import PartitionSpec as P

D = 2048
NOPE = 128
ROPE = 64
VDIM = 128
LATENT = 512
TOP = 6
CAP = 2
NEAR = 4
PAIR = 2
NEARBY = ("hop", "pair")
CTX = ("far", "hop", "pair", "core")
GRP_CTX = ("grp", *CTX)
SEGMENT = ("hop", "pair", "core")
Z = ("far", "hop", "pair")
EXTRA = 128

epsilon = 1e-06


def thirds(x):
    high = x.astype(jnp.bfloat16)
    rest = x - high.astype(jnp.float32)
    middle = rest.astype(jnp.bfloat16)
    low = (rest - middle.astype(jnp.float32)).astype(jnp.bfloat16)
    return high.astype(jnp.float32), middle.astype(jnp.float32), low.astype(jnp.float32)


def log_block(logs, rows):
    lane = lax.broadcasted_iota(jnp.int32, (rows, EXTRA), 1)
    heads = len(logs)
    block = jnp.zeros((rows, EXTRA), jnp.float32)
    for h, x in enumerate(logs):
        for piece, part in enumerate(thirds(x)):
            block = jnp.where(lane == heads * piece + h, part, block)
    return block.astype(jnp.bfloat16)


def attention_kernel(place, mine, other, own_cache, pair_cache, out, heads):
    planes = mine.shape[0]
    rows = planes * 8
    first = place[0] == 0
    scale = (NOPE + ROPE) ** (-0.5)
    per_row = 256 // NOPE
    q_rows = heads // per_row * 8
    kv_at = q_rows + 8
    caches = [(c[:LATENT, :], c[LATENT : LATENT + ROPE, :], c[LATENT + ROPE :, :]) for c in (own_cache, pair_cache)]
    logs, tops = [], []
    for h in range(heads):
        a = mine[:, kv_at + 8 * h : kv_at + 8 * h + 8, :]
        b = other[:, kv_at + 8 * h : kv_at + 8 * h + 8, :]
        up = jnp.stack([jnp.where(first, a, b), jnp.where(first, b, a)], axis=1)
        up = up.reshape(planes * 16, 256)
        at, lane = 8 * (h // per_row), NOPE * (h % per_row)
        nope = mine[:, at : at + 8, lane : lane + NOPE].reshape(rows, NOPE)
        rope = mine[:, q_rows : q_rows + 8, ROPE * h : ROPE * h + ROPE].reshape(rows, ROPE)
        absorbed = lax.dot_general(
            nope, up[:, :NOPE], (((1,), (1,)), ((), ())), preferred_element_type=jnp.float32
        ).astype(jnp.bfloat16)
        scores = []
        for latents, rotary, live in caches:
            score = jnp.dot(absorbed, latents, preferred_element_type=jnp.float32)
            score = (score + jnp.dot(rope, rotary, preferred_element_type=jnp.float32)) * scale
            scores.append(jnp.where(live[:1].astype(jnp.float32) > 0.5, score, -jnp.inf))
        highest = jnp.maximum(
            jnp.max(scores[0], axis=1, keepdims=True), jnp.max(scores[1], axis=1, keepdims=True)
        )
        total, mixed = 0.0, 0.0
        for score, (latents, _, _) in zip(scores, caches):
            weights = jnp.exp(score - highest).astype(jnp.bfloat16)
            total += jnp.sum(weights.astype(jnp.float32), axis=1, keepdims=True)
            mixed += lax.dot_general(
                weights, latents, (((1,), (1,)), ((), ())), preferred_element_type=jnp.float32
            )
        head = jnp.dot(mixed.astype(jnp.bfloat16), up[:, NOPE:], preferred_element_type=jnp.float32)
        tops.append((head / total).astype(jnp.bfloat16))
        logs.append(highest + jnp.log(total))
    result = jnp.concatenate([*tops, log_block(logs, rows)], axis=1)
    result = result.reshape(planes, 8, result.shape[1])
    for z in range(planes):
        out[z % NEAR, z // NEAR] = result[z]


def merged(parts, heads):
    sources, rows, _ = parts.shape
    width = heads * VDIM
    lane = lax.broadcasted_iota(jnp.int32, (EXTRA, width), 0)
    col = lax.broadcasted_iota(jnp.int32, (EXTRA, width), 1)
    spread = ((lane < 3 * heads) & (lane % heads == col // VDIM)).astype(jnp.bfloat16)
    packed = parts[:, :, width:].reshape(sources * rows, EXTRA)
    logs = jnp.dot(packed, spread, preferred_element_type=jnp.float32).reshape(sources, rows, width)
    top = jnp.max(logs, axis=0)
    shares = jnp.exp(logs - top[None])
    total = jnp.sum(shares, axis=0)
    mixed = jnp.sum(shares * parts[:, :, :width].astype(jnp.float32), axis=0)
    return mixed / total, top + jnp.log(total)


def merge_kernel(parts, out, heads):
    mixed, logs = merged(parts[...], heads)
    rows = mixed.shape[0]
    block = log_block([logs[:, VDIM * h : VDIM * h + EXTRA] for h in range(heads)], rows)
    out[...] = jnp.concatenate([mixed.astype(jnp.bfloat16), block], axis=1)


def project_kernel(parts, weight, out, heads, cols):
    mixed, _ = merged(parts[...], heads)
    size = 2 * PAIR * cols
    to = lax.broadcasted_iota(jnp.int32, (size, size), 1)
    source = to // cols % 2 * (PAIR * cols) + to // (2 * cols) * cols + to % cols
    turn = (lax.broadcasted_iota(jnp.int32, (size, size), 0) == source).astype(jnp.bfloat16)
    projected = lax.dot_general(
        mixed.astype(jnp.bfloat16), weight[...], (((1,), (1,)), ((), ())), preferred_element_type=jnp.float32
    ).astype(jnp.bfloat16)
    for at in range(0, projected.shape[1], size):
        part = jnp.dot(projected[:, at : at + size], turn, preferred_element_type=jnp.float32).astype(jnp.bfloat16)
        for s in range(out.shape[0]):
            out[s, :, at : at + size] = part


def named_by(ids, expert):
    found = jnp.zeros((ids.shape[0], expert.shape[1]), jnp.float32)
    for k in range(TOP):
        found = jnp.where(ids[:, k : k + 1] == expert, 1.0, found)
    return found


def earlier_rows(named, tokens):
    rows = named.shape[0]
    r = lax.broadcasted_iota(jnp.int32, (rows, rows), 0)
    c = lax.broadcasted_iota(jnp.int32, (rows, rows), 1)
    before = ((r // tokens == c // tokens) & (c < r)).astype(jnp.bfloat16)
    return jnp.dot(before, named.astype(jnp.bfloat16), preferred_element_type=jnp.float32)


def norm_kernel(place, shares, residual, gain, ids, out, hidden_part):
    tokens = residual.shape[0]
    quarter = hidden_part.shape[1]
    hidden = residual[...].astype(jnp.float32) + jnp.sum(shares[...].astype(jnp.float32), axis=0)
    inverse_rms = lax.rsqrt(jnp.mean(hidden * hidden, axis=1, keepdims=True) + epsilon)
    own = pl.ds(pl.multiple_of(place[1] * quarter, quarter), quarter)
    part = residual[:, own].astype(jnp.float32) + jnp.sum(shares[:, :, own].astype(jnp.float32), axis=0)
    hidden_part[...] = part
    normed = (part * inverse_rms * gain[:, own].astype(jnp.float32)).astype(jnp.bfloat16)
    lane = lax.broadcasted_iota(jnp.int32, (tokens, EXTRA), 1)
    named = jnp.zeros((tokens, EXTRA), jnp.float32)
    for k in range(TOP):
        named = jnp.where(lane == k, ids[:, k : k + 1].astype(jnp.float32), named)
    block = jnp.concatenate([normed, named.astype(jnp.bfloat16)], axis=1)
    for f in range(out.shape[0]):
        out[f] = block


def route_kernel(place, blocks, out):
    sources, tokens, width = blocks.shape
    segment, subs, slots, quarter = out.shape
    rows = sources * tokens
    ids = blocks[:, :, quarter:].astype(jnp.float32).reshape(rows, width - quarter)
    col = lax.broadcasted_iota(jnp.int32, (1, segment * slots), 1)
    expert = (place[2] * segment + col // slots).astype(jnp.float32)
    named = named_by(ids, expert)
    row = lax.broadcasted_iota(jnp.int32, (rows, segment * slots), 0)
    lane = lax.broadcasted_iota(jnp.int32, (rows, segment * slots), 1)
    right = (lane // CAP % sources == row // tokens) & (
        earlier_rows(named, tokens) == (lane % CAP).astype(jnp.float32)
    )
    chosen = jnp.where(right, named, 0.0)
    taken = lax.dot_general(
        chosen,
        blocks[:, :, :quarter].astype(jnp.float32).reshape(rows, quarter),
        (((0,), (0,)), ((), ())),
        preferred_element_type=jnp.float32,
    )
    taken = taken.reshape(segment, slots, quarter).astype(jnp.bfloat16)
    for s in range(subs):
        out[:, s] = taken


def expert_kernel(received, gate, up, down, out):
    subs, total, quarter = out.shape
    side = (((1,), (1,)), ((), ()))
    gate_act, up_act = 0.0, 0.0
    for s in range(subs):
        rows = received[:, s].reshape(total, quarter)
        cols = slice(s * quarter, (s + 1) * quarter)
        gate_act += lax.dot_general(rows, gate[:, cols], side, preferred_element_type=jnp.float32)
        up_act += lax.dot_general(rows, up[:, cols], side, preferred_element_type=jnp.float32)
    gated = (gate_act / (1.0 + jnp.exp(-gate_act)) * up_act).astype(jnp.bfloat16)
    for s in range(subs):
        cols = slice(s * quarter, (s + 1) * quarter)
        out[s] = jnp.dot(gated, down[:, cols], preferred_element_type=jnp.float32).astype(jnp.bfloat16)


def final_kernel(hidden_part, back, ids, weights, out, segment):
    tokens = ids.shape[0]
    slots = back.shape[0]
    fars = slots // (segment * CAP)
    col = lax.broadcasted_iota(jnp.int32, (1, slots), 1)
    expert = col // CAP % fars * segment + col // (CAP * fars)
    named = named_by(ids[...], expert)
    share = jnp.zeros((tokens, slots), jnp.float32)
    for k in range(TOP):
        share = jnp.where(ids[:, k : k + 1] == expert, weights[:, k : k + 1], share)
    lane = lax.broadcasted_iota(jnp.int32, (tokens, slots), 1)
    share = jnp.where(earlier_rows(named, tokens) == (lane % CAP).astype(jnp.float32), share, 0.0)
    routed = jnp.dot(share.astype(jnp.bfloat16), back[...], preferred_element_type=jnp.float32)
    out[...] = (hidden_part[...] + routed).astype(jnp.bfloat16)


def gathered(packed):
    near = lax.all_gather(packed, Z, axis=0, tiled=False)
    far = lax.ppermute(near, "core", [(0, 1), (1, 0)])
    return near, far


def body(
    queries,
    latent_cache,
    cache_len,
    kv_up,
    o_weight,
    residual,
    norm_gain,
    route_ids,
    route_weights,
    w_gate,
    w_up,
    w_down,
):
    ctx_count = lax.axis_size(CTX)
    sub_count = lax.axis_size("sub")
    heads = kv_up.shape[0]
    tokens = queries.shape[0]
    width = heads * VDIM + EXTRA
    planes = ctx_count // 2

    split = queries.reshape(tokens, heads, NOPE + ROPE)
    nope = split[:, :, :NOPE].reshape(tokens, heads * NOPE // 256, 256).transpose(1, 0, 2)
    rope = split[:, :, NOPE:].reshape(tokens, heads * ROPE // 256, 256).transpose(1, 0, 2)
    ups = kv_up.transpose(0, 2, 1)
    packed = jnp.concatenate(
        [nope.reshape(-1, 256), rope.reshape(-1, 256), ups.reshape(-1, 256)], axis=0
    )
    place = jnp.stack([lax.axis_index("core"), lax.axis_index("sub"), lax.axis_index("far")])
    cols = o_weight.shape[1]
    near_o = lax.all_to_all(
        jnp.broadcast_to(o_weight.T[None], (PAIR, cols, o_weight.shape[0])), "pair", 0, 0, tiled=True
    )
    o_full = lax.all_gather(near_o, ("far", "hop", "core"), axis=0, tiled=False)
    live = lax.broadcasted_iota(jnp.int32, (8, latent_cache.shape[0]), 1) < cache_len[0]
    own_cache = jnp.concatenate([latent_cache.T, live.astype(jnp.bfloat16)], axis=0)
    pair_cache = lax.ppermute(own_cache, "core", [(0, 1), (1, 0)])
    mine, other = gathered(packed)

    smem = pl.BlockSpec(memory_space=pltpu.SMEM)
    vmem = pl.BlockSpec(memory_space=pltpu.VMEM)
    fars = planes // NEAR
    rows = fars * tokens
    partial = pl.pallas_call(
        lambda *refs: attention_kernel(*refs, heads),
        out_shape=jax.ShapeDtypeStruct((NEAR, fars, tokens, width), jnp.bfloat16),
        in_specs=[smem, vmem, vmem, vmem, vmem],
        out_specs=vmem,
        compiler_params=pltpu.CompilerParams(vmem_limit_bytes=24 * 2**20),
        name="attention",
    )(place, mine, other, own_cache, pair_cache)
    segment = NEAR * 2
    partial = lax.all_to_all(partial.reshape(NEAR, rows, width), NEARBY, 0, 0, tiled=True)
    partial = pl.pallas_call(
        lambda *refs: merge_kernel(*refs, heads),
        out_shape=jax.ShapeDtypeStruct((rows, width), jnp.bfloat16),
        in_specs=[vmem],
        out_specs=vmem,
        compiler_params=pltpu.CompilerParams(vmem_limit_bytes=12 * 2**20),
        name="merge",
    )(partial)
    partial = lax.all_to_all(partial.reshape(fars, tokens, width), "far", 0, 0, tiled=True)
    projected = pl.pallas_call(
        lambda *refs: project_kernel(*refs, heads, o_weight.shape[1]),
        out_shape=jax.ShapeDtypeStruct((sub_count, tokens, D), jnp.bfloat16),
        in_specs=[vmem, vmem],
        out_specs=vmem,
        compiler_params=pltpu.CompilerParams(vmem_limit_bytes=12 * 2**20),
        name="project",
    )(partial, o_full.reshape(D, o_weight.shape[0]))

    shares = lax.all_to_all(projected, "sub", 0, 0, tiled=True)
    quarter = D // sub_count
    blocks, hidden_part = pl.pallas_call(
        norm_kernel,
        out_shape=(
            jax.ShapeDtypeStruct((fars, tokens, quarter + EXTRA), jnp.bfloat16),
            jax.ShapeDtypeStruct((tokens, quarter), jnp.float32),
        ),
        in_specs=[smem, vmem, vmem, vmem, vmem],
        out_specs=(vmem, vmem),
        compiler_params=pltpu.CompilerParams(vmem_limit_bytes=8 * 2**20),
        name="norm",
    )(place, shares, residual, norm_gain.reshape(1, D), route_ids)
    blocks = lax.all_to_all(blocks, "far", 0, 0, tiled=True)
    rows = fars * CAP
    outgoing = pl.pallas_call(
        route_kernel,
        out_shape=jax.ShapeDtypeStruct((segment, sub_count, rows, quarter), jnp.bfloat16),
        in_specs=[smem, vmem],
        out_specs=vmem,
        compiler_params=pltpu.CompilerParams(vmem_limit_bytes=8 * 2**20),
        name="route",
    )(place, blocks)
    received = lax.all_to_all(
        outgoing.reshape(segment * sub_count, rows, quarter), (*SEGMENT, "sub"), 0, 0, tiled=True
    ).reshape(segment, sub_count, rows, quarter)
    partial_out = pl.pallas_call(
        expert_kernel,
        out_shape=jax.ShapeDtypeStruct((sub_count, segment * rows, quarter), jnp.bfloat16),
        in_specs=[vmem, vmem, vmem, vmem],
        out_specs=vmem,
        compiler_params=pltpu.CompilerParams(vmem_limit_bytes=16 * 2**20),
        name="experts",
    )(received, w_gate[0].T, w_up[0].T, w_down[0])
    parts = lax.all_to_all(partial_out, "sub", 0, 0, tiled=True)
    summed = jnp.sum(parts.astype(jnp.float32), axis=0).astype(jnp.bfloat16)
    summed = summed.reshape(ctx_count, CAP, quarter)
    back = lax.all_to_all(summed, (*SEGMENT, "far"), 0, 0, tiled=True)
    return pl.pallas_call(
        lambda *refs: final_kernel(*refs, segment),
        out_shape=jax.ShapeDtypeStruct((tokens, quarter), jnp.bfloat16),
        in_specs=[vmem] * 4,
        out_specs=vmem,
        compiler_params=pltpu.CompilerParams(vmem_limit_bytes=8 * 2**20),
        name="final",
    )(hidden_part, back.reshape(ctx_count * CAP, quarter), route_ids, route_weights)


def solution(mesh):
    planes = mesh.shape["ctx"] // 2
    split = Mesh(
        mesh.devices.reshape(mesh.shape["grp"], planes // NEAR, NEAR // PAIR, PAIR, 2, mesh.shape["sub"]),
        (*GRP_CTX, "sub"),
    )
    return jax.shard_map(
        body,
        mesh=split,
        in_specs=(
            P(GRP_CTX, "sub"),
            P(GRP_CTX, None),
            P(GRP_CTX),
            P(("grp", "sub"), None, CTX),
            P("sub", CTX),
            P(GRP_CTX, None),
            P(),
            P(GRP_CTX, None),
            P(GRP_CTX, None),
            P(CTX, None, "sub"),
            P(CTX, None, "sub"),
            P(CTX, "sub", None),
        ),
        out_specs=P(GRP_CTX, "sub"),
        check_vma=False,
    )
```

```python
import jax
import jax.numpy as jnp
from jax import lax
from jax.experimental import pallas as pl
from jax.experimental.pallas import tpu as pltpu
from jax.sharding import Mesh
from jax.sharding import PartitionSpec as P

D = 2048
NOPE = 128
ROPE = 64
VDIM = 128
LATENT = 512
TOP = 6
CAP = 2
NEAR = 4
PAIR = 2
NEARBY = ("hop", "pair")
CTX = ("far", "hop", "pair", "core")
GRP_CTX = ("grp", *CTX)
SEGMENT = ("hop", "pair", "core")
Z = ("far", "hop", "pair")
EXTRA = 128

epsilon = 1e-06


def thirds(x):
    high = x.astype(jnp.bfloat16)
    rest = x - high.astype(jnp.float32)
    middle = rest.astype(jnp.bfloat16)
    low = (rest - middle.astype(jnp.float32)).astype(jnp.bfloat16)
    return high.astype(jnp.float32), middle.astype(jnp.float32), low.astype(jnp.float32)


def log_block(logs, rows):
    lane = lax.broadcasted_iota(jnp.int32, (rows, EXTRA), 1)
    heads = len(logs)
    block = jnp.zeros((rows, EXTRA), jnp.float32)
    for h, x in enumerate(logs):
        for piece, part in enumerate(thirds(x)):
            block = jnp.where(lane == heads * piece + h, part, block)
    return block.astype(jnp.bfloat16)


def pack_kernel(length, queries, ups, o_rows, cache, packed, own_cache, heads):
    step = NOPE + ROPE
    per_row = 256 // NOPE
    half = o_rows.shape[1] // 2
    rows = []
    for r in range(heads // per_row):
        rows.append([queries[:, h * step : h * step + NOPE] for h in range(per_row * r, per_row * r + per_row)])
    rows.append([queries[:, h * step + NOPE : h * step + step] for h in range(heads)])
    parts = [jnp.concatenate(r, axis=1) for r in rows]
    parts += [ups[...], o_rows[:, :half], o_rows[:, half:]]
    for p in range(packed.shape[0]):
        at = 0
        for part in parts:
            packed[p, at : at + part.shape[0], :] = part
            at += part.shape[0]
    width = cache.shape[0]
    own_cache[:width, :] = cache[...]
    shape = (own_cache.shape[0] - width, cache.shape[1])
    live = lax.broadcasted_iota(jnp.int32, shape, 1) < length[0]
    own_cache[width:, :] = jnp.where(live, 1.0, 0.0).astype(jnp.bfloat16)


def attention_kernel(place, mine, other, own_cache, pair_cache, out, heads):
    planes = mine.shape[0]
    rows = planes * 8
    first = place[0] == 0
    scale = (NOPE + ROPE) ** (-0.5)
    per_row = 256 // NOPE
    q_rows = heads // per_row * 8
    kv_at = q_rows + 8
    caches = [(c[:LATENT, :], c[LATENT : LATENT + ROPE, :], c[LATENT + ROPE :, :]) for c in (own_cache, pair_cache)]
    logs, tops = [], []
    for h in range(heads):
        a = mine[:, kv_at + 8 * h : kv_at + 8 * h + 8, :]
        b = other[:, kv_at + 8 * h : kv_at + 8 * h + 8, :]
        up = jnp.stack([jnp.where(first, a, b), jnp.where(first, b, a)], axis=1)
        up = up.reshape(planes * 16, 256)
        at, lane = 8 * (h // per_row), NOPE * (h % per_row)
        nope = mine[:, at : at + 8, lane : lane + NOPE].reshape(rows, NOPE)
        rope = mine[:, q_rows : q_rows + 8, ROPE * h : ROPE * h + ROPE].reshape(rows, ROPE)
        absorbed = lax.dot_general(
            nope, up[:, :NOPE], (((1,), (1,)), ((), ())), preferred_element_type=jnp.float32
        ).astype(jnp.bfloat16)
        scores = []
        for latents, rotary, live in caches:
            score = jnp.dot(absorbed, latents, preferred_element_type=jnp.float32)
            score = (score + jnp.dot(rope, rotary, preferred_element_type=jnp.float32)) * scale
            scores.append(jnp.where(live[:1].astype(jnp.float32) > 0.5, score, -jnp.inf))
        highest = jnp.maximum(
            jnp.max(scores[0], axis=1, keepdims=True), jnp.max(scores[1], axis=1, keepdims=True)
        )
        total, mixed = 0.0, 0.0
        for score, (latents, _, _) in zip(scores, caches):
            weights = jnp.exp(score - highest).astype(jnp.bfloat16)
            total += jnp.sum(weights.astype(jnp.float32), axis=1, keepdims=True)
            mixed += lax.dot_general(
                weights, latents, (((1,), (1,)), ((), ())), preferred_element_type=jnp.float32
            )
        head = jnp.dot(mixed.astype(jnp.bfloat16), up[:, NOPE:], preferred_element_type=jnp.float32)
        tops.append((head / total).astype(jnp.bfloat16))
        logs.append(highest + jnp.log(total))
    result = jnp.concatenate([*tops, log_block(logs, rows)], axis=1)
    result = result.reshape(planes, 8, result.shape[1])
    for z in range(planes):
        out[z % NEAR, z // NEAR] = result[z]


def merged(parts, heads):
    sources, rows, _ = parts.shape
    width = heads * VDIM
    lane = lax.broadcasted_iota(jnp.int32, (EXTRA, width), 0)
    col = lax.broadcasted_iota(jnp.int32, (EXTRA, width), 1)
    spread = ((lane < 3 * heads) & (lane % heads == col // VDIM)).astype(jnp.bfloat16)
    packed = parts[:, :, width:].reshape(sources * rows, EXTRA)
    logs = jnp.dot(packed, spread, preferred_element_type=jnp.float32).reshape(sources, rows, width)
    top = jnp.max(logs, axis=0)
    shares = jnp.exp(logs - top[None])
    total = jnp.sum(shares, axis=0)
    mixed = jnp.sum(shares * parts[:, :, :width].astype(jnp.float32), axis=0)
    return mixed / total, top + jnp.log(total)


def merge_kernel(parts, out, heads):
    mixed, logs = merged(parts[...], heads)
    rows = mixed.shape[0]
    block = log_block([logs[:, VDIM * h : VDIM * h + EXTRA] for h in range(heads)], rows)
    out[...] = jnp.concatenate([mixed.astype(jnp.bfloat16), block], axis=1)


def project_kernel(parts, weight, out, heads, cols):
    mixed, _ = merged(parts[...], heads)
    size = 2 * PAIR * cols
    to = lax.broadcasted_iota(jnp.int32, (size, size), 1)
    source = to // cols % 2 * (PAIR * cols) + to // (2 * cols) * cols + to % cols
    turn = (lax.broadcasted_iota(jnp.int32, (size, size), 0) == source).astype(jnp.bfloat16)
    mixed = mixed.astype(jnp.bfloat16)
    half = weight.shape[4]
    projected = 0.0
    for k in range(2):
        rows = weight[:, :, k].reshape(-1, half)
        projected += lax.dot_general(
            mixed[:, k * half : k * half + half],
            rows,
            (((1,), (1,)), ((), ())),
            preferred_element_type=jnp.float32,
        )
    projected = projected.astype(jnp.bfloat16)
    for at in range(0, projected.shape[1], size):
        part = jnp.dot(projected[:, at : at + size], turn, preferred_element_type=jnp.float32).astype(jnp.bfloat16)
        for s in range(out.shape[0]):
            out[s, :, at : at + size] = part


def named_by(ids, expert):
    found = jnp.zeros((ids.shape[0], expert.shape[1]), jnp.float32)
    for k in range(TOP):
        found = jnp.where(ids[:, k : k + 1] == expert, 1.0, found)
    return found


def earlier_rows(named, tokens):
    rows = named.shape[0]
    r = lax.broadcasted_iota(jnp.int32, (rows, rows), 0)
    c = lax.broadcasted_iota(jnp.int32, (rows, rows), 1)
    before = ((r // tokens == c // tokens) & (c < r)).astype(jnp.bfloat16)
    return jnp.dot(before, named.astype(jnp.bfloat16), preferred_element_type=jnp.float32)


def norm_kernel(place, shares, residual, gain, ids, out, hidden_part):
    tokens = residual.shape[0]
    quarter = hidden_part.shape[1]
    hidden = residual[...].astype(jnp.float32) + jnp.sum(shares[...].astype(jnp.float32), axis=0)
    inverse_rms = lax.rsqrt(jnp.mean(hidden * hidden, axis=1, keepdims=True) + epsilon)
    own = pl.ds(pl.multiple_of(place[1] * quarter, quarter), quarter)
    part = residual[:, own].astype(jnp.float32) + jnp.sum(shares[:, :, own].astype(jnp.float32), axis=0)
    hidden_part[...] = part
    normed = (part * inverse_rms * gain[:, own].astype(jnp.float32)).astype(jnp.bfloat16)
    lane = lax.broadcasted_iota(jnp.int32, (tokens, EXTRA), 1)
    named = jnp.zeros((tokens, EXTRA), jnp.float32)
    for k in range(TOP):
        named = jnp.where(lane == k, ids[:, k : k + 1].astype(jnp.float32), named)
    block = jnp.concatenate([normed, named.astype(jnp.bfloat16)], axis=1)
    for f in range(out.shape[0]):
        out[f] = block


def route_kernel(place, blocks, out):
    sources, tokens, width = blocks.shape
    segment, subs, slots, quarter = out.shape
    rows = sources * tokens
    ids = blocks[:, :, quarter:].astype(jnp.float32).reshape(rows, width - quarter)
    col = lax.broadcasted_iota(jnp.int32, (1, segment * slots), 1)
    expert = (place[2] * segment + col // slots).astype(jnp.float32)
    named = named_by(ids, expert)
    row = lax.broadcasted_iota(jnp.int32, (rows, segment * slots), 0)
    lane = lax.broadcasted_iota(jnp.int32, (rows, segment * slots), 1)
    right = (lane // CAP % sources == row // tokens) & (
        earlier_rows(named, tokens) == (lane % CAP).astype(jnp.float32)
    )
    chosen = jnp.where(right, named, 0.0)
    taken = lax.dot_general(
        chosen,
        blocks[:, :, :quarter].astype(jnp.float32).reshape(rows, quarter),
        (((0,), (0,)), ((), ())),
        preferred_element_type=jnp.float32,
    )
    taken = taken.reshape(segment, slots, quarter).astype(jnp.bfloat16)
    for s in range(subs):
        out[:, s] = taken


def expert_kernel(received, gate, up, down, out):
    subs, total, quarter = out.shape
    side = (((1,), (1,)), ((), ()))
    gate_act, up_act = 0.0, 0.0
    for s in range(subs):
        rows = received[:, s].reshape(total, quarter)
        cols = slice(s * quarter, (s + 1) * quarter)
        gate_act += lax.dot_general(rows, gate[:, cols], side, preferred_element_type=jnp.float32)
        up_act += lax.dot_general(rows, up[:, cols], side, preferred_element_type=jnp.float32)
    gated = (gate_act / (1.0 + jnp.exp(-gate_act)) * up_act).astype(jnp.bfloat16)
    for s in range(subs):
        cols = slice(s * quarter, (s + 1) * quarter)
        out[s] = jnp.dot(gated, down[:, cols], preferred_element_type=jnp.float32).astype(jnp.bfloat16)


def final_kernel(hidden_part, back, ids, weights, out, segment):
    tokens = ids.shape[0]
    slots = back.shape[0]
    fars = slots // (segment * CAP)
    col = lax.broadcasted_iota(jnp.int32, (1, slots), 1)
    expert = col // CAP % fars * segment + col // (CAP * fars)
    named = named_by(ids[...], expert)
    share = jnp.zeros((tokens, slots), jnp.float32)
    for k in range(TOP):
        share = jnp.where(ids[:, k : k + 1] == expert, weights[:, k : k + 1], share)
    lane = lax.broadcasted_iota(jnp.int32, (tokens, slots), 1)
    share = jnp.where(earlier_rows(named, tokens) == (lane % CAP).astype(jnp.float32), share, 0.0)
    routed = jnp.dot(share.astype(jnp.bfloat16), back[...], preferred_element_type=jnp.float32)
    out[...] = (hidden_part[...] + routed).astype(jnp.bfloat16)


def body(
    queries,
    latent_cache,
    cache_len,
    kv_up,
    o_weight,
    residual,
    norm_gain,
    route_ids,
    route_weights,
    w_gate,
    w_up,
    w_down,
):
    ctx_count = lax.axis_size(CTX)
    sub_count = lax.axis_size("sub")
    heads = kv_up.shape[0]
    tokens = queries.shape[0]
    width = heads * VDIM + EXTRA
    planes = ctx_count // 2

    smem = pl.BlockSpec(memory_space=pltpu.SMEM)
    vmem = pl.BlockSpec(memory_space=pltpu.VMEM)
    place = jnp.stack([lax.axis_index("core"), lax.axis_index("sub"), lax.axis_index("far")])
    cols = o_weight.shape[1]
    half = o_weight.shape[0] // 2
    ups = kv_up.transpose(0, 2, 1).reshape(-1, 256)
    taken = heads * (NOPE + ROPE) // 256 * tokens + ups.shape[0]
    packed, own_cache = pl.pallas_call(
        lambda *refs: pack_kernel(*refs, heads),
        out_shape=(
            jax.ShapeDtypeStruct((PAIR, taken + 2 * cols, 256), jnp.bfloat16),
            jax.ShapeDtypeStruct((latent_cache.shape[1] + 8, latent_cache.shape[0]), jnp.bfloat16),
        ),
        in_specs=[smem] + [pl.BlockSpec()] * 4,
        out_specs=(vmem, vmem),
        compiler_params=pltpu.CompilerParams(vmem_limit_bytes=8 * 2**20),
        name="pack",
    )(cache_len, queries, ups, o_weight.T, latent_cache.T)
    both = lax.all_to_all(packed, "pair", 0, 0, tiled=True)
    o_full = lax.all_gather(
        both[:, taken:].reshape(PAIR, 2, cols, half), ("far", "hop", "core"), axis=0, tiled=False
    )
    pair_cache = lax.ppermute(own_cache, "core", [(0, 1), (1, 0)])
    mine = lax.all_gather(both[:, :taken].reshape(PAIR * taken, 256), ("far", "hop"), axis=0, tiled=True)
    mine = mine.reshape(planes, taken, 256)
    other = lax.ppermute(mine, "core", [(0, 1), (1, 0)])

    fars = planes // NEAR
    rows = fars * tokens
    partial = pl.pallas_call(
        lambda *refs: attention_kernel(*refs, heads),
        out_shape=jax.ShapeDtypeStruct((NEAR, fars, tokens, width), jnp.bfloat16),
        in_specs=[smem, vmem, vmem, vmem, vmem],
        out_specs=vmem,
        compiler_params=pltpu.CompilerParams(vmem_limit_bytes=24 * 2**20),
        name="attention",
    )(place, mine, other, own_cache, pair_cache)
    segment = NEAR * 2
    partial = lax.all_to_all(partial.reshape(NEAR, rows, width), NEARBY, 0, 0, tiled=True)
    partial = pl.pallas_call(
        lambda *refs: merge_kernel(*refs, heads),
        out_shape=jax.ShapeDtypeStruct((rows, width), jnp.bfloat16),
        in_specs=[vmem],
        out_specs=vmem,
        compiler_params=pltpu.CompilerParams(vmem_limit_bytes=12 * 2**20),
        name="merge",
    )(partial)
    partial = lax.all_to_all(partial.reshape(fars, tokens, width), "far", 0, 0, tiled=True)
    projected = pl.pallas_call(
        lambda *refs: project_kernel(*refs, heads, o_weight.shape[1]),
        out_shape=jax.ShapeDtypeStruct((sub_count, tokens, D), jnp.bfloat16),
        in_specs=[vmem, vmem],
        out_specs=vmem,
        compiler_params=pltpu.CompilerParams(vmem_limit_bytes=12 * 2**20),
        name="project",
    )(partial, o_full)

    shares = lax.all_to_all(projected, "sub", 0, 0, tiled=True)
    quarter = D // sub_count
    blocks, hidden_part = pl.pallas_call(
        norm_kernel,
        out_shape=(
            jax.ShapeDtypeStruct((fars, tokens, quarter + EXTRA), jnp.bfloat16),
            jax.ShapeDtypeStruct((tokens, quarter), jnp.float32),
        ),
        in_specs=[smem, vmem, vmem, vmem, vmem],
        out_specs=(vmem, vmem),
        compiler_params=pltpu.CompilerParams(vmem_limit_bytes=8 * 2**20),
        name="norm",
    )(place, shares, residual, norm_gain.reshape(1, D), route_ids)
    blocks = lax.all_to_all(blocks, "far", 0, 0, tiled=True)
    rows = fars * CAP
    outgoing = pl.pallas_call(
        route_kernel,
        out_shape=jax.ShapeDtypeStruct((segment, sub_count, rows, quarter), jnp.bfloat16),
        in_specs=[smem, vmem],
        out_specs=vmem,
        compiler_params=pltpu.CompilerParams(vmem_limit_bytes=8 * 2**20),
        name="route",
    )(place, blocks)
    received = lax.all_to_all(
        outgoing.reshape(segment * sub_count, rows, quarter), (*SEGMENT, "sub"), 0, 0, tiled=True
    ).reshape(segment, sub_count, rows, quarter)
    partial_out = pl.pallas_call(
        expert_kernel,
        out_shape=jax.ShapeDtypeStruct((sub_count, segment * rows, quarter), jnp.bfloat16),
        in_specs=[vmem, vmem, vmem, vmem],
        out_specs=vmem,
        compiler_params=pltpu.CompilerParams(vmem_limit_bytes=16 * 2**20),
        name="experts",
    )(received, w_gate[0].T, w_up[0].T, w_down[0])
    parts = lax.all_to_all(partial_out, "sub", 0, 0, tiled=True)
    summed = jnp.sum(parts.astype(jnp.float32), axis=0).astype(jnp.bfloat16)
    summed = summed.reshape(ctx_count, CAP, quarter)
    back = lax.all_to_all(summed, (*SEGMENT, "far"), 0, 0, tiled=True)
    return pl.pallas_call(
        lambda *refs: final_kernel(*refs, segment),
        out_shape=jax.ShapeDtypeStruct((tokens, quarter), jnp.bfloat16),
        in_specs=[vmem] * 4,
        out_specs=vmem,
        compiler_params=pltpu.CompilerParams(vmem_limit_bytes=8 * 2**20),
        name="final",
    )(hidden_part, back.reshape(ctx_count * CAP, quarter), route_ids, route_weights)


def solution(mesh):
    planes = mesh.shape["ctx"] // 2
    split = Mesh(
        mesh.devices.reshape(mesh.shape["grp"], planes // NEAR, NEAR // PAIR, PAIR, 2, mesh.shape["sub"]),
        (*GRP_CTX, "sub"),
    )
    return jax.shard_map(
        body,
        mesh=split,
        in_specs=(
            P(GRP_CTX, "sub"),
            P(GRP_CTX, None),
            P(GRP_CTX),
            P(("grp", "sub"), None, CTX),
            P("sub", CTX),
            P(GRP_CTX, None),
            P(),
            P(GRP_CTX, None),
            P(GRP_CTX, None),
            P(CTX, None, "sub"),
            P(CTX, None, "sub"),
            P(CTX, "sub", None),
        ),
        out_specs=P(GRP_CTX, "sub"),
        check_vma=False,
    )
```

```python
import jax
import jax.numpy as jnp
from jax import lax
from jax.experimental import pallas as pl
from jax.experimental.pallas import tpu as pltpu
from jax.sharding import Mesh
from jax.sharding import PartitionSpec as P

D = 2048
NOPE = 128
ROPE = 64
VDIM = 128
LATENT = 512
TOP = 6
CAP = 2
NEAR = 4
PAIR = 2
NEARBY = ("hop", "pair")
CTX = ("far", "hop", "pair", "core")
GRP_CTX = ("grp", *CTX)
SEGMENT = ("hop", "pair", "core")
Z = ("far", "hop", "pair")
EXTRA = 128

epsilon = 1e-06


def thirds(x):
    high = x.astype(jnp.bfloat16)
    rest = x - high.astype(jnp.float32)
    middle = rest.astype(jnp.bfloat16)
    low = (rest - middle.astype(jnp.float32)).astype(jnp.bfloat16)
    return high.astype(jnp.float32), middle.astype(jnp.float32), low.astype(jnp.float32)


def log_block(logs, rows):
    lane = lax.broadcasted_iota(jnp.int32, (rows, EXTRA), 1)
    heads = len(logs)
    block = jnp.zeros((rows, EXTRA), jnp.float32)
    for h, x in enumerate(logs):
        for piece, part in enumerate(thirds(x)):
            block = jnp.where(lane == heads * piece + h, part, block)
    return block.astype(jnp.bfloat16)


def pack_kernel(length, queries, ups, o_rows, cache, packed, own_cache, heads):
    step = NOPE + ROPE
    per_row = 256 // NOPE
    half = o_rows.shape[1] // 2
    rows = []
    for r in range(heads // per_row):
        rows.append([queries[:, h * step : h * step + NOPE] for h in range(per_row * r, per_row * r + per_row)])
    rows.append([queries[:, h * step + NOPE : h * step + step] for h in range(heads)])
    parts = [jnp.concatenate(r, axis=1) for r in rows]
    parts += [ups[...], o_rows[:, :half], o_rows[:, half:]]
    for p in range(packed.shape[0]):
        at = 0
        for part in parts:
            packed[p, at : at + part.shape[0], :] = part
            at += part.shape[0]
    width = cache.shape[0]
    own_cache[:width, :] = cache[...]
    shape = (own_cache.shape[0] - width, cache.shape[1])
    live = lax.broadcasted_iota(jnp.int32, shape, 1) < length[0]
    own_cache[width:, :] = jnp.where(live, 1.0, 0.0).astype(jnp.bfloat16)


def attention_kernel(place, mine, other, own_cache, pair_cache, out, heads):
    planes = mine.shape[0]
    rows = planes * 8
    first = place[0] == 0
    scale = (NOPE + ROPE) ** (-0.5)
    per_row = 256 // NOPE
    q_rows = heads // per_row * 8
    kv_at = q_rows + 8
    caches = [(c[:LATENT, :], c[LATENT : LATENT + ROPE, :], c[LATENT + ROPE :, :]) for c in (own_cache, pair_cache)]
    logs, tops = [], []
    for h in range(heads):
        a = mine[:, kv_at + 8 * h : kv_at + 8 * h + 8, :]
        b = other[:, kv_at + 8 * h : kv_at + 8 * h + 8, :]
        up = jnp.stack([jnp.where(first, a, b), jnp.where(first, b, a)], axis=1)
        up = up.reshape(planes * 16, 256)
        at, lane = 8 * (h // per_row), NOPE * (h % per_row)
        nope = mine[:, at : at + 8, lane : lane + NOPE].reshape(rows, NOPE)
        rope = mine[:, q_rows : q_rows + 8, ROPE * h : ROPE * h + ROPE].reshape(rows, ROPE)
        absorbed = lax.dot_general(
            nope, up[:, :NOPE], (((1,), (1,)), ((), ())), preferred_element_type=jnp.float32
        ).astype(jnp.bfloat16)
        scores = []
        for latents, rotary, live in caches:
            score = jnp.dot(absorbed, latents, preferred_element_type=jnp.float32)
            score = (score + jnp.dot(rope, rotary, preferred_element_type=jnp.float32)) * scale
            scores.append(jnp.where(live[:1].astype(jnp.float32) > 0.5, score, -jnp.inf))
        highest = jnp.maximum(
            jnp.max(scores[0], axis=1, keepdims=True), jnp.max(scores[1], axis=1, keepdims=True)
        )
        total, mixed = 0.0, 0.0
        for score, (latents, _, _) in zip(scores, caches):
            weights = jnp.exp(score - highest).astype(jnp.bfloat16)
            total += jnp.sum(weights.astype(jnp.float32), axis=1, keepdims=True)
            mixed += lax.dot_general(
                weights, latents, (((1,), (1,)), ((), ())), preferred_element_type=jnp.float32
            )
        head = jnp.dot(mixed.astype(jnp.bfloat16), up[:, NOPE:], preferred_element_type=jnp.float32)
        tops.append((head / total).astype(jnp.bfloat16))
        logs.append(highest + jnp.log(total))
    result = jnp.concatenate([*tops, log_block(logs, rows)], axis=1)
    result = result.reshape(planes, 8, result.shape[1])
    for z in range(planes):
        out[z % NEAR, z // NEAR] = result[z]


def merged(parts, heads):
    sources, rows, _ = parts.shape
    width = heads * VDIM
    lane = lax.broadcasted_iota(jnp.int32, (EXTRA, width), 0)
    col = lax.broadcasted_iota(jnp.int32, (EXTRA, width), 1)
    spread = ((lane < 3 * heads) & (lane % heads == col // VDIM)).astype(jnp.bfloat16)
    packed = parts[:, :, width:].reshape(sources * rows, EXTRA)
    logs = jnp.dot(packed, spread, preferred_element_type=jnp.float32).reshape(sources, rows, width)
    top = jnp.max(logs, axis=0)
    shares = jnp.exp(logs - top[None])
    total = jnp.sum(shares, axis=0)
    mixed = jnp.sum(shares * parts[:, :, :width].astype(jnp.float32), axis=0)
    return mixed / total, top + jnp.log(total)


def merge_kernel(parts, out, heads):
    mixed, logs = merged(parts[...], heads)
    rows = mixed.shape[0]
    block = log_block([logs[:, VDIM * h : VDIM * h + EXTRA] for h in range(heads)], rows)
    out[...] = jnp.concatenate([mixed.astype(jnp.bfloat16), block], axis=1)


def project_kernel(parts, weight, out, heads, cols):
    mixed, _ = merged(parts[...], heads)
    size = 2 * PAIR * cols
    to = lax.broadcasted_iota(jnp.int32, (size, size), 1)
    source = to // cols % 2 * (PAIR * cols) + to // (2 * cols) * cols + to % cols
    turn = (lax.broadcasted_iota(jnp.int32, (size, size), 0) == source).astype(jnp.bfloat16)
    mixed = mixed.astype(jnp.bfloat16)
    half = weight.shape[4]
    projected = 0.0
    for k in range(2):
        rows = weight[:, :, k].reshape(-1, half)
        projected += lax.dot_general(
            mixed[:, k * half : k * half + half],
            rows,
            (((1,), (1,)), ((), ())),
            preferred_element_type=jnp.float32,
        )
    projected = projected.astype(jnp.bfloat16)
    for at in range(0, projected.shape[1], size):
        part = jnp.dot(projected[:, at : at + size], turn, preferred_element_type=jnp.float32).astype(jnp.bfloat16)
        for s in range(out.shape[0]):
            out[s, :, at : at + size] = part


def named_by(ids, expert):
    found = jnp.zeros((ids.shape[0], expert.shape[1]), jnp.float32)
    for k in range(TOP):
        found = jnp.where(ids[:, k : k + 1] == expert, 1.0, found)
    return found


def earlier_rows(named, tokens):
    rows = named.shape[0]
    r = lax.broadcasted_iota(jnp.int32, (rows, rows), 0)
    c = lax.broadcasted_iota(jnp.int32, (rows, rows), 1)
    before = ((r // tokens == c // tokens) & (c < r)).astype(jnp.bfloat16)
    return jnp.dot(before, named.astype(jnp.bfloat16), preferred_element_type=jnp.float32)


def norm_kernel(place, shares, residual, gain, ids, out, hidden_part):
    tokens = residual.shape[0]
    quarter = hidden_part.shape[1]
    hidden = residual[...].astype(jnp.float32) + jnp.sum(shares[...].astype(jnp.float32), axis=0)
    inverse_rms = lax.rsqrt(jnp.mean(hidden * hidden, axis=1, keepdims=True) + epsilon)
    own = pl.ds(pl.multiple_of(place[1] * quarter, quarter), quarter)
    part = residual[:, own].astype(jnp.float32) + jnp.sum(shares[:, :, own].astype(jnp.float32), axis=0)
    hidden_part[...] = part
    gains = gain[...].astype(jnp.float32)
    lanes = gains.shape[1]
    which = lax.broadcasted_iota(jnp.int32, gains.shape, 0) - place[1] * (quarter // lanes)
    own_gain = [
        jnp.sum(jnp.where(which == k, gains, 0.0), axis=0, keepdims=True) for k in range(quarter // lanes)
    ]
    normed = (part * inverse_rms * jnp.concatenate(own_gain, axis=1)).astype(jnp.bfloat16)
    lane = lax.broadcasted_iota(jnp.int32, (tokens, EXTRA), 1)
    named = jnp.zeros((tokens, EXTRA), jnp.float32)
    for k in range(TOP):
        named = jnp.where(lane == k, ids[:, k : k + 1].astype(jnp.float32), named)
    block = jnp.concatenate([normed, named.astype(jnp.bfloat16)], axis=1)
    for f in range(out.shape[0]):
        out[f] = block


def route_kernel(place, blocks, out):
    sources, tokens, width = blocks.shape
    segment, subs, slots, quarter = out.shape
    rows = sources * tokens
    ids = blocks[:, :, quarter:].astype(jnp.float32).reshape(rows, width - quarter)
    col = lax.broadcasted_iota(jnp.int32, (1, segment * slots), 1)
    expert = (place[2] * segment + col // slots).astype(jnp.float32)
    named = named_by(ids, expert)
    row = lax.broadcasted_iota(jnp.int32, (rows, segment * slots), 0)
    lane = lax.broadcasted_iota(jnp.int32, (rows, segment * slots), 1)
    right = (lane // CAP % sources == row // tokens) & (
        earlier_rows(named, tokens) == (lane % CAP).astype(jnp.float32)
    )
    chosen = jnp.where(right, named, 0.0)
    taken = lax.dot_general(
        chosen,
        blocks[:, :, :quarter].astype(jnp.float32).reshape(rows, quarter),
        (((0,), (0,)), ((), ())),
        preferred_element_type=jnp.float32,
    )
    taken = taken.reshape(segment, slots, quarter).astype(jnp.bfloat16)
    for s in range(subs):
        out[:, s] = taken


def expert_kernel(received, gate, up, down, out):
    subs, total, quarter = out.shape
    side = (((1,), (1,)), ((), ()))
    gate_act, up_act = 0.0, 0.0
    for s in range(subs):
        rows = received[:, s].reshape(total, quarter)
        cols = slice(s * quarter, (s + 1) * quarter)
        gate_act += lax.dot_general(rows, gate[:, cols], side, preferred_element_type=jnp.float32)
        up_act += lax.dot_general(rows, up[:, cols], side, preferred_element_type=jnp.float32)
    gated = (gate_act / (1.0 + jnp.exp(-gate_act)) * up_act).astype(jnp.bfloat16)
    for s in range(subs):
        cols = slice(s * quarter, (s + 1) * quarter)
        out[s] = jnp.dot(gated, down[:, cols], preferred_element_type=jnp.float32).astype(jnp.bfloat16)


def final_kernel(hidden_part, back, ids, weights, out, segment):
    tokens = ids.shape[0]
    slots = back.shape[0]
    fars = slots // (segment * CAP)
    col = lax.broadcasted_iota(jnp.int32, (1, slots), 1)
    expert = col // CAP % fars * segment + col // (CAP * fars)
    named = named_by(ids[...], expert)
    share = jnp.zeros((tokens, slots), jnp.float32)
    for k in range(TOP):
        share = jnp.where(ids[:, k : k + 1] == expert, weights[:, k : k + 1], share)
    lane = lax.broadcasted_iota(jnp.int32, (tokens, slots), 1)
    share = jnp.where(earlier_rows(named, tokens) == (lane % CAP).astype(jnp.float32), share, 0.0)
    routed = jnp.dot(share.astype(jnp.bfloat16), back[...], preferred_element_type=jnp.float32)
    out[...] = (hidden_part[...] + routed).astype(jnp.bfloat16)


def body(
    queries,
    latent_cache,
    cache_len,
    kv_up,
    o_weight,
    residual,
    norm_gain,
    route_ids,
    route_weights,
    w_gate,
    w_up,
    w_down,
):
    ctx_count = lax.axis_size(CTX)
    sub_count = lax.axis_size("sub")
    heads = kv_up.shape[0]
    tokens = queries.shape[0]
    width = heads * VDIM + EXTRA
    planes = ctx_count // 2

    smem = pl.BlockSpec(memory_space=pltpu.SMEM)
    vmem = pl.BlockSpec(memory_space=pltpu.VMEM)
    place = jnp.stack([lax.axis_index("core"), lax.axis_index("sub"), lax.axis_index("far")])
    cols = o_weight.shape[1]
    half = o_weight.shape[0] // 2
    ups = kv_up.transpose(0, 2, 1).reshape(-1, 256)
    taken = heads * (NOPE + ROPE) // 256 * tokens + ups.shape[0]
    packed, own_cache = pl.pallas_call(
        lambda *refs: pack_kernel(*refs, heads),
        out_shape=(
            jax.ShapeDtypeStruct((PAIR, taken + 2 * cols, 256), jnp.bfloat16),
            jax.ShapeDtypeStruct((latent_cache.shape[1] + 8, latent_cache.shape[0]), jnp.bfloat16),
        ),
        in_specs=[smem] + [pl.BlockSpec()] * 4,
        out_specs=(vmem, vmem),
        compiler_params=pltpu.CompilerParams(vmem_limit_bytes=8 * 2**20),
        name="pack",
    )(cache_len, queries, ups, o_weight.T, latent_cache.T)
    both = lax.all_to_all(packed, "pair", 0, 0, tiled=True)
    o_full = lax.all_gather(
        both[:, taken:].reshape(PAIR, 2, cols, half), ("far", "hop", "core"), axis=0, tiled=False
    )
    pair_cache = lax.ppermute(own_cache, "core", [(0, 1), (1, 0)])
    mine = lax.all_gather(both[:, :taken].reshape(PAIR * taken, 256), ("far", "hop"), axis=0, tiled=True)
    mine = mine.reshape(planes, taken, 256)
    other = lax.ppermute(mine, "core", [(0, 1), (1, 0)])

    fars = planes // NEAR
    rows = fars * tokens
    partial = pl.pallas_call(
        lambda *refs: attention_kernel(*refs, heads),
        out_shape=jax.ShapeDtypeStruct((NEAR, fars, tokens, width), jnp.bfloat16),
        in_specs=[smem, vmem, vmem, vmem, vmem],
        out_specs=vmem,
        compiler_params=pltpu.CompilerParams(vmem_limit_bytes=24 * 2**20),
        name="attention",
    )(place, mine, other, own_cache, pair_cache)
    segment = NEAR * 2
    partial = lax.all_to_all(partial.reshape(NEAR, rows, width), NEARBY, 0, 0, tiled=True)
    partial = pl.pallas_call(
        lambda *refs: merge_kernel(*refs, heads),
        out_shape=jax.ShapeDtypeStruct((rows, width), jnp.bfloat16),
        in_specs=[vmem],
        out_specs=vmem,
        compiler_params=pltpu.CompilerParams(vmem_limit_bytes=12 * 2**20),
        name="merge",
    )(partial)
    partial = lax.all_to_all(partial.reshape(fars, tokens, width), "far", 0, 0, tiled=True)
    projected = pl.pallas_call(
        lambda *refs: project_kernel(*refs, heads, o_weight.shape[1]),
        out_shape=jax.ShapeDtypeStruct((sub_count, tokens, D), jnp.bfloat16),
        in_specs=[vmem, vmem],
        out_specs=vmem,
        compiler_params=pltpu.CompilerParams(vmem_limit_bytes=12 * 2**20),
        name="project",
    )(partial, o_full)

    shares = lax.all_to_all(projected, "sub", 0, 0, tiled=True)
    quarter = D // sub_count
    blocks, hidden_part = pl.pallas_call(
        norm_kernel,
        out_shape=(
            jax.ShapeDtypeStruct((fars, tokens, quarter + EXTRA), jnp.bfloat16),
            jax.ShapeDtypeStruct((tokens, quarter), jnp.float32),
        ),
        in_specs=[smem, vmem, vmem, vmem, vmem],
        out_specs=(vmem, vmem),
        compiler_params=pltpu.CompilerParams(vmem_limit_bytes=8 * 2**20),
        name="norm",
    )(place, shares, residual, norm_gain.reshape(D // 128, 128), route_ids)
    blocks = lax.all_to_all(blocks, "far", 0, 0, tiled=True)
    rows = fars * CAP
    outgoing = pl.pallas_call(
        route_kernel,
        out_shape=jax.ShapeDtypeStruct((segment, sub_count, rows, quarter), jnp.bfloat16),
        in_specs=[smem, vmem],
        out_specs=vmem,
        compiler_params=pltpu.CompilerParams(vmem_limit_bytes=8 * 2**20),
        name="route",
    )(place, blocks)
    received = lax.all_to_all(
        outgoing.reshape(segment * sub_count, rows, quarter), (*SEGMENT, "sub"), 0, 0, tiled=True
    ).reshape(segment, sub_count, rows, quarter)
    partial_out = pl.pallas_call(
        expert_kernel,
        out_shape=jax.ShapeDtypeStruct((sub_count, segment * rows, quarter), jnp.bfloat16),
        in_specs=[vmem, vmem, vmem, vmem],
        out_specs=vmem,
        compiler_params=pltpu.CompilerParams(vmem_limit_bytes=16 * 2**20),
        name="experts",
    )(received, w_gate[0].T, w_up[0].T, w_down[0])
    parts = lax.all_to_all(partial_out, "sub", 0, 0, tiled=True)
    summed = jnp.sum(parts.astype(jnp.float32), axis=0).astype(jnp.bfloat16)
    summed = summed.reshape(ctx_count, CAP, quarter)
    back = lax.all_to_all(summed, (*SEGMENT, "far"), 0, 0, tiled=True)
    return pl.pallas_call(
        lambda *refs: final_kernel(*refs, segment),
        out_shape=jax.ShapeDtypeStruct((tokens, quarter), jnp.bfloat16),
        in_specs=[vmem] * 4,
        out_specs=vmem,
        compiler_params=pltpu.CompilerParams(vmem_limit_bytes=8 * 2**20),
        name="final",
    )(hidden_part, back.reshape(ctx_count * CAP, quarter), route_ids, route_weights)


def solution(mesh):
    planes = mesh.shape["ctx"] // 2
    split = Mesh(
        mesh.devices.reshape(mesh.shape["grp"], planes // NEAR, NEAR // PAIR, PAIR, 2, mesh.shape["sub"]),
        (*GRP_CTX, "sub"),
    )
    return jax.shard_map(
        body,
        mesh=split,
        in_specs=(
            P(GRP_CTX, "sub"),
            P(GRP_CTX, None),
            P(GRP_CTX),
            P(("grp", "sub"), None, CTX),
            P("sub", CTX),
            P(GRP_CTX, None),
            P(),
            P(GRP_CTX, None),
            P(GRP_CTX, None),
            P(CTX, None, "sub"),
            P(CTX, None, "sub"),
            P(CTX, "sub", None),
        ),
        out_specs=P(GRP_CTX, "sub"),
        check_vma=False,
    )
```

```python
import jax
import jax.numpy as jnp
from jax import lax
from jax.experimental import pallas as pl
from jax.experimental.pallas import tpu as pltpu
from jax.sharding import Mesh
from jax.sharding import PartitionSpec as P

D = 2048
NOPE = 128
ROPE = 64
VDIM = 128
LATENT = 512
TOP = 6
CAP = 2
NEAR = 4
PAIR = 2
NEARBY = ("hop", "pair")
CTX = ("far", "hop", "pair", "core")
GRP_CTX = ("grp", *CTX)
SEGMENT = ("hop", "pair", "core")
Z = ("far", "hop", "pair")
EXTRA = 128

epsilon = 1e-06


def thirds(x):
    high = x.astype(jnp.bfloat16)
    rest = x - high.astype(jnp.float32)
    middle = rest.astype(jnp.bfloat16)
    low = (rest - middle.astype(jnp.float32)).astype(jnp.bfloat16)
    return high.astype(jnp.float32), middle.astype(jnp.float32), low.astype(jnp.float32)


def log_block(logs, rows):
    lane = lax.broadcasted_iota(jnp.int32, (rows, EXTRA), 1)
    heads = len(logs)
    block = jnp.zeros((rows, EXTRA), jnp.float32)
    for h, x in enumerate(logs):
        for piece, part in enumerate(thirds(x)):
            block = jnp.where(lane == heads * piece + h, part, block)
    return block.astype(jnp.bfloat16)


def pack_kernel(queries, ups, o_rows, packed, heads):
    step = NOPE + ROPE
    per_row = 256 // NOPE
    half = o_rows.shape[1] // 2
    rows = []
    for r in range(heads // per_row):
        rows.append([queries[:, h * step : h * step + NOPE] for h in range(per_row * r, per_row * r + per_row)])
    rows.append([queries[:, h * step + NOPE : h * step + step] for h in range(heads)])
    parts = [jnp.concatenate(r, axis=1) for r in rows]
    parts += [ups[...], o_rows[:, :half], o_rows[:, half:]]
    at = 0
    for part in parts:
        packed[at : at + part.shape[0], :] = part
        at += part.shape[0]


def attention_kernel(place, mine, other, both, out, heads):
    planes = mine.shape[0]
    rows = planes * 8
    first = place[0] == 0
    scale = (NOPE + ROPE) ** (-0.5)
    per_row = 256 // NOPE
    q_rows = heads // per_row * 8
    kv_at = q_rows + 8
    caches = [(both[c, :LATENT, :], both[c, LATENT : LATENT + ROPE, :], both[c, LATENT + ROPE :, :]) for c in (0, 1)]
    logs, tops = [], []
    for h in range(heads):
        a = mine[:, kv_at + 8 * h : kv_at + 8 * h + 8, :]
        b = other[:, kv_at + 8 * h : kv_at + 8 * h + 8, :]
        up = jnp.stack([jnp.where(first, a, b), jnp.where(first, b, a)], axis=1)
        up = up.reshape(planes * 16, 256)
        at, lane = 8 * (h // per_row), NOPE * (h % per_row)
        nope = mine[:, at : at + 8, lane : lane + NOPE].reshape(rows, NOPE)
        rope = mine[:, q_rows : q_rows + 8, ROPE * h : ROPE * h + ROPE].reshape(rows, ROPE)
        absorbed = lax.dot_general(
            nope, up[:, :NOPE], (((1,), (1,)), ((), ())), preferred_element_type=jnp.float32
        ).astype(jnp.bfloat16)
        scores = []
        for latents, rotary, live in caches:
            score = jnp.dot(absorbed, latents, preferred_element_type=jnp.float32)
            score = (score + jnp.dot(rope, rotary, preferred_element_type=jnp.float32)) * scale
            scores.append(jnp.where(live[:1].astype(jnp.float32) > 0.5, score, -jnp.inf))
        highest = jnp.maximum(
            jnp.max(scores[0], axis=1, keepdims=True), jnp.max(scores[1], axis=1, keepdims=True)
        )
        total, mixed = 0.0, 0.0
        for score, (latents, _, _) in zip(scores, caches):
            weights = jnp.exp(score - highest).astype(jnp.bfloat16)
            total += jnp.sum(weights.astype(jnp.float32), axis=1, keepdims=True)
            mixed += lax.dot_general(
                weights, latents, (((1,), (1,)), ((), ())), preferred_element_type=jnp.float32
            )
        head = jnp.dot(mixed.astype(jnp.bfloat16), up[:, NOPE:], preferred_element_type=jnp.float32)
        tops.append((head / total).astype(jnp.bfloat16))
        logs.append(highest + jnp.log(total))
    result = jnp.concatenate([*tops, log_block(logs, rows)], axis=1)
    result = result.reshape(planes, 8, result.shape[1])
    for z in range(planes):
        out[z % NEAR, z // NEAR] = result[z]


def merged(parts, heads):
    sources, rows, _ = parts.shape
    width = heads * VDIM
    lane = lax.broadcasted_iota(jnp.int32, (EXTRA, width), 0)
    col = lax.broadcasted_iota(jnp.int32, (EXTRA, width), 1)
    spread = ((lane < 3 * heads) & (lane % heads == col // VDIM)).astype(jnp.bfloat16)
    packed = parts[:, :, width:].reshape(sources * rows, EXTRA)
    logs = jnp.dot(packed, spread, preferred_element_type=jnp.float32).reshape(sources, rows, width)
    top = jnp.max(logs, axis=0)
    shares = jnp.exp(logs - top[None])
    total = jnp.sum(shares, axis=0)
    mixed = jnp.sum(shares * parts[:, :, :width].astype(jnp.float32), axis=0)
    return mixed / total, top + jnp.log(total)


def merge_kernel(parts, out, heads):
    mixed, logs = merged(parts[...], heads)
    rows = mixed.shape[0]
    block = log_block([logs[:, VDIM * h : VDIM * h + EXTRA] for h in range(heads)], rows)
    out[...] = jnp.concatenate([mixed.astype(jnp.bfloat16), block], axis=1)


def project_kernel(parts, weight, out, heads, cols):
    mixed, _ = merged(parts[...], heads)
    size = 2 * PAIR * cols
    to = lax.broadcasted_iota(jnp.int32, (size, size), 1)
    source = to // cols % 2 * (PAIR * cols) + to // (2 * cols) * cols + to % cols
    turn = (lax.broadcasted_iota(jnp.int32, (size, size), 0) == source).astype(jnp.bfloat16)
    mixed = mixed.astype(jnp.bfloat16)
    half = weight.shape[4]
    projected = 0.0
    for k in range(2):
        rows = weight[:, :, k].reshape(-1, half)
        projected += lax.dot_general(
            mixed[:, k * half : k * half + half],
            rows,
            (((1,), (1,)), ((), ())),
            preferred_element_type=jnp.float32,
        )
    projected = projected.astype(jnp.bfloat16)
    for at in range(0, projected.shape[1], size):
        part = jnp.dot(projected[:, at : at + size], turn, preferred_element_type=jnp.float32).astype(jnp.bfloat16)
        for s in range(out.shape[0]):
            out[s, :, at : at + size] = part


def named_by(ids, expert):
    found = jnp.zeros((ids.shape[0], expert.shape[1]), jnp.float32)
    for k in range(TOP):
        found = jnp.where(ids[:, k : k + 1] == expert, 1.0, found)
    return found


def earlier_rows(named, tokens):
    rows = named.shape[0]
    r = lax.broadcasted_iota(jnp.int32, (rows, rows), 0)
    c = lax.broadcasted_iota(jnp.int32, (rows, rows), 1)
    before = ((r // tokens == c // tokens) & (c < r)).astype(jnp.bfloat16)
    return jnp.dot(before, named.astype(jnp.bfloat16), preferred_element_type=jnp.float32)


def norm_kernel(place, shares, residual, gain, ids, out, hidden_part):
    tokens = residual.shape[0]
    quarter = hidden_part.shape[1]
    hidden = residual[...].astype(jnp.float32) + jnp.sum(shares[...].astype(jnp.float32), axis=0)
    inverse_rms = lax.rsqrt(jnp.mean(hidden * hidden, axis=1, keepdims=True) + epsilon)
    own = pl.ds(pl.multiple_of(place[1] * quarter, quarter), quarter)
    part = residual[:, own].astype(jnp.float32) + jnp.sum(shares[:, :, own].astype(jnp.float32), axis=0)
    hidden_part[...] = part
    gains = gain[...].astype(jnp.float32)
    lanes = gains.shape[1]
    which = lax.broadcasted_iota(jnp.int32, gains.shape, 0) - place[1] * (quarter // lanes)
    own_gain = [
        jnp.sum(jnp.where(which == k, gains, 0.0), axis=0, keepdims=True) for k in range(quarter // lanes)
    ]
    normed = (part * inverse_rms * jnp.concatenate(own_gain, axis=1)).astype(jnp.bfloat16)
    lane = lax.broadcasted_iota(jnp.int32, (tokens, EXTRA), 1)
    named = jnp.zeros((tokens, EXTRA), jnp.float32)
    for k in range(TOP):
        named = jnp.where(lane == k, ids[:, k : k + 1].astype(jnp.float32), named)
    block = jnp.concatenate([normed, named.astype(jnp.bfloat16)], axis=1)
    for f in range(out.shape[0]):
        out[f] = block


def route_kernel(place, blocks, out):
    sources, tokens, width = blocks.shape
    segment, subs, slots, quarter = out.shape
    rows = sources * tokens
    ids = blocks[:, :, quarter:].astype(jnp.float32).reshape(rows, width - quarter)
    col = lax.broadcasted_iota(jnp.int32, (1, segment * slots), 1)
    expert = (place[2] * segment + col // slots).astype(jnp.float32)
    named = named_by(ids, expert)
    row = lax.broadcasted_iota(jnp.int32, (rows, segment * slots), 0)
    lane = lax.broadcasted_iota(jnp.int32, (rows, segment * slots), 1)
    right = (lane // CAP % sources == row // tokens) & (
        earlier_rows(named, tokens) == (lane % CAP).astype(jnp.float32)
    )
    chosen = jnp.where(right, named, 0.0).astype(jnp.bfloat16)
    taken = lax.dot_general(
        chosen,
        blocks[:, :, :quarter].reshape(rows, quarter),
        (((0,), (0,)), ((), ())),
        preferred_element_type=jnp.float32,
    )
    taken = taken.reshape(segment, slots, quarter).astype(jnp.bfloat16)
    for s in range(subs):
        out[:, s] = taken


def expert_kernel(received, gate, up, down, out):
    subs, total, quarter = out.shape
    side = (((1,), (1,)), ((), ()))
    gate_act, up_act = 0.0, 0.0
    for s in range(subs):
        rows = received[:, s].reshape(total, quarter)
        cols = slice(s * quarter, (s + 1) * quarter)
        gate_act += lax.dot_general(rows, gate[:, cols], side, preferred_element_type=jnp.float32)
        up_act += lax.dot_general(rows, up[:, cols], side, preferred_element_type=jnp.float32)
    gated = (gate_act / (1.0 + jnp.exp(-gate_act)) * up_act).astype(jnp.bfloat16)
    for s in range(subs):
        cols = slice(s * quarter, (s + 1) * quarter)
        out[s] = jnp.dot(gated, down[:, cols], preferred_element_type=jnp.float32).astype(jnp.bfloat16)


def final_kernel(hidden_part, back, ids, weights, out, segment):
    tokens = ids.shape[0]
    slots = back.shape[0]
    fars = slots // (segment * CAP)
    col = lax.broadcasted_iota(jnp.int32, (1, slots), 1)
    expert = col // CAP % fars * segment + col // (CAP * fars)
    named = named_by(ids[...], expert)
    share = jnp.zeros((tokens, slots), jnp.float32)
    for k in range(TOP):
        share = jnp.where(ids[:, k : k + 1] == expert, weights[:, k : k + 1], share)
    lane = lax.broadcasted_iota(jnp.int32, (tokens, slots), 1)
    share = jnp.where(earlier_rows(named, tokens) == (lane % CAP).astype(jnp.float32), share, 0.0)
    routed = jnp.dot(share.astype(jnp.bfloat16), back[...], preferred_element_type=jnp.float32)
    out[...] = (hidden_part[...] + routed).astype(jnp.bfloat16)


def body(
    queries,
    latent_cache,
    cache_len,
    kv_up,
    o_weight,
    residual,
    norm_gain,
    route_ids,
    route_weights,
    w_gate,
    w_up,
    w_down,
):
    ctx_count = lax.axis_size(CTX)
    sub_count = lax.axis_size("sub")
    heads = kv_up.shape[0]
    tokens = queries.shape[0]
    width = heads * VDIM + EXTRA
    planes = ctx_count // 2

    smem = pl.BlockSpec(memory_space=pltpu.SMEM)
    vmem = pl.BlockSpec(memory_space=pltpu.VMEM)
    place = jnp.stack([lax.axis_index("core"), lax.axis_index("sub"), lax.axis_index("far")])
    cols = o_weight.shape[1]
    half = o_weight.shape[0] // 2
    ups = kv_up.transpose(0, 2, 1).reshape(-1, 256)
    taken = heads * (NOPE + ROPE) // 256 * tokens + ups.shape[0]
    packed = pl.pallas_call(
        lambda *refs: pack_kernel(*refs, heads),
        out_shape=jax.ShapeDtypeStruct((taken + 2 * cols, 256), jnp.bfloat16),
        in_specs=[vmem] * 3,
        out_specs=vmem,
        compiler_params=pltpu.CompilerParams(vmem_limit_bytes=8 * 2**20),
        name="pack",
    )(queries, ups, o_weight.T)
    both = lax.all_gather(packed, "pair", axis=0, tiled=False)
    o_full = lax.all_gather(
        both[:, taken:].reshape(PAIR, 2, cols, half), ("far", "hop", "core"), axis=0, tiled=False
    )
    live = lax.broadcasted_iota(jnp.int32, (8, latent_cache.shape[0]), 1) < cache_len[0]
    own_cache = jnp.concatenate([latent_cache.T, live.astype(jnp.bfloat16)], axis=0)
    caches = lax.all_gather(own_cache, "core", axis=0, tiled=False)
    mine = lax.all_gather(both[:, :taken].reshape(PAIR * taken, 256), ("far", "hop"), axis=0, tiled=True)
    mine = mine.reshape(planes, taken, 256)
    other = lax.ppermute(mine, "core", [(0, 1), (1, 0)])

    fars = planes // NEAR
    rows = fars * tokens
    partial = pl.pallas_call(
        lambda *refs: attention_kernel(*refs, heads),
        out_shape=jax.ShapeDtypeStruct((NEAR, fars, tokens, width), jnp.bfloat16),
        in_specs=[smem, vmem, vmem, vmem],
        out_specs=vmem,
        compiler_params=pltpu.CompilerParams(vmem_limit_bytes=24 * 2**20),
        name="attention",
    )(place, mine, other, caches)
    segment = NEAR * 2
    partial = lax.all_to_all(partial.reshape(NEAR, rows, width), NEARBY, 0, 0, tiled=True)
    partial = pl.pallas_call(
        lambda *refs: merge_kernel(*refs, heads),
        out_shape=jax.ShapeDtypeStruct((rows, width), jnp.bfloat16),
        in_specs=[vmem],
        out_specs=vmem,
        compiler_params=pltpu.CompilerParams(vmem_limit_bytes=12 * 2**20),
        name="merge",
    )(partial)
    partial = lax.all_to_all(partial.reshape(fars, tokens, width), "far", 0, 0, tiled=True)
    projected = pl.pallas_call(
        lambda *refs: project_kernel(*refs, heads, o_weight.shape[1]),
        out_shape=jax.ShapeDtypeStruct((sub_count, tokens, D), jnp.bfloat16),
        in_specs=[vmem, vmem],
        out_specs=vmem,
        compiler_params=pltpu.CompilerParams(vmem_limit_bytes=12 * 2**20),
        name="project",
    )(partial, o_full)

    shares = lax.all_to_all(projected, "sub", 0, 0, tiled=True)
    quarter = D // sub_count
    blocks, hidden_part = pl.pallas_call(
        norm_kernel,
        out_shape=(
            jax.ShapeDtypeStruct((fars, tokens, quarter + EXTRA), jnp.bfloat16),
            jax.ShapeDtypeStruct((tokens, quarter), jnp.float32),
        ),
        in_specs=[smem, vmem, vmem, vmem, vmem],
        out_specs=(vmem, vmem),
        compiler_params=pltpu.CompilerParams(vmem_limit_bytes=8 * 2**20),
        name="norm",
    )(place, shares, residual, norm_gain.reshape(D // 128, 128), route_ids)
    blocks = lax.all_to_all(blocks, "far", 0, 0, tiled=True)
    rows = fars * CAP
    outgoing = pl.pallas_call(
        route_kernel,
        out_shape=jax.ShapeDtypeStruct((segment, sub_count, rows, quarter), jnp.bfloat16),
        in_specs=[smem, vmem],
        out_specs=vmem,
        compiler_params=pltpu.CompilerParams(vmem_limit_bytes=8 * 2**20),
        name="route",
    )(place, blocks)
    received = lax.all_to_all(
        outgoing.reshape(segment * sub_count, rows, quarter), (*SEGMENT, "sub"), 0, 0, tiled=True
    ).reshape(segment, sub_count, rows, quarter)
    partial_out = pl.pallas_call(
        expert_kernel,
        out_shape=jax.ShapeDtypeStruct((sub_count, segment * rows, quarter), jnp.bfloat16),
        in_specs=[vmem, vmem, vmem, vmem],
        out_specs=vmem,
        compiler_params=pltpu.CompilerParams(vmem_limit_bytes=16 * 2**20),
        name="experts",
    )(received, w_gate[0].T, w_up[0].T, w_down[0])
    parts = lax.all_to_all(partial_out, "sub", 0, 0, tiled=True)
    summed = jnp.sum(parts.astype(jnp.float32), axis=0).astype(jnp.bfloat16)
    summed = summed.reshape(ctx_count, CAP, quarter)
    back = lax.all_to_all(summed, (*SEGMENT, "far"), 0, 0, tiled=True)
    return pl.pallas_call(
        lambda *refs: final_kernel(*refs, segment),
        out_shape=jax.ShapeDtypeStruct((tokens, quarter), jnp.bfloat16),
        in_specs=[vmem] * 4,
        out_specs=vmem,
        compiler_params=pltpu.CompilerParams(vmem_limit_bytes=8 * 2**20),
        name="final",
    )(hidden_part, back.reshape(ctx_count * CAP, quarter), route_ids, route_weights)


def solution(mesh):
    planes = mesh.shape["ctx"] // 2
    split = Mesh(
        mesh.devices.reshape(mesh.shape["grp"], planes // NEAR, NEAR // PAIR, PAIR, 2, mesh.shape["sub"]),
        (*GRP_CTX, "sub"),
    )
    return jax.shard_map(
        body,
        mesh=split,
        in_specs=(
            P(GRP_CTX, "sub"),
            P(GRP_CTX, None),
            P(GRP_CTX),
            P(("grp", "sub"), None, CTX),
            P("sub", CTX),
            P(GRP_CTX, None),
            P(),
            P(GRP_CTX, None),
            P(GRP_CTX, None),
            P(CTX, None, "sub"),
            P(CTX, None, "sub"),
            P(CTX, "sub", None),
        ),
        out_specs=P(GRP_CTX, "sub"),
        check_vma=False,
    )
```

```python
import jax
import jax.numpy as jnp
from jax import lax
from jax.experimental import pallas as pl
from jax.experimental.pallas import tpu as pltpu
from jax.sharding import Mesh
from jax.sharding import PartitionSpec as P

D = 2048
NOPE = 128
ROPE = 64
VDIM = 128
LATENT = 512
TOP = 6
CAP = 2
NEAR = 4
PAIR = 2
NEARBY = ("hop", "pair")
CTX = ("far", "hop", "pair", "core")
GRP_CTX = ("grp", *CTX)
Z = ("far", "hop", "pair")
EXTRA = 128

epsilon = 1e-06


def thirds(x):
    high = x.astype(jnp.bfloat16)
    rest = x - high.astype(jnp.float32)
    middle = rest.astype(jnp.bfloat16)
    low = (rest - middle.astype(jnp.float32)).astype(jnp.bfloat16)
    return high.astype(jnp.float32), middle.astype(jnp.float32), low.astype(jnp.float32)


def log_block(logs, rows):
    lane = lax.broadcasted_iota(jnp.int32, (rows, EXTRA), 1)
    heads = len(logs)
    block = jnp.zeros((rows, EXTRA), jnp.float32)
    for h, x in enumerate(logs):
        for piece, part in enumerate(thirds(x)):
            block = jnp.where(lane == heads * piece + h, part, block)
    return block.astype(jnp.bfloat16)


def pack_kernel(queries, ups, o_rows, packed, heads):
    step = NOPE + ROPE
    per_row = 256 // NOPE
    half = o_rows.shape[1] // 2
    rows = []
    for r in range(heads // per_row):
        rows.append([queries[:, h * step : h * step + NOPE] for h in range(per_row * r, per_row * r + per_row)])
    rows.append([queries[:, h * step + NOPE : h * step + step] for h in range(heads)])
    parts = [jnp.concatenate(r, axis=1) for r in rows]
    parts += [ups[...], o_rows[:, :half], o_rows[:, half:]]
    at = 0
    for part in parts:
        packed[at : at + part.shape[0], :] = part
        at += part.shape[0]


def attention_kernel(place, mine, other, both, out, heads):
    planes = mine.shape[0]
    rows = planes * 8
    first = place[0] == 0
    scale = (NOPE + ROPE) ** (-0.5)
    per_row = 256 // NOPE
    q_rows = heads // per_row * 8
    kv_at = q_rows + 8
    caches = [(both[c, :LATENT, :], both[c, LATENT : LATENT + ROPE, :], both[c, LATENT + ROPE :, :]) for c in (0, 1)]
    logs, tops = [], []
    for h in range(heads):
        a = mine[:, kv_at + 8 * h : kv_at + 8 * h + 8, :]
        b = other[:, kv_at + 8 * h : kv_at + 8 * h + 8, :]
        up = jnp.stack([jnp.where(first, a, b), jnp.where(first, b, a)], axis=1)
        up = up.reshape(planes * 16, 256)
        at, lane = 8 * (h // per_row), NOPE * (h % per_row)
        nope = mine[:, at : at + 8, lane : lane + NOPE].reshape(rows, NOPE)
        rope = mine[:, q_rows : q_rows + 8, ROPE * h : ROPE * h + ROPE].reshape(rows, ROPE)
        absorbed = lax.dot_general(
            nope, up[:, :NOPE], (((1,), (1,)), ((), ())), preferred_element_type=jnp.float32
        ).astype(jnp.bfloat16)
        scores = []
        for latents, rotary, live in caches:
            score = jnp.dot(absorbed, latents, preferred_element_type=jnp.float32)
            score = (score + jnp.dot(rope, rotary, preferred_element_type=jnp.float32)) * scale
            scores.append(jnp.where(live[:1].astype(jnp.float32) > 0.5, score, -jnp.inf))
        highest = jnp.maximum(
            jnp.max(scores[0], axis=1, keepdims=True), jnp.max(scores[1], axis=1, keepdims=True)
        )
        total, mixed = 0.0, 0.0
        for score, (latents, _, _) in zip(scores, caches):
            weights = jnp.exp(score - highest).astype(jnp.bfloat16)
            total += jnp.sum(weights.astype(jnp.float32), axis=1, keepdims=True)
            mixed += lax.dot_general(
                weights, latents, (((1,), (1,)), ((), ())), preferred_element_type=jnp.float32
            )
        head = jnp.dot(mixed.astype(jnp.bfloat16), up[:, NOPE:], preferred_element_type=jnp.float32)
        tops.append((head / total).astype(jnp.bfloat16))
        logs.append(highest + jnp.log(total))
    result = jnp.concatenate([*tops, log_block(logs, rows)], axis=1)
    result = result.reshape(planes, 8, result.shape[1])
    for z in range(planes):
        out[z % NEAR, z // NEAR] = result[z]


def merged(parts, heads):
    sources, rows, _ = parts.shape
    width = heads * VDIM
    lane = lax.broadcasted_iota(jnp.int32, (EXTRA, width), 0)
    col = lax.broadcasted_iota(jnp.int32, (EXTRA, width), 1)
    spread = ((lane < 3 * heads) & (lane % heads == col // VDIM)).astype(jnp.bfloat16)
    packed = parts[:, :, width:].reshape(sources * rows, EXTRA)
    logs = jnp.dot(packed, spread, preferred_element_type=jnp.float32).reshape(sources, rows, width)
    top = jnp.max(logs, axis=0)
    shares = jnp.exp(logs - top[None])
    total = jnp.sum(shares, axis=0)
    mixed = jnp.sum(shares * parts[:, :, :width].astype(jnp.float32), axis=0)
    return mixed / total, top + jnp.log(total)


def merge_kernel(parts, out, heads):
    mixed, logs = merged(parts[...], heads)
    rows = mixed.shape[0]
    block = log_block([logs[:, VDIM * h : VDIM * h + EXTRA] for h in range(heads)], rows)
    out[...] = jnp.concatenate([mixed.astype(jnp.bfloat16), block], axis=1)


def project_kernel(parts, weight, out, heads, cols):
    mixed, _ = merged(parts[...], heads)
    size = 2 * PAIR * cols
    to = lax.broadcasted_iota(jnp.int32, (size, size), 1)
    source = to // cols % 2 * (PAIR * cols) + to // (2 * cols) * cols + to % cols
    turn = (lax.broadcasted_iota(jnp.int32, (size, size), 0) == source).astype(jnp.bfloat16)
    mixed = mixed.astype(jnp.bfloat16)
    half = weight.shape[4]
    projected = 0.0
    for k in range(2):
        rows = weight[:, :, k].reshape(-1, half)
        projected += lax.dot_general(
            mixed[:, k * half : k * half + half],
            rows,
            (((1,), (1,)), ((), ())),
            preferred_element_type=jnp.float32,
        )
    projected = projected.astype(jnp.bfloat16)
    for at in range(0, projected.shape[1], size):
        part = jnp.dot(projected[:, at : at + size], turn, preferred_element_type=jnp.float32).astype(jnp.bfloat16)
        for s in range(out.shape[0]):
            out[s, :, at : at + size] = part


def picked(ids, slots, weights=None):
    tokens = ids.shape[0]
    lane = lax.broadcasted_iota(jnp.int32, (tokens, slots), 1)
    named = jnp.zeros((tokens, slots), jnp.float32)
    share = named
    for k in range(TOP):
        same = ids[:, k : k + 1] == lane // CAP
        named = jnp.where(same, 1.0, named)
        share = jnp.where(same, 1.0 if weights is None else weights[:, k : k + 1], share)
    r = lax.broadcasted_iota(jnp.int32, (tokens, tokens), 0)
    c = lax.broadcasted_iota(jnp.int32, (tokens, tokens), 1)
    earlier = jnp.dot(
        (c < r).astype(jnp.bfloat16), named.astype(jnp.bfloat16), preferred_element_type=jnp.float32
    )
    return jnp.where(earlier == (lane % CAP).astype(jnp.float32), share, 0.0)


def norm_kernel(place, shares, residual, gain, ids, out, hidden_part):
    tokens = residual.shape[0]
    quarter = hidden_part.shape[1]
    hidden = residual[...].astype(jnp.float32) + jnp.sum(shares[...].astype(jnp.float32), axis=0)
    inverse_rms = lax.rsqrt(jnp.mean(hidden * hidden, axis=1, keepdims=True) + epsilon)
    own = pl.ds(pl.multiple_of(place[1] * quarter, quarter), quarter)
    part = residual[:, own].astype(jnp.float32) + jnp.sum(shares[:, :, own].astype(jnp.float32), axis=0)
    hidden_part[...] = part
    gains = gain[...].astype(jnp.float32)
    lanes = gains.shape[1]
    which = lax.broadcasted_iota(jnp.int32, gains.shape, 0) - place[1] * (quarter // lanes)
    own_gain = [
        jnp.sum(jnp.where(which == k, gains, 0.0), axis=0, keepdims=True) for k in range(quarter // lanes)
    ]
    normed = (part * inverse_rms * jnp.concatenate(own_gain, axis=1)).astype(jnp.bfloat16)
    out[...] = lax.dot_general(
        picked(ids[...], out.shape[0]).astype(jnp.bfloat16),
        normed,
        (((0,), (0,)), ((), ())),
        preferred_element_type=jnp.float32,
    ).astype(jnp.bfloat16)


def expert_kernel(received, gate, up, down, out):
    subs, _, quarter = out.shape
    side = (((1,), (1,)), ((), ()))
    gate_act, up_act = 0.0, 0.0
    for s in range(subs):
        rows = received[s]
        cols = slice(s * quarter, (s + 1) * quarter)
        gate_act += lax.dot_general(rows, gate[:, cols], side, preferred_element_type=jnp.float32)
        up_act += lax.dot_general(rows, up[:, cols], side, preferred_element_type=jnp.float32)
    gated = (gate_act / (1.0 + jnp.exp(-gate_act)) * up_act).astype(jnp.bfloat16)
    for s in range(subs):
        cols = slice(s * quarter, (s + 1) * quarter)
        out[s] = jnp.dot(gated, down[:, cols], preferred_element_type=jnp.float32).astype(jnp.bfloat16)


def final_kernel(hidden_part, back, ids, weights, out):
    share = picked(ids[...], back.shape[0], weights[...])
    routed = jnp.dot(share.astype(jnp.bfloat16), back[...], preferred_element_type=jnp.float32)
    out[...] = (hidden_part[...] + routed).astype(jnp.bfloat16)


def body(
    queries,
    latent_cache,
    cache_len,
    kv_up,
    o_weight,
    residual,
    norm_gain,
    route_ids,
    route_weights,
    w_gate,
    w_up,
    w_down,
):
    ctx_count = lax.axis_size(CTX)
    sub_count = lax.axis_size("sub")
    heads = kv_up.shape[0]
    tokens = queries.shape[0]
    width = heads * VDIM + EXTRA
    planes = ctx_count // 2

    smem = pl.BlockSpec(memory_space=pltpu.SMEM)
    vmem = pl.BlockSpec(memory_space=pltpu.VMEM)
    place = jnp.stack([lax.axis_index("core"), lax.axis_index("sub"), lax.axis_index("far")])
    cols = o_weight.shape[1]
    half = o_weight.shape[0] // 2
    ups = kv_up.transpose(0, 2, 1).reshape(-1, 256)
    taken = heads * (NOPE + ROPE) // 256 * tokens + ups.shape[0]
    packed = pl.pallas_call(
        lambda *refs: pack_kernel(*refs, heads),
        out_shape=jax.ShapeDtypeStruct((taken + 2 * cols, 256), jnp.bfloat16),
        in_specs=[vmem] * 3,
        out_specs=vmem,
        compiler_params=pltpu.CompilerParams(vmem_limit_bytes=8 * 2**20),
        name="pack",
    )(queries, ups, o_weight.T)
    both = lax.all_gather(packed, "pair", axis=0, tiled=False)
    o_full = lax.all_gather(
        both[:, taken:].reshape(PAIR, 2, cols, half), ("far", "hop", "core"), axis=0, tiled=False
    )
    live = lax.broadcasted_iota(jnp.int32, (8, latent_cache.shape[0]), 1) < cache_len[0]
    own_cache = jnp.concatenate([latent_cache.T, live.astype(jnp.bfloat16)], axis=0)
    caches = lax.all_gather(own_cache, "core", axis=0, tiled=False)
    mine = lax.all_gather(both[:, :taken].reshape(PAIR * taken, 256), ("far", "hop"), axis=0, tiled=True)
    mine = mine.reshape(planes, taken, 256)
    other = lax.ppermute(mine, "core", [(0, 1), (1, 0)])

    fars = planes // NEAR
    rows = fars * tokens
    partial = pl.pallas_call(
        lambda *refs: attention_kernel(*refs, heads),
        out_shape=jax.ShapeDtypeStruct((NEAR, fars, tokens, width), jnp.bfloat16),
        in_specs=[smem, vmem, vmem, vmem],
        out_specs=vmem,
        compiler_params=pltpu.CompilerParams(vmem_limit_bytes=24 * 2**20),
        name="attention",
    )(place, mine, other, caches)
    partial = lax.all_to_all(partial.reshape(NEAR, rows, width), NEARBY, 0, 0, tiled=True)
    partial = pl.pallas_call(
        lambda *refs: merge_kernel(*refs, heads),
        out_shape=jax.ShapeDtypeStruct((rows, width), jnp.bfloat16),
        in_specs=[vmem],
        out_specs=vmem,
        compiler_params=pltpu.CompilerParams(vmem_limit_bytes=12 * 2**20),
        name="merge",
    )(partial)
    partial = lax.all_to_all(partial.reshape(fars, tokens, width), "far", 0, 0, tiled=True)
    projected = pl.pallas_call(
        lambda *refs: project_kernel(*refs, heads, o_weight.shape[1]),
        out_shape=jax.ShapeDtypeStruct((sub_count, tokens, D), jnp.bfloat16),
        in_specs=[vmem, vmem],
        out_specs=vmem,
        compiler_params=pltpu.CompilerParams(vmem_limit_bytes=12 * 2**20),
        name="project",
    )(partial, o_full)

    shares = lax.all_to_all(projected, "sub", 0, 0, tiled=True)
    quarter = D // sub_count
    slots = w_gate.shape[0] * ctx_count * CAP
    outgoing, hidden_part = pl.pallas_call(
        norm_kernel,
        out_shape=(
            jax.ShapeDtypeStruct((slots, quarter), jnp.bfloat16),
            jax.ShapeDtypeStruct((tokens, quarter), jnp.float32),
        ),
        in_specs=[smem, vmem, vmem, vmem, vmem],
        out_specs=(vmem, vmem),
        compiler_params=pltpu.CompilerParams(vmem_limit_bytes=8 * 2**20),
        name="norm",
    )(place, shares, residual, norm_gain.reshape(D // 128, 128), route_ids)
    received = lax.all_to_all(outgoing.reshape(ctx_count, CAP, quarter), CTX, 0, 0, tiled=True)
    received = lax.all_gather(received.reshape(slots, quarter), "sub", axis=0, tiled=False)
    partial_out = pl.pallas_call(
        expert_kernel,
        out_shape=jax.ShapeDtypeStruct((sub_count, slots, quarter), jnp.bfloat16),
        in_specs=[vmem, vmem, vmem, vmem],
        out_specs=vmem,
        compiler_params=pltpu.CompilerParams(vmem_limit_bytes=16 * 2**20),
        name="experts",
    )(received, w_gate[0].T, w_up[0].T, w_down[0])
    parts = lax.all_to_all(partial_out, "sub", 0, 0, tiled=True)
    summed = jnp.sum(parts.astype(jnp.float32), axis=0).astype(jnp.bfloat16)
    summed = summed.reshape(ctx_count, CAP, quarter)
    back = lax.all_to_all(summed, CTX, 0, 0, tiled=True)
    return pl.pallas_call(
        final_kernel,
        out_shape=jax.ShapeDtypeStruct((tokens, quarter), jnp.bfloat16),
        in_specs=[vmem] * 4,
        out_specs=vmem,
        compiler_params=pltpu.CompilerParams(vmem_limit_bytes=8 * 2**20),
        name="final",
    )(hidden_part, back.reshape(slots, quarter), route_ids, route_weights)


def solution(mesh):
    planes = mesh.shape["ctx"] // 2
    split = Mesh(
        mesh.devices.reshape(mesh.shape["grp"], planes // NEAR, NEAR // PAIR, PAIR, 2, mesh.shape["sub"]),
        (*GRP_CTX, "sub"),
    )
    return jax.shard_map(
        body,
        mesh=split,
        in_specs=(
            P(GRP_CTX, "sub"),
            P(GRP_CTX, None),
            P(GRP_CTX),
            P(("grp", "sub"), None, CTX),
            P("sub", CTX),
            P(GRP_CTX, None),
            P(),
            P(GRP_CTX, None),
            P(GRP_CTX, None),
            P(CTX, None, "sub"),
            P(CTX, None, "sub"),
            P(CTX, "sub", None),
        ),
        out_specs=P(GRP_CTX, "sub"),
        check_vma=False,
    )
```

```python
import jax
import jax.numpy as jnp
from jax import lax
from jax.experimental import pallas as pl
from jax.experimental.pallas import tpu as pltpu
from jax.sharding import Mesh
from jax.sharding import PartitionSpec as P

D = 2048
NOPE = 128
ROPE = 64
VDIM = 128
LATENT = 512
TOP = 6
CAP = 2
NEAR = 4
PAIR = 2
NEARBY = ("hop", "pair")
CTX = ("far", "hop", "pair", "core")
GRP_CTX = ("grp", *CTX)
Z = ("far", "hop", "pair")
EXTRA = 128

epsilon = 1e-06


def thirds(x):
    high = x.astype(jnp.bfloat16)
    rest = x - high.astype(jnp.float32)
    middle = rest.astype(jnp.bfloat16)
    low = (rest - middle.astype(jnp.float32)).astype(jnp.bfloat16)
    return high.astype(jnp.float32), middle.astype(jnp.float32), low.astype(jnp.float32)


def log_block(logs, rows):
    lane = lax.broadcasted_iota(jnp.int32, (rows, EXTRA), 1)
    heads = len(logs)
    block = jnp.zeros((rows, EXTRA), jnp.float32)
    for h, x in enumerate(logs):
        for piece, part in enumerate(thirds(x)):
            block = jnp.where(lane == heads * piece + h, part, block)
    return block.astype(jnp.bfloat16)


def pack_kernel(queries, ups, packed, heads):
    step = NOPE + ROPE
    per_row = 256 // NOPE
    rows = []
    for r in range(heads // per_row):
        rows.append([queries[:, h * step : h * step + NOPE] for h in range(per_row * r, per_row * r + per_row)])
    rows.append([queries[:, h * step + NOPE : h * step + step] for h in range(heads)])
    parts = [jnp.concatenate(r, axis=1) for r in rows]
    parts.append(ups[...])
    at = 0
    for part in parts:
        packed[at : at + part.shape[0], :] = part
        at += part.shape[0]


def attention_kernel(place, mine, other, both, out, heads):
    planes = mine.shape[0]
    rows = planes * 8
    first = place[0] == 0
    scale = (NOPE + ROPE) ** (-0.5)
    per_row = 256 // NOPE
    q_rows = heads // per_row * 8
    kv_at = q_rows + 8
    caches = [(both[c, :LATENT, :], both[c, LATENT : LATENT + ROPE, :], both[c, LATENT + ROPE :, :]) for c in (0, 1)]
    logs, tops = [], []
    for h in range(heads):
        a = mine[:, kv_at + 8 * h : kv_at + 8 * h + 8, :]
        b = other[:, kv_at + 8 * h : kv_at + 8 * h + 8, :]
        up = jnp.stack([jnp.where(first, a, b), jnp.where(first, b, a)], axis=1)
        up = up.reshape(planes * 16, 256)
        at, lane = 8 * (h // per_row), NOPE * (h % per_row)
        nope = mine[:, at : at + 8, lane : lane + NOPE].reshape(rows, NOPE)
        rope = mine[:, q_rows : q_rows + 8, ROPE * h : ROPE * h + ROPE].reshape(rows, ROPE)
        absorbed = lax.dot_general(
            nope, up[:, :NOPE], (((1,), (1,)), ((), ())), preferred_element_type=jnp.float32
        ).astype(jnp.bfloat16)
        scores = []
        for latents, rotary, live in caches:
            score = jnp.dot(absorbed, latents, preferred_element_type=jnp.float32)
            score = (score + jnp.dot(rope, rotary, preferred_element_type=jnp.float32)) * scale
            scores.append(jnp.where(live[:1].astype(jnp.float32) > 0.5, score, -jnp.inf))
        highest = jnp.maximum(
            jnp.max(scores[0], axis=1, keepdims=True), jnp.max(scores[1], axis=1, keepdims=True)
        )
        total, mixed = 0.0, 0.0
        for score, (latents, _, _) in zip(scores, caches):
            weights = jnp.exp(score - highest).astype(jnp.bfloat16)
            total += jnp.sum(weights.astype(jnp.float32), axis=1, keepdims=True)
            mixed += lax.dot_general(
                weights, latents, (((1,), (1,)), ((), ())), preferred_element_type=jnp.float32
            )
        head = jnp.dot(mixed.astype(jnp.bfloat16), up[:, NOPE:], preferred_element_type=jnp.float32)
        tops.append((head / total).astype(jnp.bfloat16))
        logs.append(highest + jnp.log(total))
    result = jnp.concatenate([*tops, log_block(logs, rows)], axis=1)
    result = result.reshape(planes, 8, result.shape[1])
    for z in range(planes):
        out[z % NEAR, z // NEAR] = result[z]


def merged(parts, heads):
    sources, rows, _ = parts.shape
    width = heads * VDIM
    lane = lax.broadcasted_iota(jnp.int32, (EXTRA, width), 0)
    col = lax.broadcasted_iota(jnp.int32, (EXTRA, width), 1)
    spread = ((lane < 3 * heads) & (lane % heads == col // VDIM)).astype(jnp.bfloat16)
    packed = parts[:, :, width:].reshape(sources * rows, EXTRA)
    logs = jnp.dot(packed, spread, preferred_element_type=jnp.float32).reshape(sources, rows, width)
    top = jnp.max(logs, axis=0)
    shares = jnp.exp(logs - top[None])
    total = jnp.sum(shares, axis=0)
    mixed = jnp.sum(shares * parts[:, :, :width].astype(jnp.float32), axis=0)
    return mixed / total, top + jnp.log(total)


def merge_kernel(parts, out, heads):
    mixed, logs = merged(parts[...], heads)
    rows = mixed.shape[0]
    block = log_block([logs[:, VDIM * h : VDIM * h + EXTRA] for h in range(heads)], rows)
    out[...] = jnp.concatenate([mixed.astype(jnp.bfloat16), block], axis=1)


def join_kernel(parts, out, heads):
    out[...] = merged(parts[...], heads)[0].astype(jnp.bfloat16)


def project_kernel(rows, weight, out):
    pairs, tokens, _ = rows.shape
    projected = lax.dot_general(
        rows[...].reshape(pairs * tokens, -1),
        weight[...],
        (((1,), (1,)), ((), ())),
        preferred_element_type=jnp.float32,
    ).astype(jnp.bfloat16)
    for p in range(pairs):
        for s in range(out.shape[1]):
            out[p, s] = projected[p * tokens : p * tokens + tokens]


def picked(ids, slots, weights=None):
    tokens = ids.shape[0]
    lane = lax.broadcasted_iota(jnp.int32, (tokens, slots), 1)
    named = jnp.zeros((tokens, slots), jnp.float32)
    share = named
    for k in range(TOP):
        same = ids[:, k : k + 1] == lane // CAP
        named = jnp.where(same, 1.0, named)
        share = jnp.where(same, 1.0 if weights is None else weights[:, k : k + 1], share)
    r = lax.broadcasted_iota(jnp.int32, (tokens, tokens), 0)
    c = lax.broadcasted_iota(jnp.int32, (tokens, tokens), 1)
    earlier = jnp.dot(
        (c < r).astype(jnp.bfloat16), named.astype(jnp.bfloat16), preferred_element_type=jnp.float32
    )
    return jnp.where(earlier == (lane % CAP).astype(jnp.float32), share, 0.0)


def norm_kernel(place, shares, residual, gain, ids, out, hidden_part, held, step):
    tokens = residual.shape[0]
    quarter = hidden_part.shape[1]
    sums = [jnp.sum(shares[p].astype(jnp.float32), axis=0) for p in range(shares.shape[0])]
    whole = [x[:, at : at + step] for at in range(0, sums[0].shape[1], step) for x in sums]
    hidden = residual[...].astype(jnp.float32) + jnp.concatenate(whole, axis=1)
    held[...] = hidden
    inverse_rms = lax.rsqrt(jnp.mean(hidden * hidden, axis=1, keepdims=True) + epsilon)
    part = held[:, pl.ds(pl.multiple_of(place[1] * quarter, quarter), quarter)]
    hidden_part[...] = part
    gains = gain[...].astype(jnp.float32)
    lanes = gains.shape[1]
    which = lax.broadcasted_iota(jnp.int32, gains.shape, 0) - place[1] * (quarter // lanes)
    own_gain = [
        jnp.sum(jnp.where(which == k, gains, 0.0), axis=0, keepdims=True) for k in range(quarter // lanes)
    ]
    normed = (part * inverse_rms * jnp.concatenate(own_gain, axis=1)).astype(jnp.bfloat16)
    out[...] = lax.dot_general(
        picked(ids[...], out.shape[0]).astype(jnp.bfloat16),
        normed,
        (((0,), (0,)), ((), ())),
        preferred_element_type=jnp.float32,
    ).astype(jnp.bfloat16)


def expert_kernel(received, gate, up, down, out):
    subs, _, quarter = out.shape
    side = (((1,), (1,)), ((), ()))
    gate_act, up_act = 0.0, 0.0
    for s in range(subs):
        rows = received[s]
        cols = slice(s * quarter, (s + 1) * quarter)
        gate_act += lax.dot_general(rows, gate[:, cols], side, preferred_element_type=jnp.float32)
        up_act += lax.dot_general(rows, up[:, cols], side, preferred_element_type=jnp.float32)
    gated = (gate_act / (1.0 + jnp.exp(-gate_act)) * up_act).astype(jnp.bfloat16)
    for s in range(subs):
        cols = slice(s * quarter, (s + 1) * quarter)
        out[s] = jnp.dot(gated, down[:, cols], preferred_element_type=jnp.float32).astype(jnp.bfloat16)


def final_kernel(hidden_part, back, ids, weights, out):
    share = picked(ids[...], back.shape[0], weights[...])
    routed = jnp.dot(share.astype(jnp.bfloat16), back[...], preferred_element_type=jnp.float32)
    out[...] = (hidden_part[...] + routed).astype(jnp.bfloat16)


def body(
    queries,
    latent_cache,
    cache_len,
    kv_up,
    o_weight,
    residual,
    norm_gain,
    route_ids,
    route_weights,
    w_gate,
    w_up,
    w_down,
):
    ctx_count = lax.axis_size(CTX)
    sub_count = lax.axis_size("sub")
    heads = kv_up.shape[0]
    tokens = queries.shape[0]
    width = heads * VDIM + EXTRA
    planes = ctx_count // 2

    smem = pl.BlockSpec(memory_space=pltpu.SMEM)
    vmem = pl.BlockSpec(memory_space=pltpu.VMEM)
    place = jnp.stack([lax.axis_index("core"), lax.axis_index("sub"), lax.axis_index("far")])
    o_part = lax.all_gather(o_weight.T, ("far", "hop", "core"), axis=0, tiled=True)
    ups = kv_up.transpose(0, 2, 1).reshape(-1, 256)
    taken = heads * (NOPE + ROPE) // 256 * tokens + ups.shape[0]
    packed = pl.pallas_call(
        lambda *refs: pack_kernel(*refs, heads),
        out_shape=jax.ShapeDtypeStruct((taken, 256), jnp.bfloat16),
        in_specs=[vmem] * 2,
        out_specs=vmem,
        compiler_params=pltpu.CompilerParams(vmem_limit_bytes=8 * 2**20),
        name="pack",
    )(queries, ups)
    both = lax.all_gather(packed, "pair", axis=0, tiled=False)
    live = lax.broadcasted_iota(jnp.int32, (8, latent_cache.shape[0]), 1) < cache_len[0]
    own_cache = jnp.concatenate([latent_cache.T, live.astype(jnp.bfloat16)], axis=0)
    caches = lax.all_gather(own_cache, "core", axis=0, tiled=False)
    mine = lax.all_gather(both.reshape(PAIR * taken, 256), ("far", "hop"), axis=0, tiled=True)
    mine = mine.reshape(planes, taken, 256)
    other = lax.ppermute(mine, "core", [(0, 1), (1, 0)])

    fars = planes // NEAR
    rows = fars * tokens
    partial = pl.pallas_call(
        lambda *refs: attention_kernel(*refs, heads),
        out_shape=jax.ShapeDtypeStruct((NEAR, fars, tokens, width), jnp.bfloat16),
        in_specs=[smem, vmem, vmem, vmem],
        out_specs=vmem,
        compiler_params=pltpu.CompilerParams(vmem_limit_bytes=24 * 2**20),
        name="attention",
    )(place, mine, other, caches)
    partial = lax.all_to_all(partial.reshape(NEAR, rows, width), NEARBY, 0, 0, tiled=True)
    partial = pl.pallas_call(
        lambda *refs: merge_kernel(*refs, heads),
        out_shape=jax.ShapeDtypeStruct((rows, width), jnp.bfloat16),
        in_specs=[vmem],
        out_specs=vmem,
        compiler_params=pltpu.CompilerParams(vmem_limit_bytes=12 * 2**20),
        name="merge",
    )(partial)
    partial = lax.all_to_all(partial.reshape(fars, tokens, width), "far", 0, 0, tiled=True)
    joined = pl.pallas_call(
        lambda *refs: join_kernel(*refs, heads),
        out_shape=jax.ShapeDtypeStruct((tokens, heads * VDIM), jnp.bfloat16),
        in_specs=[vmem],
        out_specs=vmem,
        compiler_params=pltpu.CompilerParams(vmem_limit_bytes=8 * 2**20),
        name="join",
    )(partial)
    joined = lax.all_gather(joined, "pair", axis=0, tiled=False)
    projected = pl.pallas_call(
        project_kernel,
        out_shape=jax.ShapeDtypeStruct((PAIR, sub_count, tokens, D // PAIR), jnp.bfloat16),
        in_specs=[vmem, vmem],
        out_specs=vmem,
        compiler_params=pltpu.CompilerParams(vmem_limit_bytes=8 * 2**20),
        name="project",
    )(joined, o_part)

    shares = lax.all_to_all(
        projected.reshape(PAIR * sub_count, tokens, D // PAIR), ("pair", "sub"), 0, 0, tiled=True
    ).reshape(PAIR, sub_count, tokens, D // PAIR)
    quarter = D // sub_count
    slots = w_gate.shape[0] * ctx_count * CAP
    outgoing, hidden_part = pl.pallas_call(
        lambda *refs: norm_kernel(*refs, 2 * o_weight.shape[1]),
        out_shape=(
            jax.ShapeDtypeStruct((slots, quarter), jnp.bfloat16),
            jax.ShapeDtypeStruct((tokens, quarter), jnp.float32),
        ),
        in_specs=[smem, vmem, vmem, vmem, vmem],
        out_specs=(vmem, vmem),
        scratch_shapes=[pltpu.VMEM((tokens, D), jnp.float32)],
        compiler_params=pltpu.CompilerParams(vmem_limit_bytes=8 * 2**20),
        name="norm",
    )(place, shares, residual, norm_gain.reshape(D // 128, 128), route_ids)
    received = lax.all_to_all(outgoing.reshape(ctx_count, CAP, quarter), CTX, 0, 0, tiled=True)
    received = lax.all_gather(received.reshape(slots, quarter), "sub", axis=0, tiled=False)
    partial_out = pl.pallas_call(
        expert_kernel,
        out_shape=jax.ShapeDtypeStruct((sub_count, slots, quarter), jnp.bfloat16),
        in_specs=[vmem, vmem, vmem, vmem],
        out_specs=vmem,
        compiler_params=pltpu.CompilerParams(vmem_limit_bytes=16 * 2**20),
        name="experts",
    )(received, w_gate[0].T, w_up[0].T, w_down[0])
    parts = lax.all_to_all(partial_out, "sub", 0, 0, tiled=True)
    summed = jnp.sum(parts.astype(jnp.float32), axis=0).astype(jnp.bfloat16)
    summed = summed.reshape(ctx_count, CAP, quarter)
    back = lax.all_to_all(summed, CTX, 0, 0, tiled=True)
    return pl.pallas_call(
        final_kernel,
        out_shape=jax.ShapeDtypeStruct((tokens, quarter), jnp.bfloat16),
        in_specs=[vmem] * 4,
        out_specs=vmem,
        compiler_params=pltpu.CompilerParams(vmem_limit_bytes=8 * 2**20),
        name="final",
    )(hidden_part, back.reshape(slots, quarter), route_ids, route_weights)


def solution(mesh):
    planes = mesh.shape["ctx"] // 2
    split = Mesh(
        mesh.devices.reshape(mesh.shape["grp"], planes // NEAR, NEAR // PAIR, PAIR, 2, mesh.shape["sub"]),
        (*GRP_CTX, "sub"),
    )
    return jax.shard_map(
        body,
        mesh=split,
        in_specs=(
            P(GRP_CTX, "sub"),
            P(GRP_CTX, None),
            P(GRP_CTX),
            P(("grp", "sub"), None, CTX),
            P("sub", CTX),
            P(GRP_CTX, None),
            P(),
            P(GRP_CTX, None),
            P(GRP_CTX, None),
            P(CTX, None, "sub"),
            P(CTX, None, "sub"),
            P(CTX, "sub", None),
        ),
        out_specs=P(GRP_CTX, "sub"),
        check_vma=False,
    )
```

```python
import jax
import jax.numpy as jnp
from jax import lax
from jax.experimental import pallas as pl
from jax.experimental.pallas import tpu as pltpu
from jax.sharding import Mesh
from jax.sharding import PartitionSpec as P

D = 2048
NOPE = 128
ROPE = 64
VDIM = 128
LATENT = 512
TOP = 6
CAP = 2
NEAR = 4
PAIR = 2
NEARBY = ("hop", "pair")
CTX = ("far", "hop", "pair", "core")
GRP_CTX = ("grp", *CTX)
SPREAD = ("hop", "pair", "core", "far")
EXTRA = 128

epsilon = 1e-06


def thirds(x):
    high = x.astype(jnp.bfloat16)
    rest = x - high.astype(jnp.float32)
    middle = rest.astype(jnp.bfloat16)
    low = (rest - middle.astype(jnp.float32)).astype(jnp.bfloat16)
    return high.astype(jnp.float32), middle.astype(jnp.float32), low.astype(jnp.float32)


def log_block(logs, rows):
    lane = lax.broadcasted_iota(jnp.int32, (rows, EXTRA), 1)
    heads = len(logs)
    block = jnp.zeros((rows, EXTRA), jnp.float32)
    for h, x in enumerate(logs):
        for piece, part in enumerate(thirds(x)):
            block = jnp.where(lane == heads * piece + h, part, block)
    return block.astype(jnp.bfloat16)


def pack_kernel(queries, ups, packed, heads):
    step = NOPE + ROPE
    per_row = 256 // NOPE
    rows = []
    for r in range(heads // per_row):
        rows.append([queries[:, h * step : h * step + NOPE] for h in range(per_row * r, per_row * r + per_row)])
    rows.append([queries[:, h * step + NOPE : h * step + step] for h in range(heads)])
    parts = [jnp.concatenate(r, axis=1) for r in rows]
    parts.append(ups[...])
    at = 0
    for part in parts:
        packed[at : at + part.shape[0], :] = part
        at += part.shape[0]


def attention_kernel(place, mine, other, both, out, heads):
    planes = mine.shape[0]
    rows = planes * 8
    first = place[0] == 0
    scale = (NOPE + ROPE) ** (-0.5)
    per_row = 256 // NOPE
    q_rows = heads // per_row * 8
    kv_at = q_rows + 8
    caches = [(both[c, :LATENT, :], both[c, LATENT : LATENT + ROPE, :], both[c, LATENT + ROPE :, :]) for c in (0, 1)]
    logs, tops = [], []
    for h in range(heads):
        a = mine[:, kv_at + 8 * h : kv_at + 8 * h + 8, :]
        b = other[:, kv_at + 8 * h : kv_at + 8 * h + 8, :]
        up = jnp.stack([jnp.where(first, a, b), jnp.where(first, b, a)], axis=1)
        up = up.reshape(planes * 16, 256)
        at, lane = 8 * (h // per_row), NOPE * (h % per_row)
        nope = mine[:, at : at + 8, lane : lane + NOPE].reshape(rows, NOPE)
        rope = mine[:, q_rows : q_rows + 8, ROPE * h : ROPE * h + ROPE].reshape(rows, ROPE)
        absorbed = lax.dot_general(
            nope, up[:, :NOPE], (((1,), (1,)), ((), ())), preferred_element_type=jnp.float32
        ).astype(jnp.bfloat16)
        scores = []
        for latents, rotary, live in caches:
            score = jnp.dot(absorbed, latents, preferred_element_type=jnp.float32)
            score = (score + jnp.dot(rope, rotary, preferred_element_type=jnp.float32)) * scale
            scores.append(jnp.where(live[:1].astype(jnp.float32) > 0.5, score, -jnp.inf))
        highest = jnp.maximum(
            jnp.max(scores[0], axis=1, keepdims=True), jnp.max(scores[1], axis=1, keepdims=True)
        )
        total, mixed = 0.0, 0.0
        for score, (latents, _, _) in zip(scores, caches):
            weights = jnp.exp(score - highest).astype(jnp.bfloat16)
            total += jnp.sum(weights.astype(jnp.float32), axis=1, keepdims=True)
            mixed += lax.dot_general(
                weights, latents, (((1,), (1,)), ((), ())), preferred_element_type=jnp.float32
            )
        head = jnp.dot(mixed.astype(jnp.bfloat16), up[:, NOPE:], preferred_element_type=jnp.float32)
        tops.append((head / total).astype(jnp.bfloat16))
        logs.append(highest + jnp.log(total))
    result = jnp.concatenate([*tops, log_block(logs, rows)], axis=1)
    result = result.reshape(planes, 8, result.shape[1])
    for z in range(planes):
        out[z % NEAR, z // NEAR] = result[z]


def merged(parts, heads):
    sources, rows, _ = parts.shape
    width = heads * VDIM
    lane = lax.broadcasted_iota(jnp.int32, (EXTRA, width), 0)
    col = lax.broadcasted_iota(jnp.int32, (EXTRA, width), 1)
    spread = ((lane < 3 * heads) & (lane % heads == col // VDIM)).astype(jnp.bfloat16)
    packed = parts[:, :, width:].reshape(sources * rows, EXTRA)
    logs = jnp.dot(packed, spread, preferred_element_type=jnp.float32).reshape(sources, rows, width)
    top = jnp.max(logs, axis=0)
    shares = jnp.exp(logs - top[None])
    total = jnp.sum(shares, axis=0)
    mixed = jnp.sum(shares * parts[:, :, :width].astype(jnp.float32), axis=0)
    return mixed / total, top + jnp.log(total)


def merge_kernel(parts, out, heads):
    mixed, logs = merged(parts[...], heads)
    rows = mixed.shape[0]
    block = log_block([logs[:, VDIM * h : VDIM * h + EXTRA] for h in range(heads)], rows)
    out[...] = jnp.concatenate([mixed.astype(jnp.bfloat16), block], axis=1)


def join_kernel(parts, out, heads):
    out[...] = merged(parts[...], heads)[0].astype(jnp.bfloat16)


def project_kernel(rows, weight, out):
    pairs, tokens, _ = rows.shape
    projected = lax.dot_general(
        rows[...].reshape(pairs * tokens, -1),
        weight[...],
        (((1,), (1,)), ((), ())),
        preferred_element_type=jnp.float32,
    ).astype(jnp.bfloat16)
    for p in range(pairs):
        for s in range(out.shape[1]):
            out[p, s] = projected[p * tokens : p * tokens + tokens]


def picked(ids, slots, weights=None):
    tokens = ids.shape[0]
    fars = slots // (CAP * NEAR * 2)
    lane = lax.broadcasted_iota(jnp.int32, (tokens, slots), 1)
    expert = lane // CAP % fars * (NEAR * 2) + lane // (CAP * fars)
    named = jnp.zeros((tokens, slots), jnp.float32)
    share = named
    for k in range(TOP):
        same = ids[:, k : k + 1] == expert
        named = jnp.where(same, 1.0, named)
        share = jnp.where(same, 1.0 if weights is None else weights[:, k : k + 1], share)
    r = lax.broadcasted_iota(jnp.int32, (tokens, tokens), 0)
    c = lax.broadcasted_iota(jnp.int32, (tokens, tokens), 1)
    earlier = jnp.dot(
        (c < r).astype(jnp.bfloat16), named.astype(jnp.bfloat16), preferred_element_type=jnp.float32
    )
    return jnp.where(earlier == (lane % CAP).astype(jnp.float32), share, 0.0)


def norm_kernel(place, shares, residual, gain, ids, out, hidden_part, held, step):
    tokens = residual.shape[0]
    quarter = hidden_part.shape[1]
    sums = [jnp.sum(shares[p].astype(jnp.float32), axis=0) for p in range(shares.shape[0])]
    whole = [x[:, at : at + step] for at in range(0, sums[0].shape[1], step) for x in sums]
    hidden = residual[...].astype(jnp.float32) + jnp.concatenate(whole, axis=1)
    held[...] = hidden
    inverse_rms = lax.rsqrt(jnp.mean(hidden * hidden, axis=1, keepdims=True) + epsilon)
    part = held[:, pl.ds(pl.multiple_of(place[1] * quarter, quarter), quarter)]
    hidden_part[...] = part
    gains = gain[...].astype(jnp.float32)
    lanes = gains.shape[1]
    which = lax.broadcasted_iota(jnp.int32, gains.shape, 0) - place[1] * (quarter // lanes)
    own_gain = [
        jnp.sum(jnp.where(which == k, gains, 0.0), axis=0, keepdims=True) for k in range(quarter // lanes)
    ]
    normed = (part * inverse_rms * jnp.concatenate(own_gain, axis=1)).astype(jnp.bfloat16)
    out[...] = lax.dot_general(
        picked(ids[...], out.shape[0]).astype(jnp.bfloat16),
        normed,
        (((0,), (0,)), ((), ())),
        preferred_element_type=jnp.float32,
    ).astype(jnp.bfloat16)


def expert_kernel(received, gate, up, down, out):
    subs, _, quarter = out.shape
    side = (((1,), (1,)), ((), ()))
    gate_act, up_act = 0.0, 0.0
    for s in range(subs):
        rows = received[s]
        cols = slice(s * quarter, (s + 1) * quarter)
        gate_act += lax.dot_general(rows, gate[:, cols], side, preferred_element_type=jnp.float32)
        up_act += lax.dot_general(rows, up[:, cols], side, preferred_element_type=jnp.float32)
    gated = (gate_act / (1.0 + jnp.exp(-gate_act)) * up_act).astype(jnp.bfloat16)
    for s in range(subs):
        cols = slice(s * quarter, (s + 1) * quarter)
        out[s] = jnp.dot(gated, down[:, cols], preferred_element_type=jnp.float32).astype(jnp.bfloat16)


def final_kernel(hidden_part, back, ids, weights, out):
    share = picked(ids[...], back.shape[0], weights[...])
    routed = jnp.dot(share.astype(jnp.bfloat16), back[...], preferred_element_type=jnp.float32)
    out[...] = (hidden_part[...] + routed).astype(jnp.bfloat16)


def body(
    queries,
    latent_cache,
    cache_len,
    kv_up,
    o_weight,
    residual,
    norm_gain,
    route_ids,
    route_weights,
    w_gate,
    w_up,
    w_down,
):
    ctx_count = lax.axis_size(CTX)
    sub_count = lax.axis_size("sub")
    heads = kv_up.shape[0]
    tokens = queries.shape[0]
    width = heads * VDIM + EXTRA
    planes = ctx_count // 2

    smem = pl.BlockSpec(memory_space=pltpu.SMEM)
    vmem = pl.BlockSpec(memory_space=pltpu.VMEM)
    place = jnp.stack([lax.axis_index("core"), lax.axis_index("sub"), lax.axis_index("far")])
    o_part = lax.all_gather(o_weight.T, ("far", "hop", "core"), axis=0, tiled=True)
    ups = kv_up.transpose(0, 2, 1).reshape(-1, 256)
    taken = heads * (NOPE + ROPE) // 256 * tokens + ups.shape[0]
    packed = pl.pallas_call(
        lambda *refs: pack_kernel(*refs, heads),
        out_shape=jax.ShapeDtypeStruct((taken, 256), jnp.bfloat16),
        in_specs=[vmem] * 2,
        out_specs=vmem,
        compiler_params=pltpu.CompilerParams(vmem_limit_bytes=8 * 2**20),
        name="pack",
    )(queries, ups)
    both = lax.all_gather(packed, "pair", axis=0, tiled=False)
    live = lax.broadcasted_iota(jnp.int32, (8, latent_cache.shape[0]), 1) < cache_len[0]
    own_cache = jnp.concatenate([latent_cache.T, live.astype(jnp.bfloat16)], axis=0)
    caches = lax.all_gather(own_cache, "core", axis=0, tiled=False)
    mine = lax.all_gather(both.reshape(PAIR * taken, 256), ("far", "hop"), axis=0, tiled=True)
    mine = mine.reshape(planes, taken, 256)
    other = lax.ppermute(mine, "core", [(0, 1), (1, 0)])

    fars = planes // NEAR
    rows = fars * tokens
    partial = pl.pallas_call(
        lambda *refs: attention_kernel(*refs, heads),
        out_shape=jax.ShapeDtypeStruct((NEAR, fars, tokens, width), jnp.bfloat16),
        in_specs=[smem, vmem, vmem, vmem],
        out_specs=vmem,
        compiler_params=pltpu.CompilerParams(vmem_limit_bytes=24 * 2**20),
        name="attention",
    )(place, mine, other, caches)
    partial = lax.all_to_all(partial.reshape(NEAR, rows, width), NEARBY, 0, 0, tiled=True)
    partial = pl.pallas_call(
        lambda *refs: merge_kernel(*refs, heads),
        out_shape=jax.ShapeDtypeStruct((rows, width), jnp.bfloat16),
        in_specs=[vmem],
        out_specs=vmem,
        compiler_params=pltpu.CompilerParams(vmem_limit_bytes=12 * 2**20),
        name="merge",
    )(partial)
    partial = lax.all_to_all(partial.reshape(fars, tokens, width), "far", 0, 0, tiled=True)
    joined = pl.pallas_call(
        lambda *refs: join_kernel(*refs, heads),
        out_shape=jax.ShapeDtypeStruct((tokens, heads * VDIM), jnp.bfloat16),
        in_specs=[vmem],
        out_specs=vmem,
        compiler_params=pltpu.CompilerParams(vmem_limit_bytes=8 * 2**20),
        name="join",
    )(partial)
    joined = lax.all_gather(joined, "pair", axis=0, tiled=False)
    projected = pl.pallas_call(
        project_kernel,
        out_shape=jax.ShapeDtypeStruct((PAIR, sub_count, tokens, D // PAIR), jnp.bfloat16),
        in_specs=[vmem, vmem],
        out_specs=vmem,
        compiler_params=pltpu.CompilerParams(vmem_limit_bytes=8 * 2**20),
        name="project",
    )(joined, o_part)

    shares = lax.all_to_all(
        projected.reshape(PAIR * sub_count, tokens, D // PAIR), ("pair", "sub"), 0, 0, tiled=True
    ).reshape(PAIR, sub_count, tokens, D // PAIR)
    quarter = D // sub_count
    slots = w_gate.shape[0] * ctx_count * CAP
    outgoing, hidden_part = pl.pallas_call(
        lambda *refs: norm_kernel(*refs, 2 * o_weight.shape[1]),
        out_shape=(
            jax.ShapeDtypeStruct((slots, quarter), jnp.bfloat16),
            jax.ShapeDtypeStruct((tokens, quarter), jnp.float32),
        ),
        in_specs=[smem, vmem, vmem, vmem, vmem],
        out_specs=(vmem, vmem),
        scratch_shapes=[pltpu.VMEM((tokens, D), jnp.float32)],
        compiler_params=pltpu.CompilerParams(vmem_limit_bytes=8 * 2**20),
        name="norm",
    )(place, shares, residual, norm_gain.reshape(D // 128, 128), route_ids)
    received = lax.all_to_all(outgoing.reshape(ctx_count, CAP, quarter), SPREAD, 0, 0, tiled=True)
    received = lax.all_gather(received.reshape(slots, quarter), "sub", axis=0, tiled=False)
    partial_out = pl.pallas_call(
        expert_kernel,
        out_shape=jax.ShapeDtypeStruct((sub_count, slots, quarter), jnp.bfloat16),
        in_specs=[vmem, vmem, vmem, vmem],
        out_specs=vmem,
        compiler_params=pltpu.CompilerParams(vmem_limit_bytes=16 * 2**20),
        name="experts",
    )(received, w_gate[0].T, w_up[0].T, w_down[0])
    parts = lax.all_to_all(partial_out, "sub", 0, 0, tiled=True)
    summed = jnp.sum(parts.astype(jnp.float32), axis=0).astype(jnp.bfloat16)
    summed = summed.reshape(ctx_count, CAP, quarter)
    back = lax.all_to_all(summed, SPREAD, 0, 0, tiled=True)
    return pl.pallas_call(
        final_kernel,
        out_shape=jax.ShapeDtypeStruct((tokens, quarter), jnp.bfloat16),
        in_specs=[vmem] * 4,
        out_specs=vmem,
        compiler_params=pltpu.CompilerParams(vmem_limit_bytes=8 * 2**20),
        name="final",
    )(hidden_part, back.reshape(slots, quarter), route_ids, route_weights)


def solution(mesh):
    planes = mesh.shape["ctx"] // 2
    split = Mesh(
        mesh.devices.reshape(mesh.shape["grp"], planes // NEAR, NEAR // PAIR, PAIR, 2, mesh.shape["sub"]),
        (*GRP_CTX, "sub"),
    )
    return jax.shard_map(
        body,
        mesh=split,
        in_specs=(
            P(GRP_CTX, "sub"),
            P(GRP_CTX, None),
            P(GRP_CTX),
            P(("grp", "sub"), None, CTX),
            P("sub", CTX),
            P(GRP_CTX, None),
            P(),
            P(GRP_CTX, None),
            P(GRP_CTX, None),
            P(CTX, None, "sub"),
            P(CTX, None, "sub"),
            P(CTX, "sub", None),
        ),
        out_specs=P(GRP_CTX, "sub"),
        check_vma=False,
    )
```

```python
import jax
import jax.numpy as jnp
from jax import lax
from jax.experimental import pallas as pl
from jax.experimental.pallas import tpu as pltpu
from jax.sharding import Mesh
from jax.sharding import PartitionSpec as P

D = 2048
NOPE = 128
ROPE = 64
VDIM = 128
LATENT = 512
TOP = 6
CAP = 2
NEAR = 4
PAIR = 2
NEARBY = ("hop", "pair")
CTX = ("far", "hop", "pair", "core")
GRP_CTX = ("grp", *CTX)
SPREAD = ("hop", "pair", "core", "far")
EXTRA = 128

epsilon = 1e-06


def thirds(x):
    high = x.astype(jnp.bfloat16)
    rest = x - high.astype(jnp.float32)
    middle = rest.astype(jnp.bfloat16)
    low = (rest - middle.astype(jnp.float32)).astype(jnp.bfloat16)
    return high.astype(jnp.float32), middle.astype(jnp.float32), low.astype(jnp.float32)


def log_block(logs, rows):
    lane = lax.broadcasted_iota(jnp.int32, (rows, EXTRA), 1)
    heads = len(logs)
    block = jnp.zeros((rows, EXTRA), jnp.float32)
    for h, x in enumerate(logs):
        for piece, part in enumerate(thirds(x)):
            block = jnp.where(lane == heads * piece + h, part, block)
    return block.astype(jnp.bfloat16)


def pack_kernel(length, queries, ups, o_rows, cache, packed, own_cache, heads):
    step = NOPE + ROPE
    per_row = 256 // NOPE
    half = o_rows.shape[1] // 2
    rows = []
    for r in range(heads // per_row):
        rows.append([queries[:, h * step : h * step + NOPE] for h in range(per_row * r, per_row * r + per_row)])
    rows.append([queries[:, h * step + NOPE : h * step + step] for h in range(heads)])
    parts = [jnp.concatenate(r, axis=1) for r in rows]
    parts += [ups[...], o_rows[:, :half], o_rows[:, half:]]
    for p in range(packed.shape[0]):
        at = 0
        for part in parts:
            packed[p, at : at + part.shape[0], :] = part
            at += part.shape[0]
    width = cache.shape[0]
    own_cache[:width, :] = cache[...]
    shape = (own_cache.shape[0] - width, cache.shape[1])
    live = lax.broadcasted_iota(jnp.int32, shape, 1) < length[0]
    own_cache[width:, :] = jnp.where(live, 1.0, 0.0).astype(jnp.bfloat16)


def attention_kernel(place, mine, other, own_cache, pair_cache, out, heads):
    planes = mine.shape[0]
    rows = planes * 8
    first = place[0] == 0
    scale = (NOPE + ROPE) ** (-0.5)
    per_row = 256 // NOPE
    q_rows = heads // per_row * 8
    kv_at = q_rows + 8
    caches = [(c[:LATENT, :], c[LATENT : LATENT + ROPE, :], c[LATENT + ROPE :, :]) for c in (own_cache, pair_cache)]
    logs, tops = [], []
    for h in range(heads):
        a = mine[:, kv_at + 8 * h : kv_at + 8 * h + 8, :]
        b = other[:, kv_at + 8 * h : kv_at + 8 * h + 8, :]
        up = jnp.stack([jnp.where(first, a, b), jnp.where(first, b, a)], axis=1)
        up = up.reshape(planes * 16, 256)
        at, lane = 8 * (h // per_row), NOPE * (h % per_row)
        nope = mine[:, at : at + 8, lane : lane + NOPE].reshape(rows, NOPE)
        rope = mine[:, q_rows : q_rows + 8, ROPE * h : ROPE * h + ROPE].reshape(rows, ROPE)
        absorbed = lax.dot_general(
            nope, up[:, :NOPE], (((1,), (1,)), ((), ())), preferred_element_type=jnp.float32
        ).astype(jnp.bfloat16)
        scores = []
        for latents, rotary, live in caches:
            score = jnp.dot(absorbed, latents, preferred_element_type=jnp.float32)
            score = (score + jnp.dot(rope, rotary, preferred_element_type=jnp.float32)) * scale
            scores.append(jnp.where(live[:1].astype(jnp.float32) > 0.5, score, -jnp.inf))
        highest = jnp.maximum(
            jnp.max(scores[0], axis=1, keepdims=True), jnp.max(scores[1], axis=1, keepdims=True)
        )
        total, mixed = 0.0, 0.0
        for score, (latents, _, _) in zip(scores, caches):
            weights = jnp.exp(score - highest).astype(jnp.bfloat16)
            total += jnp.sum(weights.astype(jnp.float32), axis=1, keepdims=True)
            mixed += lax.dot_general(
                weights, latents, (((1,), (1,)), ((), ())), preferred_element_type=jnp.float32
            )
        head = jnp.dot(mixed.astype(jnp.bfloat16), up[:, NOPE:], preferred_element_type=jnp.float32)
        tops.append((head / total).astype(jnp.bfloat16))
        logs.append(highest + jnp.log(total))
    result = jnp.concatenate([*tops, log_block(logs, rows)], axis=1)
    result = result.reshape(planes, 8, result.shape[1])
    for z in range(planes):
        out[z % NEAR, z // NEAR] = result[z]


def merged(parts, heads):
    sources, rows, _ = parts.shape
    width = heads * VDIM
    lane = lax.broadcasted_iota(jnp.int32, (EXTRA, width), 0)
    col = lax.broadcasted_iota(jnp.int32, (EXTRA, width), 1)
    spread = ((lane < 3 * heads) & (lane % heads == col // VDIM)).astype(jnp.bfloat16)
    packed = parts[:, :, width:].reshape(sources * rows, EXTRA)
    logs = jnp.dot(packed, spread, preferred_element_type=jnp.float32).reshape(sources, rows, width)
    top = jnp.max(logs, axis=0)
    shares = jnp.exp(logs - top[None])
    total = jnp.sum(shares, axis=0)
    mixed = jnp.sum(shares * parts[:, :, :width].astype(jnp.float32), axis=0)
    return mixed / total, top + jnp.log(total)


def merge_kernel(parts, out, heads):
    mixed, logs = merged(parts[...], heads)
    rows = mixed.shape[0]
    block = log_block([logs[:, VDIM * h : VDIM * h + EXTRA] for h in range(heads)], rows)
    out[...] = jnp.concatenate([mixed.astype(jnp.bfloat16), block], axis=1)


def project_kernel(parts, weight, out, heads, cols):
    mixed, _ = merged(parts[...], heads)
    size = 2 * PAIR * cols
    to = lax.broadcasted_iota(jnp.int32, (size, size), 1)
    source = to // cols % 2 * (PAIR * cols) + to // (2 * cols) * cols + to % cols
    turn = (lax.broadcasted_iota(jnp.int32, (size, size), 0) == source).astype(jnp.bfloat16)
    mixed = mixed.astype(jnp.bfloat16)
    half = weight.shape[4]
    projected = 0.0
    for k in range(2):
        rows = weight[:, :, k].reshape(-1, half)
        projected += lax.dot_general(
            mixed[:, k * half : k * half + half],
            rows,
            (((1,), (1,)), ((), ())),
            preferred_element_type=jnp.float32,
        )
    projected = projected.astype(jnp.bfloat16)
    for at in range(0, projected.shape[1], size):
        part = jnp.dot(projected[:, at : at + size], turn, preferred_element_type=jnp.float32).astype(jnp.bfloat16)
        for s in range(out.shape[0]):
            out[s, :, at : at + size] = part


def picked(ids, slots, weights=None):
    tokens = ids.shape[0]
    fars = slots // (CAP * NEAR * 2)
    lane = lax.broadcasted_iota(jnp.int32, (tokens, slots), 1)
    expert = lane // CAP % fars * (NEAR * 2) + lane // (CAP * fars)
    named = jnp.zeros((tokens, slots), jnp.float32)
    share = named
    for k in range(TOP):
        same = ids[:, k : k + 1] == expert
        named = jnp.where(same, 1.0, named)
        share = jnp.where(same, 1.0 if weights is None else weights[:, k : k + 1], share)
    r = lax.broadcasted_iota(jnp.int32, (tokens, tokens), 0)
    c = lax.broadcasted_iota(jnp.int32, (tokens, tokens), 1)
    earlier = jnp.dot(
        (c < r).astype(jnp.bfloat16), named.astype(jnp.bfloat16), preferred_element_type=jnp.float32
    )
    return jnp.where(earlier == (lane % CAP).astype(jnp.float32), share, 0.0)


def norm_kernel(place, shares, residual, gain, ids, out, hidden_part):
    tokens = residual.shape[0]
    quarter = hidden_part.shape[1]
    hidden = residual[...].astype(jnp.float32) + jnp.sum(shares[...].astype(jnp.float32), axis=0)
    inverse_rms = lax.rsqrt(jnp.mean(hidden * hidden, axis=1, keepdims=True) + epsilon)
    own = pl.ds(pl.multiple_of(place[1] * quarter, quarter), quarter)
    part = residual[:, own].astype(jnp.float32) + jnp.sum(shares[:, :, own].astype(jnp.float32), axis=0)
    hidden_part[...] = part
    gains = gain[...].astype(jnp.float32)
    lanes = gains.shape[1]
    which = lax.broadcasted_iota(jnp.int32, gains.shape, 0) - place[1] * (quarter // lanes)
    own_gain = [
        jnp.sum(jnp.where(which == k, gains, 0.0), axis=0, keepdims=True) for k in range(quarter // lanes)
    ]
    normed = (part * inverse_rms * jnp.concatenate(own_gain, axis=1)).astype(jnp.bfloat16)
    out[...] = lax.dot_general(
        picked(ids[...], out.shape[0]).astype(jnp.bfloat16),
        normed,
        (((0,), (0,)), ((), ())),
        preferred_element_type=jnp.float32,
    ).astype(jnp.bfloat16)


def expert_kernel(received, gate, up, down, out):
    subs, _, quarter = out.shape
    side = (((1,), (1,)), ((), ()))
    gate_act, up_act = 0.0, 0.0
    for s in range(subs):
        rows = received[s]
        cols = slice(s * quarter, (s + 1) * quarter)
        gate_act += lax.dot_general(rows, gate[:, cols], side, preferred_element_type=jnp.float32)
        up_act += lax.dot_general(rows, up[:, cols], side, preferred_element_type=jnp.float32)
    gated = (gate_act / (1.0 + jnp.exp(-gate_act)) * up_act).astype(jnp.bfloat16)
    for s in range(subs):
        cols = slice(s * quarter, (s + 1) * quarter)
        out[s] = jnp.dot(gated, down[:, cols], preferred_element_type=jnp.float32).astype(jnp.bfloat16)


def final_kernel(hidden_part, back, ids, weights, out):
    share = picked(ids[...], back.shape[0], weights[...])
    routed = jnp.dot(share.astype(jnp.bfloat16), back[...], preferred_element_type=jnp.float32)
    out[...] = (hidden_part[...] + routed).astype(jnp.bfloat16)


def body(
    queries,
    latent_cache,
    cache_len,
    kv_up,
    o_weight,
    residual,
    norm_gain,
    route_ids,
    route_weights,
    w_gate,
    w_up,
    w_down,
):
    ctx_count = lax.axis_size(CTX)
    sub_count = lax.axis_size("sub")
    heads = kv_up.shape[0]
    tokens = queries.shape[0]
    width = heads * VDIM + EXTRA
    planes = ctx_count // 2

    smem = pl.BlockSpec(memory_space=pltpu.SMEM)
    vmem = pl.BlockSpec(memory_space=pltpu.VMEM)
    place = jnp.stack([lax.axis_index("core"), lax.axis_index("sub"), lax.axis_index("far")])
    cols = o_weight.shape[1]
    half = o_weight.shape[0] // 2
    ups = kv_up.transpose(0, 2, 1).reshape(-1, 256)
    taken = heads * (NOPE + ROPE) // 256 * tokens + ups.shape[0]
    packed, own_cache = pl.pallas_call(
        lambda *refs: pack_kernel(*refs, heads),
        out_shape=(
            jax.ShapeDtypeStruct((PAIR, taken + 2 * cols, 256), jnp.bfloat16),
            jax.ShapeDtypeStruct((latent_cache.shape[1] + 8, latent_cache.shape[0]), jnp.bfloat16),
        ),
        in_specs=[smem] + [pl.BlockSpec()] * 4,
        out_specs=(vmem, vmem),
        compiler_params=pltpu.CompilerParams(vmem_limit_bytes=8 * 2**20),
        name="pack",
    )(cache_len, queries, ups, o_weight.T, latent_cache.T)
    both = lax.all_to_all(packed, "pair", 0, 0, tiled=True)
    o_full = lax.all_gather(
        both[:, taken:].reshape(PAIR, 2, cols, half), ("far", "hop", "core"), axis=0, tiled=False
    )
    pair_cache = lax.ppermute(own_cache, "core", [(0, 1), (1, 0)])
    mine = lax.all_gather(both[:, :taken].reshape(PAIR * taken, 256), ("far", "hop"), axis=0, tiled=True)
    mine = mine.reshape(planes, taken, 256)
    other = lax.ppermute(mine, "core", [(0, 1), (1, 0)])

    fars = planes // NEAR
    rows = fars * tokens
    partial = pl.pallas_call(
        lambda *refs: attention_kernel(*refs, heads),
        out_shape=jax.ShapeDtypeStruct((NEAR, fars, tokens, width), jnp.bfloat16),
        in_specs=[smem, vmem, vmem, vmem, vmem],
        out_specs=vmem,
        compiler_params=pltpu.CompilerParams(vmem_limit_bytes=24 * 2**20),
        name="attention",
    )(place, mine, other, own_cache, pair_cache)
    partial = lax.all_to_all(partial.reshape(NEAR, rows, width), NEARBY, 0, 0, tiled=True)
    partial = pl.pallas_call(
        lambda *refs: merge_kernel(*refs, heads),
        out_shape=jax.ShapeDtypeStruct((rows, width), jnp.bfloat16),
        in_specs=[vmem],
        out_specs=vmem,
        compiler_params=pltpu.CompilerParams(vmem_limit_bytes=12 * 2**20),
        name="merge",
    )(partial)
    partial = lax.all_to_all(partial.reshape(fars, tokens, width), "far", 0, 0, tiled=True)
    projected = pl.pallas_call(
        lambda *refs: project_kernel(*refs, heads, o_weight.shape[1]),
        out_shape=jax.ShapeDtypeStruct((sub_count, tokens, D), jnp.bfloat16),
        in_specs=[vmem, vmem],
        out_specs=vmem,
        compiler_params=pltpu.CompilerParams(vmem_limit_bytes=12 * 2**20),
        name="project",
    )(partial, o_full)

    shares = lax.all_to_all(projected, "sub", 0, 0, tiled=True)
    quarter = D // sub_count
    slots = w_gate.shape[0] * ctx_count * CAP
    outgoing, hidden_part = pl.pallas_call(
        norm_kernel,
        out_shape=(
            jax.ShapeDtypeStruct((slots, quarter), jnp.bfloat16),
            jax.ShapeDtypeStruct((tokens, quarter), jnp.float32),
        ),
        in_specs=[smem, vmem, vmem, vmem, vmem],
        out_specs=(vmem, vmem),
        compiler_params=pltpu.CompilerParams(vmem_limit_bytes=8 * 2**20),
        name="norm",
    )(place, shares, residual, norm_gain.reshape(D // 128, 128), route_ids)
    received = lax.all_to_all(outgoing.reshape(ctx_count, CAP, quarter), SPREAD, 0, 0, tiled=True)
    received = lax.all_gather(received.reshape(slots, quarter), "sub", axis=0, tiled=False)
    partial_out = pl.pallas_call(
        expert_kernel,
        out_shape=jax.ShapeDtypeStruct((sub_count, slots, quarter), jnp.bfloat16),
        in_specs=[vmem, vmem, vmem, vmem],
        out_specs=vmem,
        compiler_params=pltpu.CompilerParams(vmem_limit_bytes=16 * 2**20),
        name="experts",
    )(received, w_gate[0].T, w_up[0].T, w_down[0])
    parts = lax.all_to_all(partial_out, "sub", 0, 0, tiled=True)
    summed = jnp.sum(parts.astype(jnp.float32), axis=0).astype(jnp.bfloat16)
    summed = summed.reshape(ctx_count, CAP, quarter)
    back = lax.all_to_all(summed, SPREAD, 0, 0, tiled=True)
    return pl.pallas_call(
        final_kernel,
        out_shape=jax.ShapeDtypeStruct((tokens, quarter), jnp.bfloat16),
        in_specs=[vmem] * 4,
        out_specs=vmem,
        compiler_params=pltpu.CompilerParams(vmem_limit_bytes=8 * 2**20),
        name="final",
    )(hidden_part, back.reshape(slots, quarter), route_ids, route_weights)


def solution(mesh):
    planes = mesh.shape["ctx"] // 2
    split = Mesh(
        mesh.devices.reshape(mesh.shape["grp"], planes // NEAR, NEAR // PAIR, PAIR, 2, mesh.shape["sub"]),
        (*GRP_CTX, "sub"),
    )
    return jax.shard_map(
        body,
        mesh=split,
        in_specs=(
            P(GRP_CTX, "sub"),
            P(GRP_CTX, None),
            P(GRP_CTX),
            P(("grp", "sub"), None, CTX),
            P("sub", CTX),
            P(GRP_CTX, None),
            P(),
            P(GRP_CTX, None),
            P(GRP_CTX, None),
            P(CTX, None, "sub"),
            P(CTX, None, "sub"),
            P(CTX, "sub", None),
        ),
        out_specs=P(GRP_CTX, "sub"),
        check_vma=False,
    )
```

```python
import jax
import jax.numpy as jnp
from jax import lax
from jax.experimental import pallas as pl
from jax.experimental.pallas import tpu as pltpu
from jax.sharding import Mesh
from jax.sharding import PartitionSpec as P

D = 2048
NOPE = 128
ROPE = 64
VDIM = 128
LATENT = 512
TOP = 6
CAP = 2
NEAR = 4
PAIR = 2
NEARBY = ("hop", "pair")
CTX = ("far", "hop", "pair", "core")
GRP_CTX = ("grp", *CTX)
SPREAD = ("hop", "pair", "core", "far")
EXTRA = 128

epsilon = 1e-06


def thirds(x):
    high = x.astype(jnp.bfloat16)
    rest = x - high.astype(jnp.float32)
    middle = rest.astype(jnp.bfloat16)
    low = (rest - middle.astype(jnp.float32)).astype(jnp.bfloat16)
    return high.astype(jnp.float32), middle.astype(jnp.float32), low.astype(jnp.float32)


def log_block(logs, rows):
    lane = lax.broadcasted_iota(jnp.int32, (rows, EXTRA), 1)
    heads = len(logs)
    block = jnp.zeros((rows, EXTRA), jnp.float32)
    for h, x in enumerate(logs):
        for piece, part in enumerate(thirds(x)):
            block = jnp.where(lane == heads * piece + h, part, block)
    return block.astype(jnp.bfloat16)


def pack_kernel(queries, ups, packed, heads):
    step = NOPE + ROPE
    per_row = 256 // NOPE
    rows = []
    for r in range(heads // per_row):
        rows.append([queries[:, h * step : h * step + NOPE] for h in range(per_row * r, per_row * r + per_row)])
    rows.append([queries[:, h * step + NOPE : h * step + step] for h in range(heads)])
    parts = [jnp.concatenate(r, axis=1) for r in rows]
    parts.append(ups[...])
    at = 0
    for part in parts:
        packed[at : at + part.shape[0], :] = part
        at += part.shape[0]


def attention_kernel(place, mine, other, both, out, heads):
    planes = mine.shape[0]
    rows = planes * 8
    first = place[0] == 0
    scale = (NOPE + ROPE) ** (-0.5)
    per_row = 256 // NOPE
    q_rows = heads // per_row * 8
    kv_at = q_rows + 8
    caches = [(both[c, :LATENT, :], both[c, LATENT : LATENT + ROPE, :], both[c, LATENT + ROPE :, :]) for c in (0, 1)]
    logs, tops = [], []
    for h in range(heads):
        a = mine[:, kv_at + 8 * h : kv_at + 8 * h + 8, :]
        b = other[:, kv_at + 8 * h : kv_at + 8 * h + 8, :]
        up = jnp.stack([jnp.where(first, a, b), jnp.where(first, b, a)], axis=1)
        up = up.reshape(planes * 16, 256)
        at, lane = 8 * (h // per_row), NOPE * (h % per_row)
        nope = mine[:, at : at + 8, lane : lane + NOPE].reshape(rows, NOPE)
        rope = mine[:, q_rows : q_rows + 8, ROPE * h : ROPE * h + ROPE].reshape(rows, ROPE)
        absorbed = lax.dot_general(
            nope, up[:, :NOPE], (((1,), (1,)), ((), ())), preferred_element_type=jnp.float32
        ).astype(jnp.bfloat16)
        scores = []
        for latents, rotary, live in caches:
            score = jnp.dot(absorbed, latents, preferred_element_type=jnp.float32)
            score = (score + jnp.dot(rope, rotary, preferred_element_type=jnp.float32)) * scale
            scores.append(jnp.where(live[:1].astype(jnp.float32) > 0.5, score, -jnp.inf))
        highest = jnp.maximum(
            jnp.max(scores[0], axis=1, keepdims=True), jnp.max(scores[1], axis=1, keepdims=True)
        )
        total, mixed = 0.0, 0.0
        for score, (latents, _, _) in zip(scores, caches):
            weights = jnp.exp(score - highest).astype(jnp.bfloat16)
            total += jnp.sum(weights.astype(jnp.float32), axis=1, keepdims=True)
            mixed += lax.dot_general(
                weights, latents, (((1,), (1,)), ((), ())), preferred_element_type=jnp.float32
            )
        head = jnp.dot(mixed.astype(jnp.bfloat16), up[:, NOPE:], preferred_element_type=jnp.float32)
        tops.append((head / total).astype(jnp.bfloat16))
        logs.append(highest + jnp.log(total))
    result = jnp.concatenate([*tops, log_block(logs, rows)], axis=1)
    result = result.reshape(planes, 8, result.shape[1])
    for z in range(planes):
        out[z % NEAR, z // NEAR] = result[z]


def merged(parts, heads):
    sources, rows, _ = parts.shape
    width = heads * VDIM
    lane = lax.broadcasted_iota(jnp.int32, (EXTRA, width), 0)
    col = lax.broadcasted_iota(jnp.int32, (EXTRA, width), 1)
    spread = ((lane < 3 * heads) & (lane % heads == col // VDIM)).astype(jnp.bfloat16)
    packed = parts[:, :, width:].reshape(sources * rows, EXTRA)
    logs = jnp.dot(packed, spread, preferred_element_type=jnp.float32).reshape(sources, rows, width)
    top = jnp.max(logs, axis=0)
    shares = jnp.exp(logs - top[None])
    total = jnp.sum(shares, axis=0)
    mixed = jnp.sum(shares * parts[:, :, :width].astype(jnp.float32), axis=0)
    return mixed / total, top + jnp.log(total)


def merge_kernel(parts, out, heads):
    mixed, logs = merged(parts[...], heads)
    rows = mixed.shape[0]
    block = log_block([logs[:, VDIM * h : VDIM * h + EXTRA] for h in range(heads)], rows)
    out[...] = jnp.concatenate([mixed.astype(jnp.bfloat16), block], axis=1)


def join_kernel(parts, out, heads):
    out[...] = merged(parts[...], heads)[0].astype(jnp.bfloat16)


def project_kernel(rows, weight, out):
    pairs, tokens, _ = rows.shape
    projected = lax.dot_general(
        rows[...].reshape(pairs * tokens, -1),
        weight[...],
        (((1,), (1,)), ((), ())),
        preferred_element_type=jnp.float32,
    ).astype(jnp.bfloat16)
    for p in range(pairs):
        for s in range(out.shape[1]):
            out[p, s] = projected[p * tokens : p * tokens + tokens]


def picked(ids, slots, weights=None):
    tokens = ids.shape[0]
    fars = slots // (CAP * NEAR * 2)
    lane = lax.broadcasted_iota(jnp.int32, (tokens, slots), 1)
    expert = lane // CAP % fars * (NEAR * 2) + lane // (CAP * fars)
    named = jnp.zeros((tokens, slots), jnp.float32)
    share = named
    for k in range(TOP):
        same = ids[:, k : k + 1] == expert
        named = jnp.where(same, 1.0, named)
        share = jnp.where(same, 1.0 if weights is None else weights[:, k : k + 1], share)
    r = lax.broadcasted_iota(jnp.int32, (tokens, tokens), 0)
    c = lax.broadcasted_iota(jnp.int32, (tokens, tokens), 1)
    earlier = jnp.dot(
        (c < r).astype(jnp.bfloat16), named.astype(jnp.bfloat16), preferred_element_type=jnp.float32
    )
    return jnp.where(earlier == (lane % CAP).astype(jnp.float32), share, 0.0)


def norm_kernel(place, shares, residual, gain, ids, out, hidden_part, held, step):
    tokens = residual.shape[0]
    quarter = hidden_part.shape[1]
    sums = [jnp.sum(shares[p].astype(jnp.float32), axis=0) for p in range(shares.shape[0])]
    whole = [x[:, at : at + step] for at in range(0, sums[0].shape[1], step) for x in sums]
    hidden = residual[...].astype(jnp.float32) + jnp.concatenate(whole, axis=1)
    held[...] = hidden
    inverse_rms = lax.rsqrt(jnp.mean(hidden * hidden, axis=1, keepdims=True) + epsilon)
    part = held[:, pl.ds(pl.multiple_of(place[1] * quarter, quarter), quarter)]
    hidden_part[...] = part
    gains = gain[...].astype(jnp.float32)
    lanes = gains.shape[1]
    which = lax.broadcasted_iota(jnp.int32, gains.shape, 0) - place[1] * (quarter // lanes)
    own_gain = [
        jnp.sum(jnp.where(which == k, gains, 0.0), axis=0, keepdims=True) for k in range(quarter // lanes)
    ]
    normed = (part * inverse_rms * jnp.concatenate(own_gain, axis=1)).astype(jnp.bfloat16)
    taken = lax.dot_general(
        picked(ids[...], out.shape[0] * CAP).astype(jnp.bfloat16),
        normed,
        (((0,), (0,)), ((), ())),
        preferred_element_type=jnp.float32,
    ).astype(jnp.bfloat16)
    out[...] = taken.reshape(out.shape)


def expert_kernel(received, gate, up, down, out):
    subs, _, quarter = out.shape
    side = (((1,), (1,)), ((), ()))
    gate_act, up_act = 0.0, 0.0
    for s in range(subs):
        rows = received[s].reshape(out.shape[1:])
        cols = slice(s * quarter, (s + 1) * quarter)
        gate_act += lax.dot_general(rows, gate[:, cols], side, preferred_element_type=jnp.float32)
        up_act += lax.dot_general(rows, up[:, cols], side, preferred_element_type=jnp.float32)
    gated = (gate_act / (1.0 + jnp.exp(-gate_act)) * up_act).astype(jnp.bfloat16)
    for s in range(subs):
        cols = slice(s * quarter, (s + 1) * quarter)
        out[s] = jnp.dot(gated, down[:, cols], preferred_element_type=jnp.float32).astype(jnp.bfloat16)


def final_kernel(hidden_part, back, ids, weights, out):
    share = picked(ids[...], back.shape[0], weights[...])
    routed = jnp.dot(share.astype(jnp.bfloat16), back[...], preferred_element_type=jnp.float32)
    out[...] = (hidden_part[...] + routed).astype(jnp.bfloat16)


def body(
    queries,
    latent_cache,
    cache_len,
    kv_up,
    o_weight,
    residual,
    norm_gain,
    route_ids,
    route_weights,
    w_gate,
    w_up,
    w_down,
):
    ctx_count = lax.axis_size(CTX)
    sub_count = lax.axis_size("sub")
    heads = kv_up.shape[0]
    tokens = queries.shape[0]
    width = heads * VDIM + EXTRA
    planes = ctx_count // 2

    smem = pl.BlockSpec(memory_space=pltpu.SMEM)
    vmem = pl.BlockSpec(memory_space=pltpu.VMEM)
    place = jnp.stack([lax.axis_index("core"), lax.axis_index("sub"), lax.axis_index("far")])
    o_part = lax.all_gather(o_weight.T, ("far", "hop", "core"), axis=0, tiled=True)
    ups = kv_up.transpose(0, 2, 1).reshape(-1, 256)
    taken = heads * (NOPE + ROPE) // 256 * tokens + ups.shape[0]
    packed = pl.pallas_call(
        lambda *refs: pack_kernel(*refs, heads),
        out_shape=jax.ShapeDtypeStruct((taken, 256), jnp.bfloat16),
        in_specs=[vmem] * 2,
        out_specs=vmem,
        compiler_params=pltpu.CompilerParams(vmem_limit_bytes=8 * 2**20),
        name="pack",
    )(queries, ups)
    both = lax.all_gather(packed, "pair", axis=0, tiled=False)
    live = lax.broadcasted_iota(jnp.int32, (8, latent_cache.shape[0]), 1) < cache_len[0]
    own_cache = jnp.concatenate([latent_cache.T, live.astype(jnp.bfloat16)], axis=0)
    caches = lax.all_gather(own_cache, "core", axis=0, tiled=False)
    mine = lax.all_gather(both.reshape(PAIR * taken, 256), ("far", "hop"), axis=0, tiled=True)
    mine = mine.reshape(planes, taken, 256)
    other = lax.ppermute(mine, "core", [(0, 1), (1, 0)])

    fars = planes // NEAR
    rows = fars * tokens
    partial = pl.pallas_call(
        lambda *refs: attention_kernel(*refs, heads),
        out_shape=jax.ShapeDtypeStruct((NEAR, fars, tokens, width), jnp.bfloat16),
        in_specs=[smem, vmem, vmem, vmem],
        out_specs=vmem,
        compiler_params=pltpu.CompilerParams(vmem_limit_bytes=24 * 2**20),
        name="attention",
    )(place, mine, other, caches)
    partial = lax.all_to_all(partial.reshape(NEAR, rows, width), NEARBY, 0, 0, tiled=True)
    partial = pl.pallas_call(
        lambda *refs: merge_kernel(*refs, heads),
        out_shape=jax.ShapeDtypeStruct((rows, width), jnp.bfloat16),
        in_specs=[vmem],
        out_specs=vmem,
        compiler_params=pltpu.CompilerParams(vmem_limit_bytes=12 * 2**20),
        name="merge",
    )(partial)
    partial = lax.all_to_all(partial.reshape(fars, tokens, width), "far", 0, 0, tiled=True)
    joined = pl.pallas_call(
        lambda *refs: join_kernel(*refs, heads),
        out_shape=jax.ShapeDtypeStruct((tokens, heads * VDIM), jnp.bfloat16),
        in_specs=[vmem],
        out_specs=vmem,
        compiler_params=pltpu.CompilerParams(vmem_limit_bytes=8 * 2**20),
        name="join",
    )(partial)
    joined = lax.all_gather(joined, "pair", axis=0, tiled=False)
    projected = pl.pallas_call(
        project_kernel,
        out_shape=jax.ShapeDtypeStruct((PAIR, sub_count, tokens, D // PAIR), jnp.bfloat16),
        in_specs=[vmem, vmem],
        out_specs=vmem,
        compiler_params=pltpu.CompilerParams(vmem_limit_bytes=8 * 2**20),
        name="project",
    )(joined, o_part)

    shares = lax.all_to_all(
        projected.reshape(PAIR * sub_count, tokens, D // PAIR), ("pair", "sub"), 0, 0, tiled=True
    ).reshape(PAIR, sub_count, tokens, D // PAIR)
    quarter = D // sub_count
    slots = w_gate.shape[0] * ctx_count * CAP
    outgoing, hidden_part = pl.pallas_call(
        lambda *refs: norm_kernel(*refs, 2 * o_weight.shape[1]),
        out_shape=(
            jax.ShapeDtypeStruct((slots // CAP, CAP, quarter), jnp.bfloat16),
            jax.ShapeDtypeStruct((tokens, quarter), jnp.float32),
        ),
        in_specs=[smem, vmem, vmem, vmem, vmem],
        out_specs=(vmem, vmem),
        scratch_shapes=[pltpu.VMEM((tokens, D), jnp.float32)],
        compiler_params=pltpu.CompilerParams(vmem_limit_bytes=8 * 2**20),
        name="norm",
    )(place, shares, residual, norm_gain.reshape(D // 128, 128), route_ids)
    received = lax.all_to_all(outgoing, SPREAD, 0, 0, tiled=True)
    received = lax.all_gather(received, "sub", axis=0, tiled=False)
    partial_out = pl.pallas_call(
        expert_kernel,
        out_shape=jax.ShapeDtypeStruct((sub_count, slots, quarter), jnp.bfloat16),
        in_specs=[vmem, vmem, vmem, vmem],
        out_specs=vmem,
        compiler_params=pltpu.CompilerParams(vmem_limit_bytes=16 * 2**20),
        name="experts",
    )(received, w_gate[0].T, w_up[0].T, w_down[0])
    parts = lax.all_to_all(partial_out, "sub", 0, 0, tiled=True)
    summed = jnp.sum(parts.astype(jnp.float32), axis=0).astype(jnp.bfloat16)
    summed = summed.reshape(ctx_count, CAP, quarter)
    back = lax.all_to_all(summed, SPREAD, 0, 0, tiled=True)
    return pl.pallas_call(
        final_kernel,
        out_shape=jax.ShapeDtypeStruct((tokens, quarter), jnp.bfloat16),
        in_specs=[vmem] * 4,
        out_specs=vmem,
        compiler_params=pltpu.CompilerParams(vmem_limit_bytes=8 * 2**20),
        name="final",
    )(hidden_part, back.reshape(slots, quarter), route_ids, route_weights)


def solution(mesh):
    planes = mesh.shape["ctx"] // 2
    split = Mesh(
        mesh.devices.reshape(mesh.shape["grp"], planes // NEAR, NEAR // PAIR, PAIR, 2, mesh.shape["sub"]),
        (*GRP_CTX, "sub"),
    )
    return jax.shard_map(
        body,
        mesh=split,
        in_specs=(
            P(GRP_CTX, "sub"),
            P(GRP_CTX, None),
            P(GRP_CTX),
            P(("grp", "sub"), None, CTX),
            P("sub", CTX),
            P(GRP_CTX, None),
            P(),
            P(GRP_CTX, None),
            P(GRP_CTX, None),
            P(CTX, None, "sub"),
            P(CTX, None, "sub"),
            P(CTX, "sub", None),
        ),
        out_specs=P(GRP_CTX, "sub"),
        check_vma=False,
    )
```
